32 devices in a mesh: grp: 1, tile: 16 (over z, x, core), mem: 2 (over y).
Axes of the slice: x: 2, y: 2, z: 4, core: 2. Of those that a mesh axis runs over, the one named last changes fastest.
Arguments:
- ens_coarse: bfloat16 [1, 80, 128, 64, 64], P('grp', 'mem', None, 'tile'), may hold values from -6 to 6
- col_interp: bfloat16 [128, 64], replicated, may hold values from -0.75 to 0.75
- row_weights: bfloat16 [3, 128], replicated, may hold values from 0.099609375 to 0.8984375
- ctrl_vec: float32 [1, 128, 128, 128], P('grp', None, 'tile'), may hold values from -24 to 24
- band_loc: bfloat16 [128, 24], P('tile'), may hold values from -1.25 to 1.25
- row_loc: bfloat16 [128, 128], replicated, may hold values from -0.5 to 0.5
- level_loc: bfloat16 [128, 128], replicated, may hold values from -0.5 to 0.5
- hx_pert: bfloat16 [1, 80, 65536], P('grp', None, ('tile', 'mem')), may hold values from -3 to 3
- innov: float32 [1, 65536], P('grp', ('tile', 'mem')), may hold values from -48 to 48
- obs_prec: float32 [1, 65536], P('grp', ('tile', 'mem')), may hold values from 0.3 to 3
- obs_region: int32 [1, 65536], P('grp', ('tile', 'mem')), may hold values from 0 to 7
Outputs:
- increment: float32 [1, 128, 128, 128], P('grp', 'mem', 'tile')
- letkf_weights: float32 [128, 80], P('tile')
The draws below stay inside these ranges and needn't reach their ends.
Inputs may be any that keep to these rules, and one draw needn't show every extreme that they name: `obs_region`: the region of an observation among the 8 regions of its block of 4096 observations.
All inputs are finite; a program needn't handle non-finite values.
Results may differ from the reference program's by a relative error of at most 0.018.
Values may be sent and summed in bfloat16 or wider, within the bound.
A program may use at most 128 MiB of HBM per device.

```python
import math
import jax
import jax.numpy as jnp
from jax import lax

MEMBERS = 80
LEV = 128
NREG = 8
FCD = 8
TSLOTS = 1
CR = 64
FR = 128
FC = 128
CC = 64
NOBS = 65536
N_TILE = 16


def place_ends(drawn, own_key, low, largest):
    spot = [jax.random.randint(jax.random.fold_in(own_key, axis), (), 0, length) for axis, length in enumerate(drawn.shape)]
    widest = drawn.shape.index(max(drawn.shape))
    neighbour = spot[:widest] + [(spot[widest] + 1) % drawn.shape[widest]] + spot[widest + 1:]
    return drawn.at[tuple(spot)].set(low).at[tuple(neighbour)].set(largest)


def level_of(rng, extent, split, least, high):
    level = 1.0
    for dim, shards_of in split:
        draws = jax.random.uniform(jax.random.fold_in(jax.random.fold_in(rng, 6), dim), (shards_of,), jnp.float32, least / len(split), high / len(split))
        level = level * jnp.repeat(jnp.exp(draws), extent[dim] // shards_of).reshape((-1,) + (1,) * (len(extent) - 1 - dim))
    return level


def noise(stream_key, extent, width, limit, pieces=(), kind=jnp.bfloat16):
    values = width * jax.random.normal(stream_key, extent, jnp.float32)
    if pieces:
        values = values * level_of(stream_key, extent, pieces, -0.22, 0.18)
    return jnp.clip(values, -limit, limit).astype(kind)


def setup_inputs(seed: int = 0) -> dict:
    arg_keys = jax.random.split(jax.random.key(seed), 12)
    return {
        "ens_coarse": noise(arg_keys[0], (TSLOTS, MEMBERS, LEV, CR, CC), 1.0, 6.0, ((1, 2), (3, 16))),
        "col_interp": noise(arg_keys[1], (FC, CC), CC ** -0.5, 0.75),
        "row_weights": jnp.clip(jax.random.uniform(arg_keys[2], (3, FR), jnp.float32, 0.099609375, 0.8984375), 0.099609375, 0.8984375).astype(jnp.bfloat16),
        "ctrl_vec": noise(arg_keys[3], (TSLOTS, LEV, FC, FR), 4.0, 24.0, ((2, 16),), jnp.float32),
        "band_loc": noise(arg_keys[4], (FC, 3 * FCD), (3 * FCD) ** -0.5, 1.25, ((0, 16),)),
        "row_loc": noise(arg_keys[5], (FR, FR), FR ** -0.5, 0.5),
        "level_loc": noise(arg_keys[6], (LEV, LEV), LEV ** -0.5, 0.5),
        "hx_pert": noise(arg_keys[7], (TSLOTS, MEMBERS, NOBS), 0.5, 3.0, ((2, 32),)),
        "innov": noise(arg_keys[8], (TSLOTS, NOBS), 8.0, 48.0, ((1, 32),), jnp.float32),
        "obs_prec": jnp.clip(jnp.exp(math.log(3.0) - 2.3025851 * jax.random.uniform(arg_keys[9], (TSLOTS, NOBS), jnp.float32) ** level_of(arg_keys[9], (TSLOTS, NOBS), ((1, 32),), -0.2, 0.2)), 0.3, 3.0),
        "obs_region": place_ends(jax.random.randint(arg_keys[10], (TSLOTS, NOBS), 0, NREG), jax.random.fold_in(arg_keys[10], 1), 0, NREG - 1).astype(jnp.int32),
    }


def to_half(value):
    return lax.optimization_barrier(value.astype(jnp.bfloat16))

def solve_weights(gram_sums, right_side):
    member_count = gram_sums.shape[-1]
    system = gram_sums + (member_count - 1) * jnp.eye(member_count, dtype=jnp.float32)
    factor = jnp.linalg.cholesky(system)
    halfway = lax.linalg.triangular_solve(factor, right_side[..., None], left_side=True, lower=True)
    result = lax.linalg.triangular_solve(factor, halfway, left_side=True, lower=True, transpose_a=True)
    return result[..., 0]

def fine_member(ens_member, col_interp, row_weights):
    coarse_cols = jnp.einsum('tlic,jc->tlij', ens_member.astype(jnp.float32), col_interp.astype(jnp.float32), precision=lax.Precision.HIGHEST)
    padded = jnp.pad(to_half(coarse_cols).astype(jnp.float32), ((0, 0), (0, 0), (1, 1), (0, 0)))
    fine_rows = row_weights.shape[1]
    parent_row = jnp.arange(fine_rows, dtype=jnp.int32) // 2
    weights = row_weights.astype(jnp.float32)
    running = jnp.zeros(padded.shape[:2] + (fine_rows, padded.shape[3]), jnp.float32)
    for offset in range(3):
        running = running + weights[offset][None, None, :, None] * jnp.take(padded, parent_row + offset, axis=2)
    return jnp.swapaxes(to_half(running), 2, 3)

def band_apply(projected, band_loc):
    levels, columns_all, rows_all = projected.shape
    band_width = band_loc.shape[1] // 3
    blocks = columns_all // band_width
    padded = jnp.pad(projected.astype(jnp.float32), ((0, 0), (band_width, band_width), (0, 0)))
    window_index = jnp.arange(blocks, dtype=jnp.int32)[:, None] * band_width + jnp.arange(3 * band_width, dtype=jnp.int32)[None, :]
    windows = jnp.take(padded, window_index, axis=1)
    band_table = band_loc.astype(jnp.float32).reshape(blocks, band_width, 3 * band_width)
    result = jnp.einsum('bjq,lbqr->lbjr', band_table, windows, precision=lax.Precision.HIGHEST)
    return to_half(result.reshape(levels, columns_all, rows_all))

def reference(ens_coarse, col_interp, row_weights, ctrl_vec, band_loc, row_loc, level_loc, hx_pert, innov, obs_prec, obs_region):
    members = ens_coarse.shape[1]
    row_table = row_loc.astype(jnp.float32)
    level_table = level_loc.astype(jnp.float32)

    def one_member(running, ens_member):
        refined = fine_member(ens_member, col_interp, row_weights)
        slot_term = to_half(refined.astype(jnp.float32) * ctrl_vec)
        projected = to_half(jnp.sum(slot_term.astype(jnp.float32), axis=0))
        banded = band_apply(projected, band_loc)
        row_mixed = to_half(jnp.einsum('ljs,rs->ljr', banded.astype(jnp.float32), row_table, precision=lax.Precision.HIGHEST))
        localized = to_half(jnp.einsum('lm,mjr->ljr', level_table, row_mixed.astype(jnp.float32), precision=lax.Precision.HIGHEST))
        return (running + refined.astype(jnp.float32) * localized.astype(jnp.float32)[None], None)
    running, unused = lax.scan(one_member, jnp.zeros(ctrl_vec.shape, jnp.float32), jnp.moveaxis(ens_coarse, 1, 0))
    increment = running / (members - 1)
    tile_count = N_TILE
    obs_tile = hx_pert.shape[2] // tile_count

    def one_tile(tile_index):
        obs_start = tile_index * obs_tile
        observed = lax.dynamic_slice_in_dim(hx_pert, obs_start, obs_tile, 2).astype(jnp.float32)
        precision_row = lax.dynamic_slice_in_dim(obs_prec, obs_start, obs_tile, 1)
        innovation = lax.dynamic_slice_in_dim(innov, obs_start, obs_tile, 1)
        region = lax.dynamic_slice_in_dim(obs_region, obs_start, obs_tile, 1)
        weighted = to_half(observed * precision_row[:, None, :]).astype(jnp.float32)
        labels = jnp.arange(NREG, dtype=jnp.int32)
        member_of = (region[:, None, :] == labels[None, :, None]).astype(jnp.float32)
        gram_sums = jnp.einsum('tko,tro,tjo->rkj', weighted, member_of, observed, precision=lax.Precision.HIGHEST)
        right_side = jnp.einsum('tko,tro,to->rk', weighted, member_of, innovation, precision=lax.Precision.HIGHEST)
        return solve_weights(gram_sums, right_side)
    weights = lax.map(one_tile, jnp.arange(tile_count, dtype=jnp.int32))
    return (increment, weights.reshape(tile_count * NREG, members))
```

```python
import functools

import jax
import jax.numpy as jnp
from jax import lax
from jax.experimental import pallas as pl
from jax.experimental.pallas import tpu as pltpu
from jax.sharding import PartitionSpec as P

NREG = 8
GROUP = 16
MESH = pl.DeviceIdType.MESH


def extended(value, sides, width):
    for axis, dim in sides:
        peers, length = (lax.axis_size(axis), value.shape[dim])
        up = [(i, (i + 1) % peers) for i in range(peers - 1)]
        down = [(j, i) for i, j in up]
        last = lax.slice_in_dim(value, length - width, length, axis=dim)
        first = lax.slice_in_dim(value, 0, width, axis=dim)
        before = lax.ppermute(last, axis, up)
        after = lax.ppermute(first, axis, down)
        value = jnp.concatenate([before, value, after], axis=dim)
    return value


def swap_add(value):
    peers = lax.axis_size("mem")
    me = lax.axis_index("mem")
    length = value.shape[0] // peers
    total = lax.dynamic_slice_in_dim(value, me * length, length, 0)
    for shift in range(1, peers):
        other = lax.rem(me + shift, peers)
        part = lax.dynamic_slice_in_dim(value, other * length, length, 0)
        pairs = [(i, (i + shift) % peers) for i in range(peers)]
        total = total + lax.ppermute(part, "mem", pairs)
    return total


def collect(value):
    peers = lax.axis_size("mem")
    me = lax.axis_index("mem")
    length = value.shape[0]
    result = jnp.zeros((peers * length,) + value.shape[1:], value.dtype)
    result = lax.dynamic_update_slice_in_dim(result, value, me * length, 0)
    for shift in range(1, peers):
        pairs = [(i, (i + shift) % peers) for i in range(peers)]
        moved = lax.ppermute(value, "mem", pairs)
        source = lax.rem(me + peers - shift, peers)
        result = lax.dynamic_update_slice_in_dim(result, moved, source * length, 0)
    return result


def row_matrix(row_weights, fine_rows, coarse_rows):
    fine_index = lax.broadcasted_iota(jnp.int32, (fine_rows, coarse_rows), 0)
    coarse_index = lax.broadcasted_iota(jnp.int32, (fine_rows, coarse_rows), 1)
    weights = row_weights.astype(jnp.float32)
    stencil = jnp.zeros((fine_rows, coarse_rows), jnp.float32)
    for offset in range(3):
        matched = coarse_index == fine_index // 2 + offset - 1
        stencil = stencil + jnp.where(matched, weights[offset][:, None], 0.0)
    return stencil.astype(jnp.bfloat16)


def solve_weights(gram_sums, right_side):
    member_count = gram_sums.shape[-1]
    system = gram_sums + (member_count - 1) * jnp.eye(member_count, dtype=jnp.float32)
    factor = jnp.linalg.cholesky(system)
    halfway = lax.linalg.triangular_solve(factor, right_side[..., None], left_side=True, lower=True)
    result = lax.linalg.triangular_solve(
        factor, halfway, left_side=True, lower=True, transpose_a=True
    )
    return result[..., 0]


def plain_increment(
    ens_coarse, col_interp, row_weights, ctrl_vec, band_loc, row_loc, level_loc, total_members
):
    fine_rows = row_weights.shape[1]
    columns = band_loc.shape[0]
    coarse_cols = jnp.einsum(
        "tklic,jc->tklij", ens_coarse, col_interp, preferred_element_type=jnp.float32
    ).astype(jnp.bfloat16)
    stencil = row_matrix(row_weights, fine_rows, fine_rows // 2)
    refined = jnp.einsum(
        "tklij,ri->tkljr",
        lax.all_to_all(coarse_cols, "tile", split_axis=4, concat_axis=3, tiled=True),
        stencil,
        preferred_element_type=jnp.float32,
    ).astype(jnp.bfloat16)
    member_fine = refined[0]
    slot_term = member_fine * ctrl_vec[0][None]
    projected = slot_term.astype(jnp.bfloat16)
    if lax.axis_size("grp") > 1:
        projected = lax.psum(projected, "grp")
    padded = extended(projected, (("tile", 2),), columns)
    banded = jnp.einsum(
        "jq,klqr->kljr", band_loc, padded, preferred_element_type=jnp.float32
    ).astype(jnp.bfloat16)
    row_mixed = jnp.einsum(
        "kljs,rs->kljr", banded, row_loc, preferred_element_type=jnp.float32
    ).astype(jnp.bfloat16)
    localized = jnp.einsum(
        "lm,kmjr->kljr", level_loc, row_mixed, preferred_element_type=jnp.float32
    ).astype(jnp.bfloat16)
    return swap_add(
        jnp.sum(member_fine.astype(jnp.float32) * localized.astype(jnp.float32), axis=0)
    ) / (total_members - 1)


def place():
    tile = lax.axis_index("tile")
    core = lax.rem(tile, 2)
    chip = lax.div(tile, 2)
    return lax.div(chip, 2), lax.rem(chip, 2), core, lax.axis_index("mem")


def target(z, x, core, y):
    return {"tile": (z * 2 + x) * 2 + core, "mem": y}


def greet(peers):
    barrier = pltpu.get_barrier_semaphore()
    for peer in peers:
        pl.semaphore_signal(barrier, inc=1, device_id=peer, device_id_type=MESH)
    pl.semaphore_wait(barrier, len(peers))


def spread_kernel(depth, own, slots, halo, send_a, recv_a, send_x, recv_x, send_y, recv_y, send_h, recv_h, local):
    z, x, core, y = place()
    per_side = 2 * depth // 4
    side = lax.div(z, per_side)
    line = [(lax.rem(z + dz, depth), lax.rem(core + dc, 2)) for dz in range(depth) for dc in range(2)]
    greet(
        [target(zz, x, cc, y) for zz, cc in line[1:]]
        + [target(z, 1 - x, core, y), target(z, x, core, 1 - y)]
    )
    mine = lax.rem(z, per_side) * 4 + x * 2 + core
    kind = lax.rem(z, per_side) * 2 + core
    for zz in range(depth):
        to_self = jnp.logical_and(z == zz, core == side)

        @pl.when(jnp.logical_not(to_self))
        def _():
            pltpu.make_async_remote_copy(
                own.at[y], slots.at[mine, y], send_a.at[zz], recv_a.at[kind],
                target(zz, x, side, y), MESH,
            ).start()

        @pl.when(to_self)
        def _():
            pltpu.make_async_copy(own.at[y], slots.at[mine, y], recv_a.at[kind]).start()

    def arrived(slot, half, sem):
        pltpu.make_async_copy(slots.at[slot, half], slots.at[slot, half], sem).wait()

    def forward(slot, half, send, recv, peer):
        pltpu.make_async_remote_copy(
            slots.at[slot, half], slots.at[slot, half], send, recv, peer, MESH
        ).start()

    count = per_side * 2
    across, beside = target(z, x, core, 1 - y), target(z, 1 - x, core, y)
    for k in range(count):
        slot = (k // 2) * 4 + x * 2 + k % 2
        arrived(slot, y, recv_a.at[k])
        forward(slot, y, send_x.at[k], recv_x.at[k], beside)
        forward(slot, y, send_y.at[k], recv_y.at[k], across)
    for k in range(count):
        slot = (k // 2) * 4 + (1 - x) * 2 + k % 2
        arrived(slot, y, recv_x.at[k])
        forward(slot, y, send_y.at[count + k], recv_y.at[count + k], across)
    for k in range(count):
        arrived((k // 2) * 4 + x * 2 + k % 2, 1 - y, recv_y.at[k])
    for k in range(count):
        arrived((k // 2) * 4 + (1 - x) * 2 + k % 2, 1 - y, recv_y.at[count + k])
    edge = (1 - core) * (2 * count - 1)
    last = pltpu.make_async_remote_copy(
        slots.at[edge], halo, send_h, recv_h, target(z, x, 1 - core, y), MESH
    )
    last.start()
    for k in range(count):
        arrived((k // 2) * 4 + x * 2 + k % 2, y, send_x.at[k])
    for k in range(2 * count):
        arrived(k, y, send_y.at[k])
    for zz in range(depth):
        @pl.when(jnp.logical_not(jnp.logical_and(z == zz, core == side)))
        def _():
            pltpu.make_async_copy(own.at[y], own.at[y], send_a.at[zz]).wait()
    last.wait()


def spread(own, depth):
    shape = (depth * 2,) + own.shape
    dma = pltpu.SemaphoreType.DMA
    count = depth
    return pl.pallas_call(
        functools.partial(spread_kernel, depth),
        out_shape=(
            jax.ShapeDtypeStruct(shape, own.dtype),
            jax.ShapeDtypeStruct(own.shape, own.dtype),
        ),
        in_specs=[pl.BlockSpec(memory_space=pltpu.VMEM)],
        out_specs=(pl.BlockSpec(memory_space=pl.ANY),) * 2,
        scratch_shapes=[
            dma((depth,)), dma((count,)), dma((count,)), dma((count,)),
            dma((2 * count,)), dma((2 * count,)), dma, dma, dma,
        ],
        compiler_params=pltpu.CompilerParams(collective_id=0, has_side_effects=True),
        cost_estimate=pl.CostEstimate(flops=10**9, bytes_accessed=10**7, transcendentals=0),
    )(own)


def ensemble_kernel(
    first, own, other, slots, halo, interp, stencil, row_loc, level_loc, start, total,
    coarse, fine, proj, banded, kron, acc
):
    member = pl.program_id(0)
    sources = own.shape[0]
    columns, rows, levels = fine.shape
    coarse_rows = stencil.shape[1]
    kept = acc.shape[0]
    stride = coarse_rows + 8
    core = lax.rem(lax.axis_index("tile"), 2)
    f32 = jnp.float32

    @pl.when(member == 0)
    def _():
        if first:
            acc[...] = jnp.zeros_like(acc)
        else:
            acc[...] = start[...].astype(f32)
        spread_rows = (
            lax.broadcasted_iota(jnp.int32, (128, 8), 0) // GROUP
            == lax.broadcasted_iota(jnp.int32, (128, 8), 1)
        ).astype(jnp.bfloat16)
        spread_cols = (
            lax.broadcasted_iota(jnp.int32, (128, 24 * GROUP), 0)
            == lax.broadcasted_iota(jnp.int32, (128, 24 * GROUP), 1) // GROUP
        ).astype(jnp.bfloat16)
        same = lax.rem(lax.broadcasted_iota(jnp.int32, (128, 24 * GROUP), 0), GROUP) == lax.rem(
            lax.broadcasted_iota(jnp.int32, (128, 24 * GROUP), 1), GROUP
        )
        for b in range(kept // 8):
            band = slots[b, 0, 4 * rows : 4 * rows + 8, :]
            tall = jnp.dot(spread_rows, band, preferred_element_type=f32).astype(jnp.bfloat16)
            wide = jnp.dot(tall, spread_cols, preferred_element_type=f32)
            kron[b] = jnp.where(same, wide, 0.0).astype(jnp.bfloat16)

    for source in range(sources):
        for part in range(2):
            held = (own, other)[part]
            row = 4 * source + 2 * (core if part == 0 else 1 - core)
            pair = jnp.concatenate([held[source, 0, 0], held[source, 0, 1]], axis=1)
            mixed = jnp.dot(interp[...], pair, preferred_element_type=f32)
            for k in range(2):
                coarse[pl.ds(row + k, columns, stride=stride), :] = mixed[:, k * levels : (k + 1) * levels]

    def refine(pair, table):
        base = 2 * pair * stride
        joined = jnp.concatenate(
            [coarse[pl.ds(base + k * stride, coarse_rows), :].astype(jnp.bfloat16) for k in range(2)], axis=1
        )
        result = jnp.dot(stencil[...], joined, preferred_element_type=f32).astype(jnp.bfloat16)
        for k in range(2):
            piece = result[:, k * levels : (k + 1) * levels]
            j = 2 * pair + k
            fine[j] = piece
            proj[j] = (piece.astype(f32) * table(k).astype(f32)).astype(jnp.bfloat16)

    def edge(pair, column):
        def table(k):
            j = column + k
            return halo[j // 4, (j % 4) * rows : (j % 4 + 1) * rows, :]
        refine(pair, table)

    for pair in range(4):
        edge(pair, 2 * pair)
        edge(columns // 2 - 4 + pair, 2 * pair)

    @pl.loop(0, kept // 8)
    def _(b):
        for pair in range(4):
            def table(k):
                j = 2 * pair + k
                return slots[b, j // 4, (j % 4) * rows : (j % 4 + 1) * rows, :]
            refine(4 + 4 * b + pair, table)

    @pl.loop(0, kept // 8)
    def _(b):
        for pair in range(rows // (2 * GROUP)):
            parts = []
            for k in range(2):
                at = (2 * pair + k) * GROUP
                parts.append(proj[pl.ds(8 * b, 24), at : at + GROUP, :].reshape(24 * GROUP, levels))
            result = jnp.dot(
                kron[b], jnp.concatenate(parts, axis=1), preferred_element_type=f32
            ).astype(jnp.bfloat16)
            for k in range(2):
                at = (2 * pair + k) * GROUP
                banded[:, at : at + GROUP, :] = result[:, k * levels : (k + 1) * levels].reshape(
                    8, GROUP, levels
                )
        for pair in range(4):
            joined = jnp.concatenate([banded[2 * pair], banded[2 * pair + 1]], axis=1)
            mixed = jnp.dot(row_loc[...], joined, preferred_element_type=f32).astype(jnp.bfloat16)
            localized = jnp.dot(mixed, level_loc[...], preferred_element_type=f32)
            for k in range(2):
                j = 8 * b + 2 * pair + k
                acc[j] += fine[8 + j].astype(f32) * localized[:, k * levels : (k + 1) * levels]

    @pl.when(member == pl.num_programs(0) - 1)
    def _():
        total[...] = acc[...].astype(total.dtype)


def ensemble_sum(own, other, slots, halo, interp, stencil, row_loc, level_loc, start):
    sources, members, _, width, levels = own.shape
    columns = interp.shape[0]
    rows, coarse_rows = stencil.shape
    kept = columns - 16
    first = start is None
    shape = (kept, rows, levels)
    if first:
        start = jnp.zeros((8, 128), jnp.float32)
    block = pl.BlockSpec((sources, 1, 2, width, levels), lambda k: (0, k, 0, 0, 0))

    def whole(value):
        return pl.BlockSpec(value.shape, lambda k: (0,) * value.ndim)

    constants = (slots, halo, interp, stencil, row_loc, level_loc, start)
    flops = 2 * members * levels * rows * columns * (coarse_rows + 24 * GROUP + rows + levels)
    bf16 = jnp.bfloat16
    return pl.pallas_call(
        functools.partial(ensemble_kernel, first),
        grid=(members,),
        out_shape=jax.ShapeDtypeStruct(shape, jnp.bfloat16),
        in_specs=[block, block] + [whole(value) for value in constants],
        out_specs=pl.BlockSpec(shape, lambda k: (0, 0, 0)),
        scratch_shapes=[
            pltpu.VMEM((columns * (coarse_rows + 8), levels), jnp.float32),
            pltpu.VMEM((columns, rows, levels), bf16),
            pltpu.VMEM((columns, rows, levels), bf16),
            pltpu.VMEM((8, rows, levels), bf16),
            pltpu.VMEM((kept // 8, 8 * GROUP, 24 * GROUP), bf16),
            pltpu.VMEM(shape, jnp.float32),
        ],
        compiler_params=pltpu.CompilerParams(
            dimension_semantics=("arbitrary",), vmem_limit_bytes=40 * 1024 * 1024
        ),
        cost_estimate=pl.CostEstimate(flops=flops, bytes_accessed=4 * own.size, transcendentals=0),
    )(own, other, *constants)


def gather_kernel(
    depth, scale, part, result, near, sums, far, turned, swap_out, swap_in,
    send_near, recv_near, send_far, recv_far, send_y, recv_y
):
    z, x, core, y = place()
    per_side = depth // 2
    side = lax.div(z, per_side)
    columns, rows = part.shape[1], part.shape[2]
    half = rows // 2
    line = [(lax.rem(z + dz, depth), lax.rem(core + dc, 2)) for dz in range(depth) for dc in range(2)]
    partners = [(1 - x, y), (x, 1 - y), (1 - x, 1 - y)]
    greet(
        [target(zz, x, cc, y) for zz, cc in line[1:]]
        + [target(z, xx, core, yy) for xx, yy in partners]
    )
    count = per_side * 2
    f32 = jnp.float32

    def rows_of(yy):
        return pl.ds(pl.multiple_of(yy * half, half), half)

    def near_copy(k, n):
        xx, yy = partners[n]
        return pltpu.make_async_remote_copy(
            part.at[(k // 2) * 4 + xx * 2 + k % 2, :, rows_of(yy), :],
            near.at[n, k], send_near.at[n, k], recv_near.at[n, k], target(z, xx, core, yy), MESH,
        )

    for k in range(count):
        for n in (2, 0, 1):
            near_copy(k, n).start()
    for k in range(count):
        for n in range(3):
            near_copy(k, n).wait_recv()
        own = part[(k // 2) * 4 + x * 2 + k % 2, :, rows_of(y), :].astype(f32)
        total = (own + near[0, k].astype(f32)) + (near[1, k].astype(f32) + near[2, k].astype(f32))
        sums[k] = total.astype(sums.dtype)
        owner = per_side * core + k // 2
        to_self = jnp.logical_and(z == owner, core == k % 2)

        @pl.when(jnp.logical_not(to_self))
        def _():
            pltpu.make_async_remote_copy(
                sums.at[k], far.at[z], send_far.at[k], recv_far.at[z],
                target(owner, x, k % 2, y), MESH,
            ).start()

        @pl.when(to_self)
        def _():
            pltpu.make_async_copy(sums.at[k], far.at[z], recv_far.at[z]).start()

    for zz in range(depth):
        pltpu.make_async_copy(far.at[zz], far.at[zz], recv_far.at[zz]).wait()
    across = target(z, x, core, 1 - y)
    levels = part.shape[3]

    def levels_of(yy):
        return pl.ds(pl.multiple_of(yy * (levels // 2), levels // 2), levels // 2)

    swaps = []
    for pair in range(columns // 2):
        pieces = []
        for k in range(2):
            value = far[0, 2 * pair + k].astype(f32)
            for zz in range(1, depth):
                value = value + far[zz, 2 * pair + k].astype(f32)
            pieces.append(value)
        turned[pair] = jnp.concatenate(pieces, axis=0).T
        swap_out[pair] = turned[pair, levels_of(1 - y), :].astype(swap_out.dtype)
        copy = pltpu.make_async_remote_copy(
            swap_out.at[pair], swap_in.at[pair], send_y.at[pair], recv_y.at[pair], across, MESH
        )
        copy.start()
        swaps.append(copy)
    for pair in range(columns // 2):
        swaps[pair].wait_recv()
        mine = turned[pair, levels_of(y), :]
        theirs = swap_in[pair].astype(f32)
        low = jnp.where(y == 0, mine, theirs)
        high = jnp.where(y == 0, theirs, mine)
        for k in range(2):
            at = slice(k * half, (k + 1) * half)
            result[:, 2 * pair + k, :] = jnp.concatenate([low[:, at], high[:, at]], axis=1) * scale
    for copy in swaps:
        copy.wait_send()
    for k in range(count):
        for n in range(3):
            near_copy(k, n).wait_send()
        owner = per_side * core + k // 2

        @pl.when(jnp.logical_not(jnp.logical_and(z == owner, core == k % 2)))
        def _():
            pltpu.make_async_copy(sums.at[k], sums.at[k], send_far.at[k]).wait()


def gather(part, depth, scale):
    columns, rows, levels = part.shape[1:]
    count = depth
    dma = pltpu.SemaphoreType.DMA
    piece = (columns, rows // 2, levels)
    swap = (columns // 2, levels // 2, rows)
    vmem = pl.BlockSpec(memory_space=pltpu.VMEM)
    return pl.pallas_call(
        functools.partial(gather_kernel, depth, scale),
        out_shape=jax.ShapeDtypeStruct((levels // 2, columns, rows), jnp.float32),
        in_specs=[vmem],
        out_specs=vmem,
        scratch_shapes=[
            pltpu.VMEM((3, count) + piece, part.dtype),
            pltpu.VMEM((count,) + piece, part.dtype),
            pltpu.VMEM((depth,) + piece, part.dtype),
            pltpu.VMEM((columns // 2, levels, rows), jnp.float32),
            pltpu.VMEM(swap, part.dtype),
            pltpu.VMEM(swap, part.dtype),
            dma((3, count)), dma((3, count)), dma((count,)), dma((depth,)),
            dma((columns // 2,)), dma((columns // 2,)),
        ],
        compiler_params=pltpu.CompilerParams(collective_id=1, has_side_effects=True),
        cost_estimate=pl.CostEstimate(flops=10**9, bytes_accessed=10**7, transcendentals=0),
    )(part)


def member_increment(
    ens_coarse, col_interp, row_weights, ctrl_vec, band_loc, row_loc, level_loc, total_members
):
    bf16 = jnp.bfloat16
    tiles = lax.axis_size("tile")
    depth, chips = tiles // 4, tiles // 2
    core = lax.rem(lax.axis_index("tile"), 2)
    columns = band_loc.shape[0]
    fine_rows = row_weights.shape[1]
    levels = level_loc.shape[0]
    members, block_rows = ens_coarse.shape[1], ens_coarse.shape[3]
    width = ens_coarse.shape[4]
    own = jnp.transpose(ctrl_vec[0], (1, 2, 0)).astype(bf16).reshape(2, columns // 2 * fine_rows, levels)
    band = jnp.pad(band_loc, ((0, 16 - columns), (0, levels - band_loc.shape[1])))
    own = jnp.concatenate([own, jnp.broadcast_to(band, (2,) + band.shape)], axis=1)
    slots, halo = spread(own, depth)
    stencil = row_matrix(row_weights, fine_rows, fine_rows // 2)
    kept = columns * tiles // 2
    padded = jnp.pad(col_interp, ((columns, columns), (0, 0)))
    interp = lax.dynamic_slice_in_dim(padded, core * kept, kept + 2 * columns, 0)
    mixing = jnp.kron(jnp.eye(2, dtype=bf16), level_loc.T)
    raw = jnp.transpose(ens_coarse[0], (0, 2, 3, 1))
    per_chip = members // chips
    raw = raw.reshape(chips, per_chip, 2, block_rows // 2, width, levels)
    pairs = [(i, i + 1 - 2 * (i % 2)) for i in range(tiles)]
    total = None
    bounds = [0, (per_chip + 1) // 2, per_chip]
    for low, high in zip(bounds[:-1], bounds[1:]):
        piece = jnp.swapaxes(raw[:, low:high], 1, 2)
        piece = piece.reshape((tiles, high - low) + raw.shape[3:])
        mine = lax.all_to_all(piece, "tile", split_axis=0, concat_axis=0, tiled=True)
        other = lax.ppermute(mine, "tile", pairs)
        total = ensemble_sum(mine, other, slots, halo, interp, stencil, row_loc, mixing, total)
    part = total.reshape(chips, columns, fine_rows, levels)
    return gather(part, depth, 1.0 / (total_members - 1))


def fits(mesh_sizes, members, columns, block_rows, fine_rows, levels):
    tiles = mesh_sizes["tile"]
    return (
        mesh_sizes["grp"] == 1
        and mesh_sizes["mem"] == 2
        and tiles % 8 == 0
        and members % (tiles // 2) == 0
        and columns == 8
        and block_rows == 4
        and fine_rows == 128
        and levels == 128
    )


def body(
    ens_coarse,
    col_interp,
    row_weights,
    ctrl_vec,
    band_loc,
    row_loc,
    level_loc,
    hx_pert,
    innov,
    obs_prec,
    obs_region,
):
    total_members = hx_pert.shape[1]
    observed = hx_pert[0]
    weighted = (observed * obs_prec[0][None, :]).astype(jnp.bfloat16)
    labels = lax.broadcasted_iota(jnp.int32, (NREG, observed.shape[1]), 0)
    member_of = obs_region[0][None, :] == labels
    masked = jnp.where(member_of[:, None, :], weighted[None], jnp.zeros((), jnp.bfloat16))
    gram_sums = jnp.einsum("rko,jo->rkj", masked, observed, preferred_element_type=jnp.float32)
    innov_rows = jnp.where(member_of, innov[0][None, :], 0.0)
    right_side = jnp.dot(
        innov_rows, weighted.astype(jnp.float32).T, precision=lax.Precision.HIGHEST
    )
    sums = jnp.concatenate([gram_sums, right_side[:, :, None]], axis=2)
    sums = swap_add(lax.psum(sums, "grp") if lax.axis_size("grp") > 1 else sums)
    sizes = {axis: lax.axis_size(axis) for axis in ("grp", "tile", "mem")}
    plan = plain_increment
    if fits(
        sizes, ens_coarse.shape[1], band_loc.shape[0], ens_coarse.shape[3], row_loc.shape[0], level_loc.shape[0]
    ):
        plan = member_increment
    increment = plan(
        ens_coarse, col_interp, row_weights, ctrl_vec, band_loc, row_loc, level_loc, total_members
    )
    own_weights = solve_weights(sums[:, :, :total_members], sums[:, :, total_members])
    weights = collect(own_weights)
    return (increment[None], weights)


def solution(mesh):
    placed = (
        P("grp", "mem", None, "tile", None),
        P(),
        P(),
        P("grp", None, "tile", None),
        P("tile", None),
        P(),
        P(),
        P("grp", None, ("tile", "mem")),
        P("grp", ("tile", "mem")),
        P("grp", ("tile", "mem")),
        P("grp", ("tile", "mem")),
    )
    return jax.shard_map(
        body,
        mesh=mesh,
        in_specs=placed,
        out_specs=(P("grp", "mem", "tile", None), P("tile", None)),
        check_vma=False,
    )
```

```python
import functools

import jax
import jax.numpy as jnp
from jax import lax
from jax.experimental import pallas as pl
from jax.experimental.pallas import tpu as pltpu
from jax.sharding import PartitionSpec as P

NREG = 8
GROUP = 16
MESH = pl.DeviceIdType.MESH


def extended(value, sides, width):
    for axis, dim in sides:
        peers, length = (lax.axis_size(axis), value.shape[dim])
        up = [(i, (i + 1) % peers) for i in range(peers - 1)]
        down = [(j, i) for i, j in up]
        last = lax.slice_in_dim(value, length - width, length, axis=dim)
        first = lax.slice_in_dim(value, 0, width, axis=dim)
        before = lax.ppermute(last, axis, up)
        after = lax.ppermute(first, axis, down)
        value = jnp.concatenate([before, value, after], axis=dim)
    return value


def swap_add(value):
    peers = lax.axis_size("mem")
    me = lax.axis_index("mem")
    length = value.shape[0] // peers
    total = lax.dynamic_slice_in_dim(value, me * length, length, 0)
    for shift in range(1, peers):
        other = lax.rem(me + shift, peers)
        part = lax.dynamic_slice_in_dim(value, other * length, length, 0)
        pairs = [(i, (i + shift) % peers) for i in range(peers)]
        total = total + lax.ppermute(part, "mem", pairs)
    return total


def collect(value):
    peers = lax.axis_size("mem")
    me = lax.axis_index("mem")
    length = value.shape[0]
    result = jnp.zeros((peers * length,) + value.shape[1:], value.dtype)
    result = lax.dynamic_update_slice_in_dim(result, value, me * length, 0)
    for shift in range(1, peers):
        pairs = [(i, (i + shift) % peers) for i in range(peers)]
        moved = lax.ppermute(value, "mem", pairs)
        source = lax.rem(me + peers - shift, peers)
        result = lax.dynamic_update_slice_in_dim(result, moved, source * length, 0)
    return result


def row_matrix(row_weights, fine_rows, coarse_rows):
    fine_index = lax.broadcasted_iota(jnp.int32, (fine_rows, coarse_rows), 0)
    coarse_index = lax.broadcasted_iota(jnp.int32, (fine_rows, coarse_rows), 1)
    weights = row_weights.astype(jnp.float32)
    stencil = jnp.zeros((fine_rows, coarse_rows), jnp.float32)
    for offset in range(3):
        matched = coarse_index == fine_index // 2 + offset - 1
        stencil = stencil + jnp.where(matched, weights[offset][:, None], 0.0)
    return stencil.astype(jnp.bfloat16)


def solve_kernel(sums, result):
    regions, members, lanes = sums.shape
    row_index = lax.broadcasted_iota(jnp.int32, (members, lanes), 0)
    col_index = lax.broadcasted_iota(jnp.int32, (members, lanes), 1)
    tables = []
    for region in range(regions):
        table = sums[region]
        square = jnp.concatenate([table, jnp.zeros((lanes - members, lanes), jnp.float32)], axis=0)
        mirrored = square.T[:members]
        table = jnp.where(col_index < members, 0.5 * (table + mirrored), table)
        tables.append(table + jnp.where(row_index == col_index, float(members - 1), 0.0))
    for k in range(members):
        for region in range(regions):
            table = tables[region]
            row = table[k : k + 1]
            pivot = row[:, k : k + 1]
            row = row / pivot
            column = table[:, k : k + 1] - jnp.where(row_index[:, :1] == k, 1.0, 0.0)
            tables[region] = table - column * row
    for region in range(regions):
        result[region] = jnp.concatenate(
            [tables[region], jnp.zeros((lanes - members, lanes), jnp.float32)], axis=0
        ).T[members : members + 8, :]


def solve_weights(sums):
    regions, members, width = sums.shape
    lanes = 128 * (-(-(members + 8) // 128))
    padded = jnp.pad(sums, ((0, 0), (0, 0), (0, lanes - width)))
    result = pl.pallas_call(
        solve_kernel,
        out_shape=jax.ShapeDtypeStruct((regions, 8, lanes), jnp.float32),
        in_specs=[pl.BlockSpec(memory_space=pltpu.VMEM)],
        out_specs=pl.BlockSpec(memory_space=pltpu.VMEM),
        cost_estimate=pl.CostEstimate(flops=10**9, bytes_accessed=4 * padded.size, transcendentals=0),
    )(padded)
    return result[:, 0, :members]


def plain_increment(
    ens_coarse, col_interp, row_weights, ctrl_vec, band_loc, row_loc, level_loc, total_members
):
    fine_rows = row_weights.shape[1]
    columns = band_loc.shape[0]
    coarse_cols = jnp.einsum(
        "tklic,jc->tklij", ens_coarse, col_interp, preferred_element_type=jnp.float32
    ).astype(jnp.bfloat16)
    stencil = row_matrix(row_weights, fine_rows, fine_rows // 2)
    refined = jnp.einsum(
        "tklij,ri->tkljr",
        lax.all_to_all(coarse_cols, "tile", split_axis=4, concat_axis=3, tiled=True),
        stencil,
        preferred_element_type=jnp.float32,
    ).astype(jnp.bfloat16)
    member_fine = refined[0]
    slot_term = member_fine * ctrl_vec[0][None]
    projected = slot_term.astype(jnp.bfloat16)
    if lax.axis_size("grp") > 1:
        projected = lax.psum(projected, "grp")
    padded = extended(projected, (("tile", 2),), columns)
    banded = jnp.einsum(
        "jq,klqr->kljr", band_loc, padded, preferred_element_type=jnp.float32
    ).astype(jnp.bfloat16)
    row_mixed = jnp.einsum(
        "kljs,rs->kljr", banded, row_loc, preferred_element_type=jnp.float32
    ).astype(jnp.bfloat16)
    localized = jnp.einsum(
        "lm,kmjr->kljr", level_loc, row_mixed, preferred_element_type=jnp.float32
    ).astype(jnp.bfloat16)
    return swap_add(
        jnp.sum(member_fine.astype(jnp.float32) * localized.astype(jnp.float32), axis=0)
    ) / (total_members - 1)


def place():
    tile = lax.axis_index("tile")
    core = lax.rem(tile, 2)
    chip = lax.div(tile, 2)
    return lax.div(chip, 2), lax.rem(chip, 2), core, lax.axis_index("mem")


def target(z, x, core, y):
    return {"tile": (z * 2 + x) * 2 + core, "mem": y}


def greet(peers):
    barrier = pltpu.get_barrier_semaphore()
    for peer in peers:
        pl.semaphore_signal(barrier, inc=1, device_id=peer, device_id_type=MESH)
    pl.semaphore_wait(barrier, len(peers))


def spread_kernel(depth, own, slots, halo, send_a, recv_a, send_x, recv_x, send_y, recv_y, send_h, recv_h, local):
    z, x, core, y = place()
    per_side = 2 * depth // 4
    side = lax.div(z, per_side)
    line = [(lax.rem(z + dz, depth), lax.rem(core + dc, 2)) for dz in range(depth) for dc in range(2)]
    greet(
        [target(zz, x, cc, y) for zz, cc in line[1:]]
        + [target(z, 1 - x, core, y), target(z, x, core, 1 - y)]
    )
    mine = lax.rem(z, per_side) * 4 + x * 2 + core
    kind = lax.rem(z, per_side) * 2 + core
    for zz in range(depth):
        to_self = jnp.logical_and(z == zz, core == side)

        @pl.when(jnp.logical_not(to_self))
        def _():
            pltpu.make_async_remote_copy(
                own.at[y], slots.at[mine, y], send_a.at[zz], recv_a.at[kind],
                target(zz, x, side, y), MESH,
            ).start()

        @pl.when(to_self)
        def _():
            pltpu.make_async_copy(own.at[y], slots.at[mine, y], recv_a.at[kind]).start()

    def arrived(slot, half, sem):
        pltpu.make_async_copy(slots.at[slot, half], slots.at[slot, half], sem).wait()

    def forward(slot, half, send, recv, peer):
        pltpu.make_async_remote_copy(
            slots.at[slot, half], slots.at[slot, half], send, recv, peer, MESH
        ).start()

    count = per_side * 2
    across, beside = target(z, x, core, 1 - y), target(z, 1 - x, core, y)
    for k in range(count):
        slot = (k // 2) * 4 + x * 2 + k % 2
        arrived(slot, y, recv_a.at[k])
        forward(slot, y, send_x.at[k], recv_x.at[k], beside)
        forward(slot, y, send_y.at[k], recv_y.at[k], across)
    for k in range(count):
        slot = (k // 2) * 4 + (1 - x) * 2 + k % 2
        arrived(slot, y, recv_x.at[k])
        forward(slot, y, send_y.at[count + k], recv_y.at[count + k], across)
    for k in range(count):
        arrived((k // 2) * 4 + x * 2 + k % 2, 1 - y, recv_y.at[k])
    for k in range(count):
        arrived((k // 2) * 4 + (1 - x) * 2 + k % 2, 1 - y, recv_y.at[count + k])
    edge = (1 - core) * (2 * count - 1)
    last = pltpu.make_async_remote_copy(
        slots.at[edge], halo, send_h, recv_h, target(z, x, 1 - core, y), MESH
    )
    last.start()
    for k in range(count):
        arrived((k // 2) * 4 + x * 2 + k % 2, y, send_x.at[k])
    for k in range(2 * count):
        arrived(k, y, send_y.at[k])
    for zz in range(depth):
        @pl.when(jnp.logical_not(jnp.logical_and(z == zz, core == side)))
        def _():
            pltpu.make_async_copy(own.at[y], own.at[y], send_a.at[zz]).wait()
    last.wait()


def spread(own, depth):
    shape = (depth * 2,) + own.shape
    dma = pltpu.SemaphoreType.DMA
    count = depth
    return pl.pallas_call(
        functools.partial(spread_kernel, depth),
        out_shape=(
            jax.ShapeDtypeStruct(shape, own.dtype),
            jax.ShapeDtypeStruct(own.shape, own.dtype),
        ),
        in_specs=[pl.BlockSpec(memory_space=pltpu.VMEM)],
        out_specs=(pl.BlockSpec(memory_space=pl.ANY),) * 2,
        scratch_shapes=[
            dma((depth,)), dma((count,)), dma((count,)), dma((count,)),
            dma((2 * count,)), dma((2 * count,)), dma, dma, dma,
        ],
        compiler_params=pltpu.CompilerParams(collective_id=0, has_side_effects=True),
        cost_estimate=pl.CostEstimate(flops=10**9, bytes_accessed=10**7, transcendentals=0),
    )(own)


def ensemble_kernel(
    first, own, other, slots, halo, interp, stencil, row_loc, level_loc, start, total,
    coarse, fine, proj, banded, kron, acc
):
    member = pl.program_id(0)
    sources = own.shape[0]
    columns, rows, levels = fine.shape
    coarse_rows = stencil.shape[1]
    kept = acc.shape[0]
    stride = coarse_rows + 8
    core = lax.rem(lax.axis_index("tile"), 2)
    f32 = jnp.float32

    @pl.when(member == 0)
    def _():
        if first:
            acc[...] = jnp.zeros_like(acc)
        else:
            acc[...] = start[...].astype(f32)
        spread_rows = (
            lax.broadcasted_iota(jnp.int32, (128, 8), 0) // GROUP
            == lax.broadcasted_iota(jnp.int32, (128, 8), 1)
        ).astype(jnp.bfloat16)
        spread_cols = (
            lax.broadcasted_iota(jnp.int32, (128, 24 * GROUP), 0)
            == lax.broadcasted_iota(jnp.int32, (128, 24 * GROUP), 1) // GROUP
        ).astype(jnp.bfloat16)
        same = lax.rem(lax.broadcasted_iota(jnp.int32, (128, 24 * GROUP), 0), GROUP) == lax.rem(
            lax.broadcasted_iota(jnp.int32, (128, 24 * GROUP), 1), GROUP
        )
        for b in range(kept // 8):
            band = slots[b, 0, 4 * rows : 4 * rows + 8, :]
            tall = jnp.dot(spread_rows, band, preferred_element_type=f32).astype(jnp.bfloat16)
            wide = jnp.dot(tall, spread_cols, preferred_element_type=f32)
            kron[b] = jnp.where(same, wide, 0.0).astype(jnp.bfloat16)

    for source in range(sources):
        for part in range(2):
            held = (own, other)[part]
            row = 4 * source + 2 * (core if part == 0 else 1 - core)
            pair = jnp.concatenate([held[source, 0, 0], held[source, 0, 1]], axis=1)
            mixed = jnp.dot(interp[...], pair, preferred_element_type=f32)
            for k in range(2):
                coarse[pl.ds(row + k, columns, stride=stride), :] = mixed[:, k * levels : (k + 1) * levels]

    def refine(pair, table):
        base = 2 * pair * stride
        joined = jnp.concatenate(
            [coarse[pl.ds(base + k * stride, coarse_rows), :].astype(jnp.bfloat16) for k in range(2)], axis=1
        )
        result = jnp.dot(stencil[...], joined, preferred_element_type=f32).astype(jnp.bfloat16)
        for k in range(2):
            piece = result[:, k * levels : (k + 1) * levels]
            j = 2 * pair + k
            fine[j] = piece
            proj[j] = (piece.astype(f32) * table(k).astype(f32)).astype(jnp.bfloat16)

    def edge(pair, column):
        def table(k):
            j = column + k
            return halo[j // 4, (j % 4) * rows : (j % 4 + 1) * rows, :]
        refine(pair, table)

    for pair in range(4):
        edge(pair, 2 * pair)
        edge(columns // 2 - 4 + pair, 2 * pair)

    @pl.loop(0, kept // 8)
    def _(b):
        for pair in range(4):
            def table(k):
                j = 2 * pair + k
                return slots[b, j // 4, (j % 4) * rows : (j % 4 + 1) * rows, :]
            refine(4 + 4 * b + pair, table)

    @pl.loop(0, kept // 8)
    def _(b):
        for pair in range(rows // (2 * GROUP)):
            parts = []
            for k in range(2):
                at = (2 * pair + k) * GROUP
                parts.append(proj[pl.ds(8 * b, 24), at : at + GROUP, :].reshape(24 * GROUP, levels))
            result = jnp.dot(
                kron[b], jnp.concatenate(parts, axis=1), preferred_element_type=f32
            ).astype(jnp.bfloat16)
            for k in range(2):
                at = (2 * pair + k) * GROUP
                banded[:, at : at + GROUP, :] = result[:, k * levels : (k + 1) * levels].reshape(
                    8, GROUP, levels
                )
        for pair in range(4):
            joined = jnp.concatenate([banded[2 * pair], banded[2 * pair + 1]], axis=1)
            mixed = jnp.dot(row_loc[...], joined, preferred_element_type=f32).astype(jnp.bfloat16)
            localized = jnp.dot(mixed, level_loc[...], preferred_element_type=f32)
            for k in range(2):
                j = 8 * b + 2 * pair + k
                acc[j] += fine[8 + j].astype(f32) * localized[:, k * levels : (k + 1) * levels]

    @pl.when(member == pl.num_programs(0) - 1)
    def _():
        total[...] = acc[...].astype(total.dtype)


def ensemble_sum(own, other, slots, halo, interp, stencil, row_loc, level_loc, start):
    sources, members, _, width, levels = own.shape
    columns = interp.shape[0]
    rows, coarse_rows = stencil.shape
    kept = columns - 16
    first = start is None
    shape = (kept, rows, levels)
    if first:
        start = jnp.zeros((8, 128), jnp.float32)
    block = pl.BlockSpec((sources, 1, 2, width, levels), lambda k: (0, k, 0, 0, 0))

    def whole(value):
        return pl.BlockSpec(value.shape, lambda k: (0,) * value.ndim)

    constants = (slots, halo, interp, stencil, row_loc, level_loc, start)
    flops = 2 * members * levels * rows * columns * (coarse_rows + 24 * GROUP + rows + levels)
    bf16 = jnp.bfloat16
    return pl.pallas_call(
        functools.partial(ensemble_kernel, first),
        grid=(members,),
        out_shape=jax.ShapeDtypeStruct(shape, jnp.bfloat16),
        in_specs=[block, block] + [whole(value) for value in constants],
        out_specs=pl.BlockSpec(shape, lambda k: (0, 0, 0)),
        scratch_shapes=[
            pltpu.VMEM((columns * (coarse_rows + 8), levels), jnp.float32),
            pltpu.VMEM((columns, rows, levels), bf16),
            pltpu.VMEM((columns, rows, levels), bf16),
            pltpu.VMEM((8, rows, levels), bf16),
            pltpu.VMEM((kept // 8, 8 * GROUP, 24 * GROUP), bf16),
            pltpu.VMEM(shape, jnp.float32),
        ],
        compiler_params=pltpu.CompilerParams(
            dimension_semantics=("arbitrary",), vmem_limit_bytes=40 * 1024 * 1024
        ),
        cost_estimate=pl.CostEstimate(flops=flops, bytes_accessed=4 * own.size, transcendentals=0),
    )(own, other, *constants)


def gather_kernel(
    depth, scale, part, result, near, sums, far, turned, swap_out, swap_in,
    send_near, recv_near, send_far, recv_far, send_y, recv_y
):
    z, x, core, y = place()
    per_side = depth // 2
    side = lax.div(z, per_side)
    columns, rows = part.shape[1], part.shape[2]
    half = rows // 2
    line = [(lax.rem(z + dz, depth), lax.rem(core + dc, 2)) for dz in range(depth) for dc in range(2)]
    partners = [(1 - x, y), (x, 1 - y), (1 - x, 1 - y)]
    greet(
        [target(zz, x, cc, y) for zz, cc in line[1:]]
        + [target(z, xx, core, yy) for xx, yy in partners]
    )
    count = per_side * 2
    f32 = jnp.float32

    def rows_of(yy):
        return pl.ds(pl.multiple_of(yy * half, half), half)

    def near_copy(k, n):
        xx, yy = partners[n]
        return pltpu.make_async_remote_copy(
            part.at[(k // 2) * 4 + xx * 2 + k % 2, :, rows_of(yy), :],
            near.at[n, k], send_near.at[n, k], recv_near.at[n, k], target(z, xx, core, yy), MESH,
        )

    for k in range(count):
        for n in (2, 0, 1):
            near_copy(k, n).start()
    for k in range(count):
        for n in range(3):
            near_copy(k, n).wait_recv()
        own = part[(k // 2) * 4 + x * 2 + k % 2, :, rows_of(y), :].astype(f32)
        total = (own + near[0, k].astype(f32)) + (near[1, k].astype(f32) + near[2, k].astype(f32))
        sums[k] = total.astype(sums.dtype)
        owner = per_side * core + k // 2
        to_self = jnp.logical_and(z == owner, core == k % 2)

        @pl.when(jnp.logical_not(to_self))
        def _():
            pltpu.make_async_remote_copy(
                sums.at[k], far.at[z], send_far.at[k], recv_far.at[z],
                target(owner, x, k % 2, y), MESH,
            ).start()

        @pl.when(to_self)
        def _():
            pltpu.make_async_copy(sums.at[k], far.at[z], recv_far.at[z]).start()

    for zz in range(depth):
        pltpu.make_async_copy(far.at[zz], far.at[zz], recv_far.at[zz]).wait()
    across = target(z, x, core, 1 - y)
    levels = part.shape[3]

    def levels_of(yy):
        return pl.ds(pl.multiple_of(yy * (levels // 2), levels // 2), levels // 2)

    swaps = []
    for pair in range(columns // 2):
        pieces = []
        for k in range(2):
            value = far[0, 2 * pair + k].astype(f32)
            for zz in range(1, depth):
                value = value + far[zz, 2 * pair + k].astype(f32)
            pieces.append(value)
        turned[pair] = jnp.concatenate(pieces, axis=0).T
        swap_out[pair] = turned[pair, levels_of(1 - y), :].astype(swap_out.dtype)
        copy = pltpu.make_async_remote_copy(
            swap_out.at[pair], swap_in.at[pair], send_y.at[pair], recv_y.at[pair], across, MESH
        )
        copy.start()
        swaps.append(copy)
    for pair in range(columns // 2):
        swaps[pair].wait_recv()
        mine = turned[pair, levels_of(y), :]
        theirs = swap_in[pair].astype(f32)
        low = jnp.where(y == 0, mine, theirs)
        high = jnp.where(y == 0, theirs, mine)
        for k in range(2):
            at = slice(k * half, (k + 1) * half)
            result[:, 2 * pair + k, :] = jnp.concatenate([low[:, at], high[:, at]], axis=1) * scale
    for copy in swaps:
        copy.wait_send()
    for k in range(count):
        for n in range(3):
            near_copy(k, n).wait_send()
        owner = per_side * core + k // 2

        @pl.when(jnp.logical_not(jnp.logical_and(z == owner, core == k % 2)))
        def _():
            pltpu.make_async_copy(sums.at[k], sums.at[k], send_far.at[k]).wait()


def gather(part, depth, scale):
    columns, rows, levels = part.shape[1:]
    count = depth
    dma = pltpu.SemaphoreType.DMA
    piece = (columns, rows // 2, levels)
    swap = (columns // 2, levels // 2, rows)
    vmem = pl.BlockSpec(memory_space=pltpu.VMEM)
    return pl.pallas_call(
        functools.partial(gather_kernel, depth, scale),
        out_shape=jax.ShapeDtypeStruct((levels // 2, columns, rows), jnp.float32),
        in_specs=[vmem],
        out_specs=vmem,
        scratch_shapes=[
            pltpu.VMEM((3, count) + piece, part.dtype),
            pltpu.VMEM((count,) + piece, part.dtype),
            pltpu.VMEM((depth,) + piece, part.dtype),
            pltpu.VMEM((columns // 2, levels, rows), jnp.float32),
            pltpu.VMEM(swap, part.dtype),
            pltpu.VMEM(swap, part.dtype),
            dma((3, count)), dma((3, count)), dma((count,)), dma((depth,)),
            dma((columns // 2,)), dma((columns // 2,)),
        ],
        compiler_params=pltpu.CompilerParams(collective_id=1, has_side_effects=True),
        cost_estimate=pl.CostEstimate(flops=10**9, bytes_accessed=10**7, transcendentals=0),
    )(part)


def member_increment(
    ens_coarse, col_interp, row_weights, ctrl_vec, band_loc, row_loc, level_loc, total_members
):
    bf16 = jnp.bfloat16
    tiles = lax.axis_size("tile")
    depth, chips = tiles // 4, tiles // 2
    core = lax.rem(lax.axis_index("tile"), 2)
    columns = band_loc.shape[0]
    fine_rows = row_weights.shape[1]
    levels = level_loc.shape[0]
    members, block_rows = ens_coarse.shape[1], ens_coarse.shape[3]
    width = ens_coarse.shape[4]
    own = jnp.transpose(ctrl_vec[0], (1, 2, 0)).astype(bf16).reshape(2, columns // 2 * fine_rows, levels)
    band = jnp.pad(band_loc, ((0, 16 - columns), (0, levels - band_loc.shape[1])))
    own = jnp.concatenate([own, jnp.broadcast_to(band, (2,) + band.shape)], axis=1)
    slots, halo = spread(own, depth)
    stencil = row_matrix(row_weights, fine_rows, fine_rows // 2)
    kept = columns * tiles // 2
    padded = jnp.pad(col_interp, ((columns, columns), (0, 0)))
    interp = lax.dynamic_slice_in_dim(padded, core * kept, kept + 2 * columns, 0)
    mixing = jnp.kron(jnp.eye(2, dtype=bf16), level_loc.T)
    raw = jnp.transpose(ens_coarse[0], (0, 2, 3, 1))
    per_chip = members // chips
    raw = raw.reshape(chips, per_chip, 2, block_rows // 2, width, levels)
    pairs = [(i, i + 1 - 2 * (i % 2)) for i in range(tiles)]
    total = None
    bounds = [0, (per_chip + 1) // 2, per_chip]
    for low, high in zip(bounds[:-1], bounds[1:]):
        piece = jnp.swapaxes(raw[:, low:high], 1, 2)
        piece = piece.reshape((tiles, high - low) + raw.shape[3:])
        mine = lax.all_to_all(piece, "tile", split_axis=0, concat_axis=0, tiled=True)
        other = lax.ppermute(mine, "tile", pairs)
        total = ensemble_sum(mine, other, slots, halo, interp, stencil, row_loc, mixing, total)
    part = total.reshape(chips, columns, fine_rows, levels)
    return gather(part, depth, 1.0 / (total_members - 1))


def fits(mesh_sizes, members, columns, block_rows, fine_rows, levels):
    tiles = mesh_sizes["tile"]
    return (
        mesh_sizes["grp"] == 1
        and mesh_sizes["mem"] == 2
        and tiles % 8 == 0
        and members % (tiles // 2) == 0
        and columns == 8
        and block_rows == 4
        and fine_rows == 128
        and levels == 128
    )


def body(
    ens_coarse,
    col_interp,
    row_weights,
    ctrl_vec,
    band_loc,
    row_loc,
    level_loc,
    hx_pert,
    innov,
    obs_prec,
    obs_region,
):
    total_members = hx_pert.shape[1]
    observed = hx_pert[0]
    weighted = (observed * obs_prec[0][None, :]).astype(jnp.bfloat16)
    labels = lax.broadcasted_iota(jnp.int32, (NREG, observed.shape[1]), 0)
    member_of = obs_region[0][None, :] == labels
    masked = jnp.where(member_of[:, None, :], weighted[None], jnp.zeros((), jnp.bfloat16))
    gram_sums = jnp.einsum("rko,jo->rkj", masked, observed, preferred_element_type=jnp.float32)
    innov_rows = jnp.where(member_of, innov[0][None, :], 0.0)
    right_side = jnp.dot(
        innov_rows, weighted.astype(jnp.float32).T, precision=lax.Precision.HIGHEST
    )
    sums = jnp.concatenate([gram_sums, right_side[:, :, None]], axis=2)
    sums = swap_add(lax.psum(sums, "grp") if lax.axis_size("grp") > 1 else sums)
    sizes = {axis: lax.axis_size(axis) for axis in ("grp", "tile", "mem")}
    plan = plain_increment
    if fits(
        sizes, ens_coarse.shape[1], band_loc.shape[0], ens_coarse.shape[3], row_loc.shape[0], level_loc.shape[0]
    ):
        plan = member_increment
    increment = plan(
        ens_coarse, col_interp, row_weights, ctrl_vec, band_loc, row_loc, level_loc, total_members
    )
    own_weights = solve_weights(sums)
    weights = collect(own_weights)
    return (increment[None], weights)


def solution(mesh):
    placed = (
        P("grp", "mem", None, "tile", None),
        P(),
        P(),
        P("grp", None, "tile", None),
        P("tile", None),
        P(),
        P(),
        P("grp", None, ("tile", "mem")),
        P("grp", ("tile", "mem")),
        P("grp", ("tile", "mem")),
        P("grp", ("tile", "mem")),
    )
    return jax.shard_map(
        body,
        mesh=mesh,
        in_specs=placed,
        out_specs=(P("grp", "mem", "tile", None), P("tile", None)),
        check_vma=False,
    )
```

```python
import functools

import jax
import jax.numpy as jnp
from jax import lax
from jax.experimental import pallas as pl
from jax.experimental.pallas import tpu as pltpu
from jax.sharding import PartitionSpec as P

NREG = 8
GROUP = 16
MESH = pl.DeviceIdType.MESH


def extended(value, sides, width):
    for axis, dim in sides:
        peers, length = (lax.axis_size(axis), value.shape[dim])
        up = [(i, (i + 1) % peers) for i in range(peers - 1)]
        down = [(j, i) for i, j in up]
        last = lax.slice_in_dim(value, length - width, length, axis=dim)
        first = lax.slice_in_dim(value, 0, width, axis=dim)
        before = lax.ppermute(last, axis, up)
        after = lax.ppermute(first, axis, down)
        value = jnp.concatenate([before, value, after], axis=dim)
    return value


def swap_add(value):
    peers = lax.axis_size("mem")
    me = lax.axis_index("mem")
    length = value.shape[0] // peers
    total = lax.dynamic_slice_in_dim(value, me * length, length, 0)
    for shift in range(1, peers):
        other = lax.rem(me + shift, peers)
        part = lax.dynamic_slice_in_dim(value, other * length, length, 0)
        pairs = [(i, (i + shift) % peers) for i in range(peers)]
        total = total + lax.ppermute(part, "mem", pairs)
    return total


def collect(value):
    peers = lax.axis_size("mem")
    me = lax.axis_index("mem")
    length = value.shape[0]
    result = jnp.zeros((peers * length,) + value.shape[1:], value.dtype)
    result = lax.dynamic_update_slice_in_dim(result, value, me * length, 0)
    for shift in range(1, peers):
        pairs = [(i, (i + shift) % peers) for i in range(peers)]
        moved = lax.ppermute(value, "mem", pairs)
        source = lax.rem(me + peers - shift, peers)
        result = lax.dynamic_update_slice_in_dim(result, moved, source * length, 0)
    return result


def row_matrix(row_weights, fine_rows, coarse_rows):
    fine_index = lax.broadcasted_iota(jnp.int32, (fine_rows, coarse_rows), 0)
    coarse_index = lax.broadcasted_iota(jnp.int32, (fine_rows, coarse_rows), 1)
    weights = row_weights.astype(jnp.float32)
    stencil = jnp.zeros((fine_rows, coarse_rows), jnp.float32)
    for offset in range(3):
        matched = coarse_index == fine_index // 2 + offset - 1
        stencil = stencil + jnp.where(matched, weights[offset][:, None], 0.0)
    return stencil.astype(jnp.bfloat16)


def solve_kernel(sums, result):
    regions, members, lanes = sums.shape
    row_index = lax.broadcasted_iota(jnp.int32, (members, lanes), 0)
    col_index = lax.broadcasted_iota(jnp.int32, (members, lanes), 1)
    tables = []
    for region in range(regions):
        table = sums[region]
        square = jnp.concatenate([table, jnp.zeros((lanes - members, lanes), jnp.float32)], axis=0)
        mirrored = square.T[:members]
        table = jnp.where(col_index < members, 0.5 * (table + mirrored), table)
        tables.append(table + jnp.where(row_index == col_index, float(members - 1), 0.0))
    for k in range(members):
        for region in range(regions):
            table = tables[region]
            row = table[k : k + 1]
            pivot = row[:, k : k + 1]
            row = row / pivot
            column = table[:, k : k + 1] - jnp.where(row_index[:, :1] == k, 1.0, 0.0)
            tables[region] = table - column * row
    for region in range(regions):
        result[region] = jnp.concatenate(
            [tables[region], jnp.zeros((lanes - members, lanes), jnp.float32)], axis=0
        ).T[members : members + 8, :]


def solve_weights(sums):
    regions, members, width = sums.shape
    lanes = 128 * (-(-(members + 8) // 128))
    padded = jnp.pad(sums, ((0, 0), (0, 0), (0, lanes - width)))
    result = pl.pallas_call(
        solve_kernel,
        out_shape=jax.ShapeDtypeStruct((regions, 8, lanes), jnp.float32),
        in_specs=[pl.BlockSpec(memory_space=pltpu.VMEM)],
        out_specs=pl.BlockSpec(memory_space=pltpu.VMEM),
        cost_estimate=pl.CostEstimate(flops=10**9, bytes_accessed=4 * padded.size, transcendentals=0),
    )(padded)
    return result[:, 0, :members]


def plain_increment(
    ens_coarse, col_interp, row_weights, ctrl_vec, band_loc, row_loc, level_loc, total_members
):
    fine_rows = row_weights.shape[1]
    columns = band_loc.shape[0]
    coarse_cols = jnp.einsum(
        "tklic,jc->tklij", ens_coarse, col_interp, preferred_element_type=jnp.float32
    ).astype(jnp.bfloat16)
    stencil = row_matrix(row_weights, fine_rows, fine_rows // 2)
    refined = jnp.einsum(
        "tklij,ri->tkljr",
        lax.all_to_all(coarse_cols, "tile", split_axis=4, concat_axis=3, tiled=True),
        stencil,
        preferred_element_type=jnp.float32,
    ).astype(jnp.bfloat16)
    member_fine = refined[0]
    slot_term = member_fine * ctrl_vec[0][None]
    projected = slot_term.astype(jnp.bfloat16)
    if lax.axis_size("grp") > 1:
        projected = lax.psum(projected, "grp")
    padded = extended(projected, (("tile", 2),), columns)
    banded = jnp.einsum(
        "jq,klqr->kljr", band_loc, padded, preferred_element_type=jnp.float32
    ).astype(jnp.bfloat16)
    row_mixed = jnp.einsum(
        "kljs,rs->kljr", banded, row_loc, preferred_element_type=jnp.float32
    ).astype(jnp.bfloat16)
    localized = jnp.einsum(
        "lm,kmjr->kljr", level_loc, row_mixed, preferred_element_type=jnp.float32
    ).astype(jnp.bfloat16)
    return swap_add(
        jnp.sum(member_fine.astype(jnp.float32) * localized.astype(jnp.float32), axis=0)
    ) / (total_members - 1)


def place():
    tile = lax.axis_index("tile")
    core = lax.rem(tile, 2)
    chip = lax.div(tile, 2)
    return lax.div(chip, 2), lax.rem(chip, 2), core, lax.axis_index("mem")


def target(z, x, core, y):
    return {"tile": (z * 2 + x) * 2 + core, "mem": y}


def greet(peers):
    barrier = pltpu.get_barrier_semaphore()
    for peer in peers:
        pl.semaphore_signal(barrier, inc=1, device_id=peer, device_id_type=MESH)
    pl.semaphore_wait(barrier, len(peers))


def fused_kernel(
    depth, scale, raw, own, interp, stencil, row_loc, level_loc, result,
    blocks, slots, halo, coarse, fine, proj, banded, kron, acc, part,
    near, sums, far, turned, swap_out, swap_in,
    send_raw, recv_raw, send_pair, recv_pair,
    send_a, recv_a, send_x, recv_x, send_y, recv_y, send_h, recv_h,
    send_near, recv_near, send_far, recv_far, send_s, recv_s
):
    z, x, core, y = place()
    f32, bf16 = jnp.float32, jnp.bfloat16
    members, chips = blocks.shape[0], blocks.shape[1]
    columns, rows, levels = fine.shape
    coarse_rows = stencil.shape[1]
    stride = coarse_rows + 8
    kept = acc.shape[0]
    per_side = depth // 2
    count = per_side * 2
    side = lax.div(z, per_side)
    chip = z * 2 + x
    across, beside = target(z, x, core, 1 - y), target(z, 1 - x, core, y)
    partner = target(z, x, 1 - core, y)
    line = [(lax.rem(z + dz, depth), lax.rem(core + dc, 2)) for dz in range(depth) for dc in range(2)]
    greet(
        [target(zz, x, cc, y) for zz, cc in line[1:]]
        + [target(lax.rem(z + dz, depth), 1 - x, core, y) for dz in range(depth)]
        + [across, target(z, 1 - x, core, 1 - y)]
    )

    mine = lax.rem(z, per_side) * 4 + x * 2 + core
    kind = lax.rem(z, per_side) * 2 + core

    def is_self(zz):
        return jnp.logical_and(z == zz, core == side)

    for zz in range(depth):
        @pl.when(jnp.logical_not(is_self(zz)))
        def _():
            pltpu.make_async_remote_copy(
                own.at[y], slots.at[mine, y], send_a.at[zz], recv_a.at[kind],
                target(zz, x, side, y), MESH,
            ).start()

        @pl.when(is_self(zz))
        def _():
            pltpu.make_async_copy(own.at[y], slots.at[mine, y], recv_a.at[kind]).start()

    def raw_copy(m, step):
        to = lax.rem(chip + step, chips)
        return pltpu.make_async_remote_copy(
            raw.at[to * members + m], blocks.at[m, chip, core], send_raw.at[m, step],
            recv_raw.at[m, chip], target(lax.div(to, 2), lax.rem(to, 2), core, y), MESH,
        )

    def send_member(m):
        for step in range(1, chips):
            raw_copy(m, step).start()
        pltpu.make_async_copy(
            raw.at[chip * members + m], blocks.at[m, chip, core], recv_raw.at[m, chip]
        ).start()

    def pair_copy(m):
        held = blocks.at[m, :, core]
        return pltpu.make_async_remote_copy(held, held, send_pair.at[m], recv_pair.at[m], partner, MESH)

    early = min(2, members)
    for m in range(early):
        send_member(m)

    def done(ref, sem):
        pltpu.make_async_copy(ref, ref, sem).wait()

    def forward(slot, send, recv, peer):
        held = slots.at[slot, y]
        pltpu.make_async_remote_copy(held, held, send, recv, peer, MESH).start()

    for k in range(count):
        slot = (k // 2) * 4 + x * 2 + k % 2
        done(slots.at[slot, y], recv_a.at[k])
        forward(slot, send_x.at[k], recv_x.at[k], beside)
        forward(slot, send_y.at[k], recv_y.at[k], across)
    for k in range(count):
        slot = (k // 2) * 4 + (1 - x) * 2 + k % 2
        done(slots.at[slot, y], recv_x.at[k])
        forward(slot, send_y.at[count + k], recv_y.at[count + k], across)
    for m in range(early, members):
        send_member(m)
    for k in range(count):
        done(slots.at[(k // 2) * 4 + x * 2 + k % 2, 1 - y], recv_y.at[k])
    for k in range(count):
        done(slots.at[(k // 2) * 4 + (1 - x) * 2 + k % 2, 1 - y], recv_y.at[count + k])
    edges = pltpu.make_async_remote_copy(
        slots.at[(1 - core) * (2 * count - 1)], halo, send_h, recv_h, partner, MESH
    )
    edges.start()

    acc[...] = jnp.zeros_like(acc)
    tall_at = lax.broadcasted_iota(jnp.int32, (128, 8), 0)
    wide_at = lax.broadcasted_iota(jnp.int32, (128, 24 * GROUP), 1)
    deep_at = lax.broadcasted_iota(jnp.int32, (128, 24 * GROUP), 0)
    spread_rows = (tall_at // GROUP == lax.broadcasted_iota(jnp.int32, (128, 8), 1)).astype(bf16)
    spread_cols = (deep_at == wide_at // GROUP).astype(bf16)
    same = lax.rem(deep_at, GROUP) == lax.rem(wide_at, GROUP)
    for b in range(kept // 8):
        band = slots[b, 0, 4 * rows : 4 * rows + 8, :]
        tall = jnp.dot(spread_rows, band, preferred_element_type=f32).astype(bf16)
        wide = jnp.dot(tall, spread_cols, preferred_element_type=f32)
        kron[b] = jnp.where(same, wide, 0.0).astype(bf16)
    edges.wait()

    partners = [(1 - x, y), (x, 1 - y), (1 - x, 1 - y)]

    def rows_of(yy):
        return pl.ds(pl.multiple_of(yy * (rows // 2), rows // 2), rows // 2)

    def near_copy(k, n):
        xx, yy = partners[n]
        slot = lax.div(k, 2) * 4 + xx * 2 + lax.rem(k, 2)
        return pltpu.make_async_remote_copy(
            part.at[slot, :, rows_of(yy), :], near.at[n, k], send_near.at[n, k],
            recv_near.at[n, k], target(z, xx, core, yy), MESH,
        )

    def send_slot(b):
        k = lax.div(b, 4) * 2 + lax.rem(b, 2)
        inside = lax.rem(lax.div(b, 2), 2) == x

        @pl.when(inside)
        def _():
            near_copy(k, 1).start()

        @pl.when(jnp.logical_not(inside))
        def _():
            near_copy(k, 2).start()
            near_copy(k, 0).start()

    def refine(pair, table):
        base = 2 * pair * stride
        joined = jnp.concatenate(
            [coarse[pl.ds(base + k * stride, coarse_rows), :].astype(bf16) for k in range(2)], axis=1
        )
        fresh = jnp.dot(stencil[...], joined, preferred_element_type=f32).astype(bf16)
        for k in range(2):
            piece = fresh[:, k * levels : (k + 1) * levels]
            j = 2 * pair + k
            fine[j] = piece
            proj[j] = (piece.astype(f32) * table(k).astype(f32)).astype(bf16)

    @pl.loop(0, members)
    def _(m):
        for c in range(chips):
            done(blocks.at[m, c, core], recv_raw.at[m, c])
        copy = pair_copy(m)
        copy.start()
        copy.wait_recv()

        @pl.loop(0, chips)
        def _(c):
            for half in range(2):
                for two in range(2):
                    pair = jnp.concatenate(
                        [blocks[m, c, half, 2 * two], blocks[m, c, half, 2 * two + 1]], axis=1
                    )
                    mixed = jnp.dot(interp[...], pair, preferred_element_type=f32)
                    row = 8 * c + 4 * half + 2 * two
                    for k in range(2):
                        coarse[pl.ds(row + k, columns, stride=stride), :] = mixed[
                            :, k * levels : (k + 1) * levels
                        ]

        for pair in range(4):
            def table(k):
                j = 2 * pair + k
                return halo[j // 4, (j % 4) * rows : (j % 4 + 1) * rows, :]

            refine(pair, table)
            refine(columns // 2 - 4 + pair, table)

        @pl.loop(0, kept // 8)
        def _(b):
            for pair in range(4):
                def table(k):
                    j = 2 * pair + k
                    return slots[b, j // 4, (j % 4) * rows : (j % 4 + 1) * rows, :]

                refine(4 + 4 * b + pair, table)

        @pl.loop(0, kept // 8)
        def _(b):
            for pair in range(rows // (2 * GROUP)):
                parts = []
                for k in range(2):
                    at = (2 * pair + k) * GROUP
                    parts.append(proj[pl.ds(8 * b, 24), at : at + GROUP, :].reshape(24 * GROUP, levels))
                mixed = jnp.dot(
                    kron[b], jnp.concatenate(parts, axis=1), preferred_element_type=f32
                ).astype(bf16)
                for k in range(2):
                    at = (2 * pair + k) * GROUP
                    banded[:, at : at + GROUP, :] = mixed[:, k * levels : (k + 1) * levels].reshape(
                        8, GROUP, levels
                    )
            for pair in range(4):
                joined = jnp.concatenate([banded[2 * pair], banded[2 * pair + 1]], axis=1)
                mixed = jnp.dot(row_loc[...], joined, preferred_element_type=f32).astype(bf16)
                localized = jnp.dot(mixed, level_loc[...], preferred_element_type=f32)
                for k in range(2):
                    j = 8 * b + 2 * pair + k
                    acc[j] += fine[8 + j].astype(f32) * localized[:, k * levels : (k + 1) * levels]

            @pl.when(m == members - 1)
            def _():
                part[b] = acc[pl.ds(8 * b, 8)].astype(bf16)

                @pl.when(b > 0)
                def _():
                    send_slot(b - 1)

    send_slot(kept // 8 - 1)

    for k in range(count):
        for n in range(3):
            near_copy(k, n).wait_recv()
        slot = (k // 2) * 4 + x * 2 + k % 2
        total = acc[pl.ds(8 * slot, 8), rows_of(y), :]
        total = (total + near[0, k].astype(f32)) + (near[1, k].astype(f32) + near[2, k].astype(f32))
        sums[k] = total.astype(bf16)
        owner = per_side * core + k // 2
        to_self = jnp.logical_and(z == owner, core == k % 2)

        @pl.when(jnp.logical_not(to_self))
        def _():
            pltpu.make_async_remote_copy(
                sums.at[k], far.at[z], send_far.at[k], recv_far.at[z],
                target(owner, x, k % 2, y), MESH,
            ).start()

        @pl.when(to_self)
        def _():
            pltpu.make_async_copy(sums.at[k], far.at[z], recv_far.at[z]).start()

    for m in range(members):
        for step in range(1, chips):
            raw_copy(m, step).wait_send()
        pair_copy(m).wait_send()
    for k in range(count):
        done(slots.at[(k // 2) * 4 + x * 2 + k % 2, y], send_x.at[k])
    for k in range(2 * count):
        done(slots.at[k, y], send_y.at[k])
    for zz in range(depth):
        @pl.when(jnp.logical_not(is_self(zz)))
        def _():
            done(own.at[y], send_a.at[zz])

    for zz in range(depth):
        done(far.at[zz], recv_far.at[zz])

    def levels_of(yy):
        return pl.ds(pl.multiple_of(yy * (levels // 2), levels // 2), levels // 2)

    half = rows // 2
    swaps = []
    for pair in range(4):
        pieces = []
        for k in range(2):
            value = far[0, 2 * pair + k].astype(f32)
            for zz in range(1, depth):
                value = value + far[zz, 2 * pair + k].astype(f32)
            pieces.append(value)
        turned[pair] = jnp.concatenate(pieces, axis=0).T
        swap_out[pair] = turned[pair, levels_of(1 - y), :].astype(bf16)
        copy = pltpu.make_async_remote_copy(
            swap_out.at[pair], swap_in.at[pair], send_s.at[pair], recv_s.at[pair], across, MESH
        )
        copy.start()
        swaps.append(copy)
    for pair in range(4):
        swaps[pair].wait_recv()
        held = turned[pair, levels_of(y), :]
        came = swap_in[pair].astype(f32)
        low = jnp.where(y == 0, held, came)
        high = jnp.where(y == 0, came, held)
        for k in range(2):
            at = slice(k * half, (k + 1) * half)
            result[:, 2 * pair + k, :] = jnp.concatenate([low[:, at], high[:, at]], axis=1) * scale
    for copy in swaps:
        copy.wait_send()
    for k in range(count):
        for n in range(3):
            near_copy(k, n).wait_send()
        owner = per_side * core + k // 2

        @pl.when(jnp.logical_not(jnp.logical_and(z == owner, core == k % 2)))
        def _():
            done(sums.at[k], send_far.at[k])


def fused(raw, own, interp, stencil, row_loc, level_loc, depth, scale):
    bf16, f32 = jnp.bfloat16, jnp.float32
    chips = depth * 2
    members = raw.shape[0] // chips
    columns = interp.shape[0]
    rows, coarse_rows = stencil.shape
    levels = row_loc.shape[0]
    kept = columns - 16
    count = depth
    dma = pltpu.SemaphoreType.DMA
    vmem = pl.BlockSpec(memory_space=pltpu.VMEM)
    piece = (8, rows // 2, levels)
    swap = (4, levels // 2, rows)
    flops = 2 * members * levels * rows * columns * (coarse_rows + 24 * GROUP + rows + levels)
    return pl.pallas_call(
        functools.partial(fused_kernel, depth, scale),
        out_shape=jax.ShapeDtypeStruct((levels // 2, 8, rows), f32),
        in_specs=[pl.BlockSpec(memory_space=pl.ANY)] + [vmem] * 5,
        out_specs=vmem,
        scratch_shapes=[
            pltpu.VMEM((members, chips, 2) + raw.shape[1:], bf16),
            pltpu.VMEM((kept // 8,) + own.shape, bf16),
            pltpu.VMEM(own.shape, bf16),
            pltpu.VMEM((columns * (coarse_rows + 8), levels), f32),
            pltpu.VMEM((columns, rows, levels), bf16),
            pltpu.VMEM((columns, rows, levels), bf16),
            pltpu.VMEM((8, rows, levels), bf16),
            pltpu.VMEM((kept // 8, 8 * GROUP, 24 * GROUP), bf16),
            pltpu.VMEM((kept, rows, levels), f32),
            pltpu.VMEM((kept // 8, 8, rows, levels), bf16),
            pltpu.VMEM((3, count) + piece, bf16),
            pltpu.VMEM((count,) + piece, bf16),
            pltpu.VMEM((depth,) + piece, bf16),
            pltpu.VMEM((4, levels, rows), f32),
            pltpu.VMEM(swap, bf16),
            pltpu.VMEM(swap, bf16),
            dma((members, chips)), dma((members, chips)), dma((members,)), dma((members,)),
            dma((depth,)), dma((count,)), dma((count,)), dma((count,)),
            dma((2 * count,)), dma((2 * count,)), dma, dma,
            dma((3, count)), dma((3, count)), dma((count,)), dma((depth,)), dma((4,)), dma((4,)),
        ],
        compiler_params=pltpu.CompilerParams(
            collective_id=0, has_side_effects=True, vmem_limit_bytes=48 * 1024 * 1024
        ),
        cost_estimate=pl.CostEstimate(flops=flops, bytes_accessed=4 * raw.size, transcendentals=0),
    )(raw, own, interp, stencil, row_loc, level_loc)


def member_increment(
    ens_coarse, col_interp, row_weights, ctrl_vec, band_loc, row_loc, level_loc, total_members
):
    bf16 = jnp.bfloat16
    tiles = lax.axis_size("tile")
    core = lax.rem(lax.axis_index("tile"), 2)
    columns = band_loc.shape[0]
    fine_rows = row_weights.shape[1]
    levels = level_loc.shape[0]
    own = jnp.transpose(ctrl_vec[0], (1, 2, 0)).astype(bf16).reshape(2, columns // 2 * fine_rows, levels)
    band = jnp.pad(band_loc, ((0, 16 - columns), (0, levels - band_loc.shape[1])))
    own = jnp.concatenate([own, jnp.broadcast_to(band, (2,) + band.shape)], axis=1)
    stencil = row_matrix(row_weights, fine_rows, fine_rows // 2)
    kept = columns * tiles // 2
    padded = jnp.pad(col_interp, ((columns, columns), (0, 0)))
    interp = lax.dynamic_slice_in_dim(padded, core * kept, kept + 2 * columns, 0)
    mixing = jnp.kron(jnp.eye(2, dtype=bf16), level_loc.T)
    raw = jnp.transpose(ens_coarse[0], (0, 2, 3, 1))
    return fused(raw, own, interp, stencil, row_loc, mixing, tiles // 4, 1.0 / (total_members - 1))


def fits(mesh_sizes, members, columns, block_rows, fine_rows, levels):
    tiles = mesh_sizes["tile"]
    return (
        mesh_sizes["grp"] == 1
        and mesh_sizes["mem"] == 2
        and tiles % 8 == 0
        and members % (tiles // 2) == 0
        and columns == 8
        and block_rows == 4
        and fine_rows == 128
        and levels == 128
    )


def body(
    ens_coarse,
    col_interp,
    row_weights,
    ctrl_vec,
    band_loc,
    row_loc,
    level_loc,
    hx_pert,
    innov,
    obs_prec,
    obs_region,
):
    total_members = hx_pert.shape[1]
    observed = hx_pert[0]
    weighted = (observed * obs_prec[0][None, :]).astype(jnp.bfloat16)
    labels = lax.broadcasted_iota(jnp.int32, (NREG, observed.shape[1]), 0)
    member_of = obs_region[0][None, :] == labels
    masked = jnp.where(member_of[:, None, :], weighted[None], jnp.zeros((), jnp.bfloat16))
    gram_sums = jnp.einsum("rko,jo->rkj", masked, observed, preferred_element_type=jnp.float32)
    innov_rows = jnp.where(member_of, innov[0][None, :], 0.0)
    right_side = jnp.dot(
        innov_rows, weighted.astype(jnp.float32).T, precision=lax.Precision.HIGHEST
    )
    sums = jnp.concatenate([gram_sums, right_side[:, :, None]], axis=2)
    sums = swap_add(lax.psum(sums, "grp") if lax.axis_size("grp") > 1 else sums)
    sizes = {axis: lax.axis_size(axis) for axis in ("grp", "tile", "mem")}
    plan = plain_increment
    if fits(
        sizes, ens_coarse.shape[1], band_loc.shape[0], ens_coarse.shape[3], row_loc.shape[0], level_loc.shape[0]
    ):
        plan = member_increment
    increment = plan(
        ens_coarse, col_interp, row_weights, ctrl_vec, band_loc, row_loc, level_loc, total_members
    )
    own_weights = solve_weights(sums)
    weights = collect(own_weights)
    return (increment[None], weights)


def solution(mesh):
    placed = (
        P("grp", "mem", None, "tile", None),
        P(),
        P(),
        P("grp", None, "tile", None),
        P("tile", None),
        P(),
        P(),
        P("grp", None, ("tile", "mem")),
        P("grp", ("tile", "mem")),
        P("grp", ("tile", "mem")),
        P("grp", ("tile", "mem")),
    )
    return jax.shard_map(
        body,
        mesh=mesh,
        in_specs=placed,
        out_specs=(P("grp", "mem", "tile", None), P("tile", None)),
        check_vma=False,
    )
```

```python
import functools

import jax
import jax.numpy as jnp
from jax import lax
from jax.experimental import pallas as pl
from jax.experimental.pallas import tpu as pltpu
from jax.sharding import PartitionSpec as P

NREG = 8
GROUP = 16
MESH = pl.DeviceIdType.MESH


def extended(value, sides, width):
    for axis, dim in sides:
        peers, length = (lax.axis_size(axis), value.shape[dim])
        up = [(i, (i + 1) % peers) for i in range(peers - 1)]
        down = [(j, i) for i, j in up]
        last = lax.slice_in_dim(value, length - width, length, axis=dim)
        first = lax.slice_in_dim(value, 0, width, axis=dim)
        before = lax.ppermute(last, axis, up)
        after = lax.ppermute(first, axis, down)
        value = jnp.concatenate([before, value, after], axis=dim)
    return value


def swap_add(value):
    peers = lax.axis_size("mem")
    me = lax.axis_index("mem")
    length = value.shape[0] // peers
    total = lax.dynamic_slice_in_dim(value, me * length, length, 0)
    for shift in range(1, peers):
        other = lax.rem(me + shift, peers)
        part = lax.dynamic_slice_in_dim(value, other * length, length, 0)
        pairs = [(i, (i + shift) % peers) for i in range(peers)]
        total = total + lax.ppermute(part, "mem", pairs)
    return total


def collect(value):
    peers = lax.axis_size("mem")
    me = lax.axis_index("mem")
    length = value.shape[0]
    result = jnp.zeros((peers * length,) + value.shape[1:], value.dtype)
    result = lax.dynamic_update_slice_in_dim(result, value, me * length, 0)
    for shift in range(1, peers):
        pairs = [(i, (i + shift) % peers) for i in range(peers)]
        moved = lax.ppermute(value, "mem", pairs)
        source = lax.rem(me + peers - shift, peers)
        result = lax.dynamic_update_slice_in_dim(result, moved, source * length, 0)
    return result


def row_matrix(row_weights, fine_rows, coarse_rows):
    fine_index = lax.broadcasted_iota(jnp.int32, (fine_rows, coarse_rows), 0)
    coarse_index = lax.broadcasted_iota(jnp.int32, (fine_rows, coarse_rows), 1)
    weights = row_weights.astype(jnp.float32)
    stencil = jnp.zeros((fine_rows, coarse_rows), jnp.float32)
    for offset in range(3):
        matched = coarse_index == fine_index // 2 + offset - 1
        stencil = stencil + jnp.where(matched, weights[offset][:, None], 0.0)
    return stencil.astype(jnp.bfloat16)


def eliminate(tables):
    members, lanes = tables[0].shape
    row_index = lax.broadcasted_iota(jnp.int32, (members, lanes), 0)
    col_index = lax.broadcasted_iota(jnp.int32, (members, lanes), 1)
    filler = jnp.zeros((lanes - members, lanes), jnp.float32)
    systems = []
    for table in tables:
        mirrored = jnp.concatenate([table, filler], axis=0).T[:members]
        table = jnp.where(col_index < members, 0.5 * (table + mirrored), table)
        systems.append(table + jnp.where(row_index == col_index, float(members - 1), 0.0))
    for k in range(members):
        for region, table in enumerate(systems):
            row = table[k : k + 1]
            row = row / row[:, k : k + 1]
            column = table[:, k : k + 1] - jnp.where(row_index[:, :1] == k, 1.0, 0.0)
            systems[region] = table - column * row
    return [jnp.concatenate([table, filler], axis=0).T[members : members + 8] for table in systems]


def solve_kernel(sums, result):
    for region, rows in enumerate(eliminate([sums[r] for r in range(sums.shape[0])])):
        result[region] = rows


def solve_weights(sums):
    regions, members, width = sums.shape
    lanes = 128 * (-(-(members + 8) // 128))
    padded = jnp.pad(sums, ((0, 0), (0, 0), (0, lanes - width)))
    result = pl.pallas_call(
        solve_kernel,
        out_shape=jax.ShapeDtypeStruct((regions, 8, lanes), jnp.float32),
        in_specs=[pl.BlockSpec(memory_space=pltpu.VMEM)],
        out_specs=pl.BlockSpec(memory_space=pltpu.VMEM),
        cost_estimate=pl.CostEstimate(flops=10**9, bytes_accessed=4 * padded.size, transcendentals=0),
    )(padded)
    return result[:, 0, :members]


def plain_increment(
    ens_coarse, col_interp, row_weights, ctrl_vec, band_loc, row_loc, level_loc, total_members
):
    fine_rows = row_weights.shape[1]
    columns = band_loc.shape[0]
    coarse_cols = jnp.einsum(
        "tklic,jc->tklij", ens_coarse, col_interp, preferred_element_type=jnp.float32
    ).astype(jnp.bfloat16)
    stencil = row_matrix(row_weights, fine_rows, fine_rows // 2)
    refined = jnp.einsum(
        "tklij,ri->tkljr",
        lax.all_to_all(coarse_cols, "tile", split_axis=4, concat_axis=3, tiled=True),
        stencil,
        preferred_element_type=jnp.float32,
    ).astype(jnp.bfloat16)
    member_fine = refined[0]
    slot_term = member_fine * ctrl_vec[0][None]
    projected = slot_term.astype(jnp.bfloat16)
    if lax.axis_size("grp") > 1:
        projected = lax.psum(projected, "grp")
    padded = extended(projected, (("tile", 2),), columns)
    banded = jnp.einsum(
        "jq,klqr->kljr", band_loc, padded, preferred_element_type=jnp.float32
    ).astype(jnp.bfloat16)
    row_mixed = jnp.einsum(
        "kljs,rs->kljr", banded, row_loc, preferred_element_type=jnp.float32
    ).astype(jnp.bfloat16)
    localized = jnp.einsum(
        "lm,kmjr->kljr", level_loc, row_mixed, preferred_element_type=jnp.float32
    ).astype(jnp.bfloat16)
    return swap_add(
        jnp.sum(member_fine.astype(jnp.float32) * localized.astype(jnp.float32), axis=0)
    ) / (total_members - 1)


def place():
    tile = lax.axis_index("tile")
    core = lax.rem(tile, 2)
    chip = lax.div(tile, 2)
    return lax.div(chip, 2), lax.rem(chip, 2), core, lax.axis_index("mem")


def target(z, x, core, y):
    return {"tile": (z * 2 + x) * 2 + core, "mem": y}


def greet(peers):
    barrier = pltpu.get_barrier_semaphore()
    for peer in peers:
        pl.semaphore_signal(barrier, inc=1, device_id=peer, device_id_type=MESH)
    pl.semaphore_wait(barrier, len(peers))


def fused_kernel(
    depth, scale, raw, *refs
):
    sources, refs = refs[:10], refs[10:]
    outputs, places, refs = refs[:2], refs[2:12], refs[12:]
    loads, refs = refs[0], refs[1:]
    copies = [
        pltpu.make_async_copy(source, place_in, loads.at[n])
        for n, (source, place_in) in enumerate(zip(sources, places))
    ]
    for copy in copies:
        copy.start()
    fused_steps(depth, scale, raw, copies, *places, *outputs, *refs)


def fused_steps(
    depth, scale, raw, copies, ctrl, band_in, columns_in, row_weights, row_loc, levels_in,
    observed, innov, precision, region, result, weights,
    own, interp, stencil, level_loc, shifted, gram, gram_in, solved, solved_in,
    blocks, slots, halo, coarse, fine, proj, banded, kron, acc, part,
    near, sums, far, turned, swap_out, swap_in,
    send_raw, recv_raw, send_pair, recv_pair,
    send_a, recv_a, send_x, recv_x, send_y, recv_y, send_h, recv_h,
    send_near, recv_near, send_far, recv_far, send_s, recv_s,
    send_g, recv_g, send_w, recv_w
):
    z, x, core, y = place()
    f32, bf16 = jnp.float32, jnp.bfloat16
    members, chips = blocks.shape[0], blocks.shape[1]
    columns, rows, levels = fine.shape
    coarse_rows = stencil.shape[1]
    stride = coarse_rows + 8
    kept = acc.shape[0]
    per_side = depth // 2
    count = per_side * 2
    side = lax.div(z, per_side)
    chip = z * 2 + x
    across, beside = target(z, x, core, 1 - y), target(z, 1 - x, core, y)
    partner = target(z, x, 1 - core, y)
    copies[0].wait()
    for j in range(8):
        own[j // 4, (j % 4) * rows : (j % 4 + 1) * rows, :] = ctrl[:, j, :].T.astype(bf16)
    copies[1].wait()
    window = band_in.shape[1]
    widen = (
        lax.broadcasted_iota(jnp.int32, (window, levels), 0)
        == lax.broadcasted_iota(jnp.int32, (window, levels), 1)
    ).astype(bf16)
    band_rows = jnp.dot(band_in[...], widen, preferred_element_type=f32)
    band_rows = jnp.concatenate([band_rows, jnp.zeros_like(band_rows)], axis=0).astype(bf16)
    for h in range(2):
        own[h, 4 * rows : 4 * rows + 16, :] = band_rows
    line = [(lax.rem(z + dz, depth), lax.rem(core + dc, 2)) for dz in range(depth) for dc in range(2)]
    greet(
        [target(zz, x, cc, y) for zz, cc in line[1:]]
        + [target(lax.rem(z + dz, depth), 1 - x, core, y) for dz in range(depth)]
        + [across, target(z, 1 - x, core, 1 - y)]
    )

    mine = lax.rem(z, per_side) * 4 + x * 2 + core
    kind = lax.rem(z, per_side) * 2 + core

    def is_self(zz):
        return jnp.logical_and(z == zz, core == side)

    for zz in range(depth):
        @pl.when(jnp.logical_not(is_self(zz)))
        def _():
            pltpu.make_async_remote_copy(
                own.at[y], slots.at[mine, y], send_a.at[zz], recv_a.at[kind],
                target(zz, x, side, y), MESH,
            ).start()

        @pl.when(is_self(zz))
        def _():
            pltpu.make_async_copy(own.at[y], slots.at[mine, y], recv_a.at[kind]).start()

    def raw_copy(m, step):
        to = lax.rem(chip + step, chips)
        return pltpu.make_async_remote_copy(
            raw.at[to * members + m], blocks.at[m, chip, core], send_raw.at[m, step],
            recv_raw.at[m, chip], target(lax.div(to, 2), lax.rem(to, 2), core, y), MESH,
        )

    def send_member(m):
        for step in range(1, chips):
            raw_copy(m, step).start()
        pltpu.make_async_copy(
            raw.at[chip * members + m], blocks.at[m, chip, core], recv_raw.at[m, chip]
        ).start()

    def pair_copy(m):
        held = blocks.at[m, :, core]
        return pltpu.make_async_remote_copy(held, held, send_pair.at[m], recv_pair.at[m], partner, MESH)

    early = min(2, members)
    for m in range(early):
        send_member(m)

    def done(ref, sem):
        pltpu.make_async_copy(ref, ref, sem).wait()

    for copy in copies[2:]:
        copy.wait()
    people, spots = observed.shape
    hx = observed[...]
    weighted = (hx.astype(f32) * precision[...]).astype(bf16).astype(f32)
    rest = innov[...]
    thirds = jnp.zeros((48, spots), f32)
    third_at = lax.broadcasted_iota(jnp.int32, (48, spots), 0)
    for n in range(3):
        third = rest.astype(bf16).astype(f32)
        thirds = jnp.where(third_at == n, third, thirds)
        rest = rest - third
    right = jnp.concatenate([hx, thirds.astype(bf16)], axis=0)
    for g in range(NREG):
        masked = jnp.where(region[...] == g, weighted, 0.0).astype(bf16)
        gram[g] = lax.dot_general(
            masked, right, (((1,), (1,)), ((), ())), preferred_element_type=f32
        )
    per_half = NREG // 2
    grams = pltpu.make_async_remote_copy(
        gram.at[pl.ds((1 - y) * per_half, per_half)], gram_in, send_g, recv_g, across, MESH
    )
    grams.start()

    coarse_width = columns_in.shape[0]
    fill = jnp.zeros((levels - coarse_width, levels), f32)
    shifted[...] = jnp.zeros_like(shifted)
    shifted[8 : 8 + levels, :] = jnp.concatenate([columns_in[...].astype(f32), fill], axis=0).T
    interp[...] = shifted[pl.ds(pl.multiple_of(core * kept, 8), columns), :][:, :coarse_width].astype(bf16)
    coarse_at = lax.broadcasted_iota(jnp.int32, (coarse_rows, rows), 0)
    parent_at = lax.broadcasted_iota(jnp.int32, (coarse_rows, rows), 1) // 2
    spreading = jnp.zeros((coarse_rows, rows), f32)
    for n in range(3):
        spreading = spreading + jnp.where(
            coarse_at == parent_at + n - 1, row_weights[n : n + 1, :].astype(f32), 0.0
        )
    stencil[...] = jnp.concatenate([spreading, fill], axis=0).T[:, :coarse_rows].astype(bf16)
    flipped = levels_in[...].astype(f32).T.astype(bf16)
    level_loc[...] = jnp.zeros_like(level_loc)
    level_loc[:levels, :levels] = flipped
    level_loc[levels:, levels:] = flipped

    def forward(slot, send, recv, peer):
        held = slots.at[slot, y]
        pltpu.make_async_remote_copy(held, held, send, recv, peer, MESH).start()

    for k in range(count):
        slot = (k // 2) * 4 + x * 2 + k % 2
        done(slots.at[slot, y], recv_a.at[k])
        forward(slot, send_x.at[k], recv_x.at[k], beside)
        forward(slot, send_y.at[k], recv_y.at[k], across)
    for k in range(count):
        slot = (k // 2) * 4 + (1 - x) * 2 + k % 2
        done(slots.at[slot, y], recv_x.at[k])
        forward(slot, send_y.at[count + k], recv_y.at[count + k], across)
    for m in range(early, members):
        send_member(m)
    grams.wait_recv()
    answers = eliminate([gram[y * per_half + g] + gram_in[g] for g in range(per_half)])
    for g, rows_solved in enumerate(answers):
        solved[g : g + 1, :] = rows_solved[0:1] + rows_solved[1:2] + rows_solved[2:3]
    solved[per_half:, :] = jnp.zeros_like(solved[per_half:, :])
    for k in range(count):
        done(slots.at[(k // 2) * 4 + x * 2 + k % 2, 1 - y], recv_y.at[k])
    for k in range(count):
        done(slots.at[(k // 2) * 4 + (1 - x) * 2 + k % 2, 1 - y], recv_y.at[count + k])
    edges = pltpu.make_async_remote_copy(
        slots.at[(1 - core) * (2 * count - 1)], halo, send_h, recv_h, partner, MESH
    )
    edges.start()

    acc[...] = jnp.zeros_like(acc)
    tall_at = lax.broadcasted_iota(jnp.int32, (128, 8), 0)
    wide_at = lax.broadcasted_iota(jnp.int32, (128, 24 * GROUP), 1)
    deep_at = lax.broadcasted_iota(jnp.int32, (128, 24 * GROUP), 0)
    spread_rows = (tall_at // GROUP == lax.broadcasted_iota(jnp.int32, (128, 8), 1)).astype(bf16)
    spread_cols = (deep_at == wide_at // GROUP).astype(bf16)
    same = lax.rem(deep_at, GROUP) == lax.rem(wide_at, GROUP)
    for b in range(kept // 8):
        band = slots[b, 0, 4 * rows : 4 * rows + 8, :]
        tall = jnp.dot(spread_rows, band, preferred_element_type=f32).astype(bf16)
        wide = jnp.dot(tall, spread_cols, preferred_element_type=f32)
        kron[b] = jnp.where(same, wide, 0.0).astype(bf16)
    edges.wait()
    answer = pltpu.make_async_remote_copy(solved, solved_in, send_w, recv_w, across, MESH)
    answer.start()

    partners = [(1 - x, y), (x, 1 - y), (1 - x, 1 - y)]

    def rows_of(yy):
        return pl.ds(pl.multiple_of(yy * (rows // 2), rows // 2), rows // 2)

    def near_copy(k, n):
        xx, yy = partners[n]
        slot = lax.div(k, 2) * 4 + xx * 2 + lax.rem(k, 2)
        return pltpu.make_async_remote_copy(
            part.at[slot, :, rows_of(yy), :], near.at[n, k], send_near.at[n, k],
            recv_near.at[n, k], target(z, xx, core, yy), MESH,
        )

    def send_slot(b):
        k = lax.div(b, 4) * 2 + lax.rem(b, 2)
        inside = lax.rem(lax.div(b, 2), 2) == x

        @pl.when(inside)
        def _():
            near_copy(k, 1).start()

        @pl.when(jnp.logical_not(inside))
        def _():
            near_copy(k, 2).start()
            near_copy(k, 0).start()

    def refine(pair, table):
        base = 2 * pair * stride
        joined = jnp.concatenate(
            [coarse[pl.ds(base + k * stride, coarse_rows), :].astype(bf16) for k in range(2)], axis=1
        )
        fresh = jnp.dot(stencil[...], joined, preferred_element_type=f32).astype(bf16)
        for k in range(2):
            piece = fresh[:, k * levels : (k + 1) * levels]
            j = 2 * pair + k
            fine[j] = piece
            proj[j] = (piece.astype(f32) * table(k).astype(f32)).astype(bf16)

    @pl.loop(0, members)
    def _(m):
        for c in range(chips):
            done(blocks.at[m, c, core], recv_raw.at[m, c])
        copy = pair_copy(m)
        copy.start()
        copy.wait_recv()

        @pl.loop(0, chips)
        def _(c):
            for half in range(2):
                for two in range(2):
                    pair = jnp.concatenate(
                        [blocks[m, c, half, 2 * two], blocks[m, c, half, 2 * two + 1]], axis=1
                    )
                    mixed = jnp.dot(interp[...], pair, preferred_element_type=f32)
                    row = 8 * c + 4 * half + 2 * two
                    for k in range(2):
                        coarse[pl.ds(row + k, columns, stride=stride), :] = mixed[
                            :, k * levels : (k + 1) * levels
                        ]

        for pair in range(4):
            def table(k):
                j = 2 * pair + k
                return halo[j // 4, (j % 4) * rows : (j % 4 + 1) * rows, :]

            refine(pair, table)
            refine(columns // 2 - 4 + pair, table)

        @pl.loop(0, kept // 8)
        def _(b):
            for pair in range(4):
                def table(k):
                    j = 2 * pair + k
                    return slots[b, j // 4, (j % 4) * rows : (j % 4 + 1) * rows, :]

                refine(4 + 4 * b + pair, table)

        @pl.loop(0, kept // 8)
        def _(b):
            for pair in range(rows // (2 * GROUP)):
                parts = []
                for k in range(2):
                    at = (2 * pair + k) * GROUP
                    parts.append(proj[pl.ds(8 * b, 24), at : at + GROUP, :].reshape(24 * GROUP, levels))
                mixed = jnp.dot(
                    kron[b], jnp.concatenate(parts, axis=1), preferred_element_type=f32
                ).astype(bf16)
                for k in range(2):
                    at = (2 * pair + k) * GROUP
                    banded[:, at : at + GROUP, :] = mixed[:, k * levels : (k + 1) * levels].reshape(
                        8, GROUP, levels
                    )
            for pair in range(4):
                joined = jnp.concatenate([banded[2 * pair], banded[2 * pair + 1]], axis=1)
                mixed = jnp.dot(row_loc[...], joined, preferred_element_type=f32).astype(bf16)
                localized = jnp.dot(mixed, level_loc[...], preferred_element_type=f32)
                for k in range(2):
                    j = 8 * b + 2 * pair + k
                    acc[j] += fine[8 + j].astype(f32) * localized[:, k * levels : (k + 1) * levels]

            @pl.when(m == members - 1)
            def _():
                part[b] = acc[pl.ds(8 * b, 8)].astype(bf16)

                @pl.when(b > 0)
                def _():
                    send_slot(b - 1)

    send_slot(kept // 8 - 1)

    for k in range(count):
        for n in range(3):
            near_copy(k, n).wait_recv()
        slot = (k // 2) * 4 + x * 2 + k % 2
        total = acc[pl.ds(8 * slot, 8), rows_of(y), :]
        total = (total + near[0, k].astype(f32)) + (near[1, k].astype(f32) + near[2, k].astype(f32))
        sums[k] = total.astype(bf16)
        owner = per_side * core + k // 2
        to_self = jnp.logical_and(z == owner, core == k % 2)

        @pl.when(jnp.logical_not(to_self))
        def _():
            pltpu.make_async_remote_copy(
                sums.at[k], far.at[z], send_far.at[k], recv_far.at[z],
                target(owner, x, k % 2, y), MESH,
            ).start()

        @pl.when(to_self)
        def _():
            pltpu.make_async_copy(sums.at[k], far.at[z], recv_far.at[z]).start()

    answer.wait()
    held, came = solved[:per_half, :people], solved_in[:per_half, :people]
    weights[:per_half, :] = jnp.where(y == 0, held, came)
    weights[per_half:, :] = jnp.where(y == 0, came, held)
    grams.wait_send()
    for m in range(members):
        for step in range(1, chips):
            raw_copy(m, step).wait_send()
        pair_copy(m).wait_send()
    for k in range(count):
        done(slots.at[(k // 2) * 4 + x * 2 + k % 2, y], send_x.at[k])
    for k in range(2 * count):
        done(slots.at[k, y], send_y.at[k])
    for zz in range(depth):
        @pl.when(jnp.logical_not(is_self(zz)))
        def _():
            done(own.at[y], send_a.at[zz])

    for zz in range(depth):
        done(far.at[zz], recv_far.at[zz])

    def levels_of(yy):
        return pl.ds(pl.multiple_of(yy * (levels // 2), levels // 2), levels // 2)

    half = rows // 2
    swaps = []
    for pair in range(4):
        pieces = []
        for k in range(2):
            value = far[0, 2 * pair + k].astype(f32)
            for zz in range(1, depth):
                value = value + far[zz, 2 * pair + k].astype(f32)
            pieces.append(value)
        turned[pair] = jnp.concatenate(pieces, axis=0).T
        swap_out[pair] = turned[pair, levels_of(1 - y), :].astype(bf16)
        copy = pltpu.make_async_remote_copy(
            swap_out.at[pair], swap_in.at[pair], send_s.at[pair], recv_s.at[pair], across, MESH
        )
        copy.start()
        swaps.append(copy)
    for pair in range(4):
        swaps[pair].wait_recv()
        held = turned[pair, levels_of(y), :]
        came = swap_in[pair].astype(f32)
        low = jnp.where(y == 0, held, came)
        high = jnp.where(y == 0, came, held)
        for k in range(2):
            at = slice(k * half, (k + 1) * half)
            result[:, 2 * pair + k, :] = jnp.concatenate([low[:, at], high[:, at]], axis=1) * scale
    for copy in swaps:
        copy.wait_send()
    for k in range(count):
        for n in range(3):
            near_copy(k, n).wait_send()
        owner = per_side * core + k // 2

        @pl.when(jnp.logical_not(jnp.logical_and(z == owner, core == k % 2)))
        def _():
            done(sums.at[k], send_far.at[k])


def fused(
    raw, ctrl, band, columns_in, row_weights, row_loc, level_loc, observed, innov, precision, region,
    depth, scale
):
    bf16, f32 = jnp.bfloat16, jnp.float32
    chips = depth * 2
    members = raw.shape[0] // chips
    columns = 8 * chips + 16
    coarse_rows, rows = row_weights.shape[1] // 2, row_weights.shape[1]
    levels = row_loc.shape[0]
    people = observed.shape[0]
    kept = columns - 16
    count = depth
    loaded = (
        ctrl, band, columns_in, row_weights, row_loc, level_loc, observed, innov, precision, region
    )
    dma = pltpu.SemaphoreType.DMA
    vmem = pl.BlockSpec(memory_space=pltpu.VMEM)
    own = jax.ShapeDtypeStruct((2, 4 * rows + 16, levels), bf16)
    piece = (8, rows // 2, levels)
    swap = (4, levels // 2, rows)
    flops = 2 * members * levels * rows * columns * (coarse_rows + 24 * GROUP + rows + levels)
    return pl.pallas_call(
        functools.partial(fused_kernel, depth, scale),
        out_shape=(
            jax.ShapeDtypeStruct((levels // 2, 8, rows), f32),
            jax.ShapeDtypeStruct((NREG, people), f32),
        ),
        in_specs=[pl.BlockSpec(memory_space=pltpu.HBM)] * 11,
        out_specs=(vmem, vmem),
        scratch_shapes=[
            *[pltpu.VMEM(value.shape, value.dtype) for value in loaded],
            dma((len(loaded),)),
            pltpu.VMEM(own.shape, bf16),
            pltpu.VMEM((columns, raw.shape[2]), bf16),
            pltpu.VMEM((rows, coarse_rows), bf16),
            pltpu.VMEM((2 * levels, 2 * levels), bf16),
            pltpu.VMEM((2 * kept + 16, levels), f32),
            pltpu.VMEM((NREG, people, 128), f32),
            pltpu.VMEM((NREG // 2, people, 128), f32),
            pltpu.VMEM((8, 128), f32),
            pltpu.VMEM((8, 128), f32),
            pltpu.VMEM((members, chips, 2) + raw.shape[1:], bf16),
            pltpu.VMEM((kept // 8,) + own.shape, bf16),
            pltpu.VMEM(own.shape, bf16),
            pltpu.VMEM((columns * (coarse_rows + 8), levels), f32),
            pltpu.VMEM((columns, rows, levels), bf16),
            pltpu.VMEM((columns, rows, levels), bf16),
            pltpu.VMEM((8, rows, levels), bf16),
            pltpu.VMEM((kept // 8, 8 * GROUP, 24 * GROUP), bf16),
            pltpu.VMEM((kept, rows, levels), f32),
            pltpu.VMEM((kept // 8, 8, rows, levels), bf16),
            pltpu.VMEM((3, count) + piece, bf16),
            pltpu.VMEM((count,) + piece, bf16),
            pltpu.VMEM((depth,) + piece, bf16),
            pltpu.VMEM((4, levels, rows), f32),
            pltpu.VMEM(swap, bf16),
            pltpu.VMEM(swap, bf16),
            dma((members, chips)), dma((members, chips)), dma((members,)), dma((members,)),
            dma((depth,)), dma((count,)), dma((count,)), dma((count,)),
            dma((2 * count,)), dma((2 * count,)), dma, dma,
            dma((3, count)), dma((3, count)), dma((count,)), dma((depth,)), dma((4,)), dma((4,)),
            dma, dma, dma, dma,
        ],
        compiler_params=pltpu.CompilerParams(
            collective_id=0, has_side_effects=True, vmem_limit_bytes=48 * 1024 * 1024
        ),
        cost_estimate=pl.CostEstimate(flops=flops, bytes_accessed=4 * raw.size, transcendentals=0),
    )(raw, *loaded)


def member_plan(
    ens_coarse,
    col_interp,
    row_weights,
    ctrl_vec,
    band_loc,
    row_loc,
    level_loc,
    hx_pert,
    innov,
    obs_prec,
    obs_region,
):
    raw = jnp.transpose(ens_coarse[0], (0, 2, 3, 1))
    increment, weights = fused(
        raw, ctrl_vec[0], band_loc, col_interp.T, row_weights, row_loc, level_loc,
        hx_pert[0], innov, obs_prec, obs_region,
        lax.axis_size("tile") // 4, 1.0 / (hx_pert.shape[1] - 1),
    )
    return (increment[None], weights)


def fits(mesh_sizes, total_members, block, columns, fine_rows, levels):
    tiles = mesh_sizes["tile"]
    members, block_rows, width = block[1], block[3], block[4]
    return (
        mesh_sizes["grp"] == 1
        and mesh_sizes["mem"] == 2
        and tiles % 8 == 0
        and members % (tiles // 2) == 0
        and tiles * columns == levels
        and width <= levels
        and total_members % 8 == 0
        and total_members + 48 == levels
        and columns == 8
        and block_rows == 4
        and fine_rows == 128
        and levels == 128
    )


def body(
    ens_coarse,
    col_interp,
    row_weights,
    ctrl_vec,
    band_loc,
    row_loc,
    level_loc,
    hx_pert,
    innov,
    obs_prec,
    obs_region,
):
    sizes = {axis: lax.axis_size(axis) for axis in ("grp", "tile", "mem")}
    total_members = hx_pert.shape[1]
    if fits(sizes, total_members, ens_coarse.shape, band_loc.shape[0], row_loc.shape[0], level_loc.shape[0]):
        return member_plan(
            ens_coarse, col_interp, row_weights, ctrl_vec, band_loc, row_loc, level_loc,
            hx_pert, innov, obs_prec, obs_region,
        )
    observed = hx_pert[0]
    weighted = (observed * obs_prec[0][None, :]).astype(jnp.bfloat16)
    labels = lax.broadcasted_iota(jnp.int32, (NREG, observed.shape[1]), 0)
    member_of = obs_region[0][None, :] == labels
    masked = jnp.where(member_of[:, None, :], weighted[None], jnp.zeros((), jnp.bfloat16))
    gram_sums = jnp.einsum("rko,jo->rkj", masked, observed, preferred_element_type=jnp.float32)
    innov_rows = jnp.where(member_of, innov[0][None, :], 0.0)
    right_side = jnp.dot(
        innov_rows, weighted.astype(jnp.float32).T, precision=lax.Precision.HIGHEST
    )
    sums = jnp.concatenate([gram_sums, right_side[:, :, None]], axis=2)
    sums = swap_add(lax.psum(sums, "grp") if lax.axis_size("grp") > 1 else sums)
    increment = plain_increment(
        ens_coarse, col_interp, row_weights, ctrl_vec, band_loc, row_loc, level_loc, total_members
    )
    own_weights = solve_weights(sums)
    weights = collect(own_weights)
    return (increment[None], weights)


def solution(mesh):
    placed = (
        P("grp", "mem", None, "tile", None),
        P(),
        P(),
        P("grp", None, "tile", None),
        P("tile", None),
        P(),
        P(),
        P("grp", None, ("tile", "mem")),
        P("grp", ("tile", "mem")),
        P("grp", ("tile", "mem")),
        P("grp", ("tile", "mem")),
    )
    return jax.shard_map(
        body,
        mesh=mesh,
        in_specs=placed,
        out_specs=(P("grp", "mem", "tile", None), P("tile", None)),
        check_vma=False,
    )
```

```python
import functools

import jax
import jax.numpy as jnp
from jax import lax
from jax.experimental import pallas as pl
from jax.experimental.pallas import tpu as pltpu
from jax.sharding import PartitionSpec as P

NREG = 8
GROUP = 16
MESH = pl.DeviceIdType.MESH


def extended(value, sides, width):
    for axis, dim in sides:
        peers, length = (lax.axis_size(axis), value.shape[dim])
        up = [(i, (i + 1) % peers) for i in range(peers - 1)]
        down = [(j, i) for i, j in up]
        last = lax.slice_in_dim(value, length - width, length, axis=dim)
        first = lax.slice_in_dim(value, 0, width, axis=dim)
        before = lax.ppermute(last, axis, up)
        after = lax.ppermute(first, axis, down)
        value = jnp.concatenate([before, value, after], axis=dim)
    return value


def swap_add(value):
    peers = lax.axis_size("mem")
    me = lax.axis_index("mem")
    length = value.shape[0] // peers
    total = lax.dynamic_slice_in_dim(value, me * length, length, 0)
    for shift in range(1, peers):
        other = lax.rem(me + shift, peers)
        part = lax.dynamic_slice_in_dim(value, other * length, length, 0)
        pairs = [(i, (i + shift) % peers) for i in range(peers)]
        total = total + lax.ppermute(part, "mem", pairs)
    return total


def collect(value):
    peers = lax.axis_size("mem")
    me = lax.axis_index("mem")
    length = value.shape[0]
    result = jnp.zeros((peers * length,) + value.shape[1:], value.dtype)
    result = lax.dynamic_update_slice_in_dim(result, value, me * length, 0)
    for shift in range(1, peers):
        pairs = [(i, (i + shift) % peers) for i in range(peers)]
        moved = lax.ppermute(value, "mem", pairs)
        source = lax.rem(me + peers - shift, peers)
        result = lax.dynamic_update_slice_in_dim(result, moved, source * length, 0)
    return result


def row_matrix(row_weights, fine_rows, coarse_rows):
    fine_index = lax.broadcasted_iota(jnp.int32, (fine_rows, coarse_rows), 0)
    coarse_index = lax.broadcasted_iota(jnp.int32, (fine_rows, coarse_rows), 1)
    weights = row_weights.astype(jnp.float32)
    stencil = jnp.zeros((fine_rows, coarse_rows), jnp.float32)
    for offset in range(3):
        matched = coarse_index == fine_index // 2 + offset - 1
        stencil = stencil + jnp.where(matched, weights[offset][:, None], 0.0)
    return stencil.astype(jnp.bfloat16)


def eliminate(tables):
    members, lanes = tables[0].shape
    row_index = lax.broadcasted_iota(jnp.int32, (members, lanes), 0)
    col_index = lax.broadcasted_iota(jnp.int32, (members, lanes), 1)
    filler = jnp.zeros((lanes - members, lanes), jnp.float32)
    systems = []
    for table in tables:
        mirrored = jnp.concatenate([table, filler], axis=0).T[:members]
        table = jnp.where(col_index < members, 0.5 * (table + mirrored), table)
        systems.append(table + jnp.where(row_index == col_index, float(members - 1), 0.0))
    for k in range(members):
        for region, table in enumerate(systems):
            row = table[k : k + 1]
            row = row / row[:, k : k + 1]
            column = table[:, k : k + 1] - jnp.where(row_index[:, :1] == k, 1.0, 0.0)
            systems[region] = table - column * row
    return [jnp.concatenate([table, filler], axis=0).T[members : members + 8] for table in systems]


def solve_kernel(sums, result):
    for region, rows in enumerate(eliminate([sums[r] for r in range(sums.shape[0])])):
        result[region] = rows


def solve_weights(sums):
    regions, members, width = sums.shape
    lanes = 128 * (-(-(members + 8) // 128))
    padded = jnp.pad(sums, ((0, 0), (0, 0), (0, lanes - width)))
    result = pl.pallas_call(
        solve_kernel,
        out_shape=jax.ShapeDtypeStruct((regions, 8, lanes), jnp.float32),
        in_specs=[pl.BlockSpec(memory_space=pltpu.VMEM)],
        out_specs=pl.BlockSpec(memory_space=pltpu.VMEM),
        cost_estimate=pl.CostEstimate(flops=10**9, bytes_accessed=4 * padded.size, transcendentals=0),
    )(padded)
    return result[:, 0, :members]


def plain_increment(
    ens_coarse, col_interp, row_weights, ctrl_vec, band_loc, row_loc, level_loc, total_members
):
    fine_rows = row_weights.shape[1]
    columns = band_loc.shape[0]
    coarse_cols = jnp.einsum(
        "tklic,jc->tklij", ens_coarse, col_interp, preferred_element_type=jnp.float32
    ).astype(jnp.bfloat16)
    stencil = row_matrix(row_weights, fine_rows, fine_rows // 2)
    refined = jnp.einsum(
        "tklij,ri->tkljr",
        lax.all_to_all(coarse_cols, "tile", split_axis=4, concat_axis=3, tiled=True),
        stencil,
        preferred_element_type=jnp.float32,
    ).astype(jnp.bfloat16)
    member_fine = refined[0]
    slot_term = member_fine * ctrl_vec[0][None]
    projected = slot_term.astype(jnp.bfloat16)
    if lax.axis_size("grp") > 1:
        projected = lax.psum(projected, "grp")
    padded = extended(projected, (("tile", 2),), columns)
    banded = jnp.einsum(
        "jq,klqr->kljr", band_loc, padded, preferred_element_type=jnp.float32
    ).astype(jnp.bfloat16)
    row_mixed = jnp.einsum(
        "kljs,rs->kljr", banded, row_loc, preferred_element_type=jnp.float32
    ).astype(jnp.bfloat16)
    localized = jnp.einsum(
        "lm,kmjr->kljr", level_loc, row_mixed, preferred_element_type=jnp.float32
    ).astype(jnp.bfloat16)
    return swap_add(
        jnp.sum(member_fine.astype(jnp.float32) * localized.astype(jnp.float32), axis=0)
    ) / (total_members - 1)


def place():
    tile = lax.axis_index("tile")
    core = lax.rem(tile, 2)
    chip = lax.div(tile, 2)
    return lax.div(chip, 2), lax.rem(chip, 2), core, lax.axis_index("mem")


def target(z, x, core, y):
    return {"tile": (z * 2 + x) * 2 + core, "mem": y}


def greet(peers):
    barrier = pltpu.get_barrier_semaphore()
    for peer in peers:
        pl.semaphore_signal(barrier, inc=1, device_id=peer, device_id_type=MESH)
    pl.semaphore_wait(barrier, len(peers))


def fused_kernel(
    depth, scale, raw, *refs
):
    sources, refs = refs[:10], refs[10:]
    outputs, places, refs = refs[:2], refs[2:12], refs[12:]
    loads, refs = refs[0], refs[1:]
    copies = [
        pltpu.make_async_copy(source, place_in, loads.at[n])
        for n, (source, place_in) in enumerate(zip(sources, places))
    ]
    for copy in copies:
        copy.start()
    fused_steps(depth, scale, raw, copies, *places, *outputs, *refs)


def fused_steps(
    depth, scale, raw, copies, ctrl, band_in, columns_in, row_weights, row_loc, levels_in,
    observed, innov, precision, region, result, weights,
    own, interp, stencil, level_loc, shifted, gram, gram_in, solved, solved_in,
    blocks, slots, halo, coarse, fine, proj, banded, kron, acc, part,
    near, sums, far, turned, swap_out, swap_in,
    send_raw, recv_raw, send_pair, recv_pair,
    send_a, recv_a, send_x, recv_x, send_y, recv_y, send_h, recv_h,
    send_near, recv_near, send_far, recv_far, send_s, recv_s,
    send_g, recv_g, send_w, recv_w
):
    z, x, core, y = place()
    f32, bf16 = jnp.float32, jnp.bfloat16
    members, chips = blocks.shape[0], blocks.shape[1]
    columns, rows, levels = fine.shape
    coarse_rows = stencil.shape[1]
    stride = coarse_rows + 8
    kept = acc.shape[0]
    per_side = depth // 2
    count = per_side * 2
    side = lax.div(z, per_side)
    chip = z * 2 + x
    across, beside = target(z, x, core, 1 - y), target(z, 1 - x, core, y)
    partner = target(z, x, 1 - core, y)
    copies[0].wait()
    for j in range(8):
        own[j // 4, (j % 4) * rows : (j % 4 + 1) * rows, :] = ctrl[:, j, :].T.astype(bf16)
    copies[1].wait()
    window = band_in.shape[1]
    widen = (
        lax.broadcasted_iota(jnp.int32, (window, levels), 0)
        == lax.broadcasted_iota(jnp.int32, (window, levels), 1)
    ).astype(bf16)
    band_rows = jnp.dot(band_in[...], widen, preferred_element_type=f32)
    band_rows = jnp.concatenate([band_rows, jnp.zeros_like(band_rows)], axis=0).astype(bf16)
    for h in range(2):
        own[h, 4 * rows : 4 * rows + 16, :] = band_rows
    line = [(lax.rem(z + dz, depth), lax.rem(core + dc, 2)) for dz in range(depth) for dc in range(2)]
    greet(
        [target(zz, x, cc, y) for zz, cc in line[1:]]
        + [target(lax.rem(z + dz, depth), 1 - x, core, y) for dz in range(depth)]
        + [across, target(z, 1 - x, core, 1 - y)]
    )

    mine = lax.rem(z, per_side) * 4 + x * 2 + core
    kind = lax.rem(z, per_side) * 2 + core

    def is_self(zz):
        return jnp.logical_and(z == zz, core == side)

    for zz in range(depth):
        @pl.when(jnp.logical_not(is_self(zz)))
        def _():
            pltpu.make_async_remote_copy(
                own.at[y], slots.at[mine, y], send_a.at[zz], recv_a.at[kind],
                target(zz, x, side, y), MESH,
            ).start()

        @pl.when(is_self(zz))
        def _():
            pltpu.make_async_copy(own.at[y], slots.at[mine, y], recv_a.at[kind]).start()

    def raw_copy(m, step):
        to = lax.rem(chip + step, chips)
        return pltpu.make_async_remote_copy(
            raw.at[to * members + m], blocks.at[m, chip, core], send_raw.at[m, step],
            recv_raw.at[m, chip], target(lax.div(to, 2), lax.rem(to, 2), core, y), MESH,
        )

    def send_member(m):
        for step in range(1, chips):
            raw_copy(m, step).start()
        pltpu.make_async_copy(
            raw.at[chip * members + m], blocks.at[m, chip, core], recv_raw.at[m, chip]
        ).start()

    def pair_copy(m):
        held = blocks.at[m, :, core]
        return pltpu.make_async_remote_copy(held, held, send_pair.at[m], recv_pair.at[m], partner, MESH)

    early = min(2, members)
    for m in range(early):
        send_member(m)

    def done(ref, sem):
        pltpu.make_async_copy(ref, ref, sem).wait()

    for copy in copies[2:]:
        copy.wait()
    people, spots = observed.shape
    hx = observed[...]
    weighted = (hx.astype(f32) * precision[...]).astype(bf16).astype(f32)
    rest = innov[...]
    thirds = jnp.zeros((48, spots), f32)
    third_at = lax.broadcasted_iota(jnp.int32, (48, spots), 0)
    for n in range(3):
        third = rest.astype(bf16).astype(f32)
        thirds = jnp.where(third_at == n, third, thirds)
        rest = rest - third
    right = jnp.concatenate([hx, thirds.astype(bf16)], axis=0)
    for g in range(NREG):
        masked = jnp.where(region[...] == g, weighted, 0.0).astype(bf16)
        gram[g] = lax.dot_general(
            masked, right, (((1,), (1,)), ((), ())), preferred_element_type=f32
        )
    per_half = NREG // 2
    grams = pltpu.make_async_remote_copy(
        gram.at[pl.ds((1 - y) * per_half, per_half)], gram_in, send_g, recv_g, across, MESH
    )
    grams.start()

    coarse_width = columns_in.shape[0]
    fill = jnp.zeros((levels - coarse_width, levels), f32)
    shifted[...] = jnp.zeros_like(shifted)
    shifted[8 : 8 + levels, :] = jnp.concatenate([columns_in[...].astype(f32), fill], axis=0).T
    interp[...] = shifted[pl.ds(pl.multiple_of(core * kept, 8), columns), :][:, :coarse_width].astype(bf16)
    coarse_at = lax.broadcasted_iota(jnp.int32, (coarse_rows, rows), 0)
    parent_at = lax.broadcasted_iota(jnp.int32, (coarse_rows, rows), 1) // 2
    spreading = jnp.zeros((coarse_rows, rows), f32)
    for n in range(3):
        spreading = spreading + jnp.where(
            coarse_at == parent_at + n - 1, row_weights[n : n + 1, :].astype(f32), 0.0
        )
    stencil[...] = jnp.concatenate([spreading, fill], axis=0).T[:, :coarse_rows].astype(bf16)
    flipped = levels_in[...].astype(f32).T.astype(bf16)
    level_loc[...] = jnp.zeros_like(level_loc)
    level_loc[:levels, :levels] = flipped
    level_loc[levels:, levels:] = flipped

    def forward(slot, send, recv, peer):
        held = slots.at[slot, y]
        pltpu.make_async_remote_copy(held, held, send, recv, peer, MESH).start()

    for k in range(count):
        slot = (k // 2) * 4 + x * 2 + k % 2
        done(slots.at[slot, y], recv_a.at[k])
        forward(slot, send_x.at[k], recv_x.at[k], beside)
        forward(slot, send_y.at[k], recv_y.at[k], across)
    for k in range(count):
        slot = (k // 2) * 4 + (1 - x) * 2 + k % 2
        done(slots.at[slot, y], recv_x.at[k])
        forward(slot, send_y.at[count + k], recv_y.at[count + k], across)
    for m in range(early, members):
        send_member(m)
    grams.wait_recv()
    answers = eliminate([gram[y * per_half + g] + gram_in[g] for g in range(per_half)])
    for g, rows_solved in enumerate(answers):
        solved[g : g + 1, :] = rows_solved[0:1] + rows_solved[1:2] + rows_solved[2:3]
    solved[per_half:, :] = jnp.zeros_like(solved[per_half:, :])
    for k in range(count):
        done(slots.at[(k // 2) * 4 + x * 2 + k % 2, 1 - y], recv_y.at[k])
    for k in range(count):
        done(slots.at[(k // 2) * 4 + (1 - x) * 2 + k % 2, 1 - y], recv_y.at[count + k])
    edges = pltpu.make_async_remote_copy(
        slots.at[(1 - core) * (2 * count - 1)], halo, send_h, recv_h, partner, MESH
    )
    edges.start()

    acc[...] = jnp.zeros_like(acc)
    tall_at = lax.broadcasted_iota(jnp.int32, (128, 8), 0)
    wide_at = lax.broadcasted_iota(jnp.int32, (128, 24 * GROUP), 1)
    deep_at = lax.broadcasted_iota(jnp.int32, (128, 24 * GROUP), 0)
    spread_rows = (tall_at // GROUP == lax.broadcasted_iota(jnp.int32, (128, 8), 1)).astype(bf16)
    spread_cols = (deep_at == wide_at // GROUP).astype(bf16)
    same = lax.rem(deep_at, GROUP) == lax.rem(wide_at, GROUP)
    for b in range(kept // 8):
        band = slots[b, 0, 4 * rows : 4 * rows + 8, :]
        tall = jnp.dot(spread_rows, band, preferred_element_type=f32).astype(bf16)
        wide = jnp.dot(tall, spread_cols, preferred_element_type=f32)
        kron[b] = jnp.where(same, wide, 0.0).astype(bf16)
    edges.wait()
    answer = pltpu.make_async_remote_copy(solved, solved_in, send_w, recv_w, across, MESH)
    answer.start()

    partners = [(1 - x, y), (x, 1 - y), (1 - x, 1 - y)]

    def rows_of(yy):
        return pl.ds(pl.multiple_of(yy * (rows // 2), rows // 2), rows // 2)

    def near_copy(k, n):
        xx, yy = partners[n]
        slot = lax.div(k, 2) * 4 + xx * 2 + lax.rem(k, 2)
        return pltpu.make_async_remote_copy(
            part.at[slot, :, rows_of(yy), :], near.at[n, k], send_near.at[n, k],
            recv_near.at[n, k], target(z, xx, core, yy), MESH,
        )

    def send_slot(b):
        k = lax.div(b, 4) * 2 + lax.rem(b, 2)
        inside = lax.rem(lax.div(b, 2), 2) == x

        @pl.when(inside)
        def _():
            near_copy(k, 1).start()

        @pl.when(jnp.logical_not(inside))
        def _():
            near_copy(k, 2).start()
            near_copy(k, 0).start()

    def refine(pair, table):
        base = 2 * pair * stride
        joined = jnp.concatenate(
            [coarse[pl.ds(base + k * stride, coarse_rows), :].astype(bf16) for k in range(2)], axis=1
        )
        fresh = jnp.dot(stencil[...], joined, preferred_element_type=f32).astype(bf16)
        for k in range(2):
            piece = fresh[:, k * levels : (k + 1) * levels]
            j = 2 * pair + k
            fine[j] = piece
            proj[j] = (piece.astype(f32) * table(k).astype(f32)).astype(bf16)

    @pl.loop(0, members)
    def _(m):
        for c in range(chips):
            done(blocks.at[m, c, core], recv_raw.at[m, c])
        copy = pair_copy(m)
        copy.start()
        copy.wait_recv()

        for c in range(chips):
            for half in range(2):
                for two in range(2):
                    pair = jnp.concatenate(
                        [blocks[m, c, half, 2 * two], blocks[m, c, half, 2 * two + 1]], axis=1
                    )
                    mixed = jnp.dot(interp[...], pair, preferred_element_type=f32)
                    row = 8 * c + 4 * half + 2 * two
                    for k in range(2):
                        coarse[pl.ds(row + k, columns, stride=stride), :] = mixed[
                            :, k * levels : (k + 1) * levels
                        ]

        for pair in range(4):
            def table(k):
                j = 2 * pair + k
                return halo[j // 4, (j % 4) * rows : (j % 4 + 1) * rows, :]

            refine(pair, table)
            refine(columns // 2 - 4 + pair, table)

        for b in range(kept // 8):
            for pair in range(4):
                def table(k):
                    j = 2 * pair + k
                    return slots[b, j // 4, (j % 4) * rows : (j % 4 + 1) * rows, :]

                refine(4 + 4 * b + pair, table)

        def band_mix(b):
            for pair in range(rows // (2 * GROUP)):
                parts = []
                for k in range(2):
                    at = (2 * pair + k) * GROUP
                    parts.append(proj[8 * b : 8 * b + 24, at : at + GROUP, :].reshape(24 * GROUP, levels))
                mixed = jnp.dot(
                    kron[b], jnp.concatenate(parts, axis=1), preferred_element_type=f32
                ).astype(bf16)
                for k in range(2):
                    at = (2 * pair + k) * GROUP
                    banded[b % 2, :, at : at + GROUP, :] = mixed[
                        :, k * levels : (k + 1) * levels
                    ].reshape(8, GROUP, levels)

        def level_mix(b):
            for pair in range(4):
                joined = jnp.concatenate(
                    [banded[b % 2, 2 * pair], banded[b % 2, 2 * pair + 1]], axis=1
                )
                mixed = jnp.dot(row_loc[...], joined, preferred_element_type=f32).astype(bf16)
                localized = jnp.dot(mixed, level_loc[...], preferred_element_type=f32)
                for k in range(2):
                    j = 8 * b + 2 * pair + k
                    acc[j] += fine[8 + j].astype(f32) * localized[:, k * levels : (k + 1) * levels]

        for b in range(0, kept // 8, 2):
            band_mix(b)
            band_mix(b + 1)
            level_mix(b)
            level_mix(b + 1)

            @pl.when(m == members - 1)
            def _():
                for slot in (b, b + 1):
                    part[slot] = acc[8 * slot : 8 * slot + 8].astype(bf16)
                if b > 0:
                    send_slot(b - 2)
                    send_slot(b - 1)

    send_slot(kept // 8 - 2)
    send_slot(kept // 8 - 1)

    for k in range(count):
        for n in range(3):
            near_copy(k, n).wait_recv()
        slot = (k // 2) * 4 + x * 2 + k % 2
        total = acc[pl.ds(8 * slot, 8), rows_of(y), :]
        total = (total + near[0, k].astype(f32)) + (near[1, k].astype(f32) + near[2, k].astype(f32))
        sums[k] = total.astype(bf16)
        owner = per_side * core + k // 2
        to_self = jnp.logical_and(z == owner, core == k % 2)

        @pl.when(jnp.logical_not(to_self))
        def _():
            pltpu.make_async_remote_copy(
                sums.at[k], far.at[z], send_far.at[k], recv_far.at[z],
                target(owner, x, k % 2, y), MESH,
            ).start()

        @pl.when(to_self)
        def _():
            pltpu.make_async_copy(sums.at[k], far.at[z], recv_far.at[z]).start()

    answer.wait()
    held, came = solved[:per_half, :people], solved_in[:per_half, :people]
    weights[:per_half, :] = jnp.where(y == 0, held, came)
    weights[per_half:, :] = jnp.where(y == 0, came, held)
    grams.wait_send()
    for m in range(members):
        for step in range(1, chips):
            raw_copy(m, step).wait_send()
        pair_copy(m).wait_send()
    for k in range(count):
        done(slots.at[(k // 2) * 4 + x * 2 + k % 2, y], send_x.at[k])
    for k in range(2 * count):
        done(slots.at[k, y], send_y.at[k])
    for zz in range(depth):
        @pl.when(jnp.logical_not(is_self(zz)))
        def _():
            done(own.at[y], send_a.at[zz])

    for zz in range(depth):
        done(far.at[zz], recv_far.at[zz])

    def levels_of(yy):
        return pl.ds(pl.multiple_of(yy * (levels // 2), levels // 2), levels // 2)

    half = rows // 2
    swaps = []
    for pair in range(4):
        pieces = []
        for k in range(2):
            value = far[0, 2 * pair + k].astype(f32)
            for zz in range(1, depth):
                value = value + far[zz, 2 * pair + k].astype(f32)
            pieces.append(value)
        turned[pair] = jnp.concatenate(pieces, axis=0).T
        swap_out[pair] = turned[pair, levels_of(1 - y), :].astype(bf16)
        copy = pltpu.make_async_remote_copy(
            swap_out.at[pair], swap_in.at[pair], send_s.at[pair], recv_s.at[pair], across, MESH
        )
        copy.start()
        swaps.append(copy)
    for pair in range(4):
        swaps[pair].wait_recv()
        held = turned[pair, levels_of(y), :]
        came = swap_in[pair].astype(f32)
        low = jnp.where(y == 0, held, came)
        high = jnp.where(y == 0, came, held)
        for k in range(2):
            at = slice(k * half, (k + 1) * half)
            result[:, 2 * pair + k, :] = jnp.concatenate([low[:, at], high[:, at]], axis=1) * scale
    for copy in swaps:
        copy.wait_send()
    for k in range(count):
        for n in range(3):
            near_copy(k, n).wait_send()
        owner = per_side * core + k // 2

        @pl.when(jnp.logical_not(jnp.logical_and(z == owner, core == k % 2)))
        def _():
            done(sums.at[k], send_far.at[k])


def fused(
    raw, ctrl, band, columns_in, row_weights, row_loc, level_loc, observed, innov, precision, region,
    depth, scale
):
    bf16, f32 = jnp.bfloat16, jnp.float32
    chips = depth * 2
    members = raw.shape[0] // chips
    columns = 8 * chips + 16
    coarse_rows, rows = row_weights.shape[1] // 2, row_weights.shape[1]
    levels = row_loc.shape[0]
    people = observed.shape[0]
    kept = columns - 16
    count = depth
    loaded = (
        ctrl, band, columns_in, row_weights, row_loc, level_loc, observed, innov, precision, region
    )
    dma = pltpu.SemaphoreType.DMA
    vmem = pl.BlockSpec(memory_space=pltpu.VMEM)
    own = jax.ShapeDtypeStruct((2, 4 * rows + 16, levels), bf16)
    piece = (8, rows // 2, levels)
    swap = (4, levels // 2, rows)
    flops = 2 * members * levels * rows * columns * (coarse_rows + 24 * GROUP + rows + levels)
    return pl.pallas_call(
        functools.partial(fused_kernel, depth, scale),
        out_shape=(
            jax.ShapeDtypeStruct((levels // 2, 8, rows), f32),
            jax.ShapeDtypeStruct((NREG, people), f32),
        ),
        in_specs=[pl.BlockSpec(memory_space=pltpu.HBM)] * 11,
        out_specs=(vmem, vmem),
        scratch_shapes=[
            *[pltpu.VMEM(value.shape, value.dtype) for value in loaded],
            dma((len(loaded),)),
            pltpu.VMEM(own.shape, bf16),
            pltpu.VMEM((columns, raw.shape[2]), bf16),
            pltpu.VMEM((rows, coarse_rows), bf16),
            pltpu.VMEM((2 * levels, 2 * levels), bf16),
            pltpu.VMEM((2 * kept + 16, levels), f32),
            pltpu.VMEM((NREG, people, 128), f32),
            pltpu.VMEM((NREG // 2, people, 128), f32),
            pltpu.VMEM((8, 128), f32),
            pltpu.VMEM((8, 128), f32),
            pltpu.VMEM((members, chips, 2) + raw.shape[1:], bf16),
            pltpu.VMEM((kept // 8,) + own.shape, bf16),
            pltpu.VMEM(own.shape, bf16),
            pltpu.VMEM((columns * (coarse_rows + 8), levels), f32),
            pltpu.VMEM((columns, rows, levels), bf16),
            pltpu.VMEM((columns, rows, levels), bf16),
            pltpu.VMEM((2, 8, rows, levels), bf16),
            pltpu.VMEM((kept // 8, 8 * GROUP, 24 * GROUP), bf16),
            pltpu.VMEM((kept, rows, levels), f32),
            pltpu.VMEM((kept // 8, 8, rows, levels), bf16),
            pltpu.VMEM((3, count) + piece, bf16),
            pltpu.VMEM((count,) + piece, bf16),
            pltpu.VMEM((depth,) + piece, bf16),
            pltpu.VMEM((4, levels, rows), f32),
            pltpu.VMEM(swap, bf16),
            pltpu.VMEM(swap, bf16),
            dma((members, chips)), dma((members, chips)), dma((members,)), dma((members,)),
            dma((depth,)), dma((count,)), dma((count,)), dma((count,)),
            dma((2 * count,)), dma((2 * count,)), dma, dma,
            dma((3, count)), dma((3, count)), dma((count,)), dma((depth,)), dma((4,)), dma((4,)),
            dma, dma, dma, dma,
        ],
        compiler_params=pltpu.CompilerParams(
            collective_id=0, has_side_effects=True, vmem_limit_bytes=67043328
        ),
        cost_estimate=pl.CostEstimate(flops=flops, bytes_accessed=4 * raw.size, transcendentals=0),
    )(raw, *loaded)


def member_plan(
    ens_coarse,
    col_interp,
    row_weights,
    ctrl_vec,
    band_loc,
    row_loc,
    level_loc,
    hx_pert,
    innov,
    obs_prec,
    obs_region,
):
    raw = jnp.transpose(ens_coarse[0], (0, 2, 3, 1))
    increment, weights = fused(
        raw, ctrl_vec[0], band_loc, col_interp.T, row_weights, row_loc, level_loc,
        hx_pert[0], innov, obs_prec, obs_region,
        lax.axis_size("tile") // 4, 1.0 / (hx_pert.shape[1] - 1),
    )
    return (increment[None], weights)


def fits(mesh_sizes, total_members, block, columns, fine_rows, levels):
    tiles = mesh_sizes["tile"]
    members, block_rows, width = block[1], block[3], block[4]
    return (
        mesh_sizes["grp"] == 1
        and mesh_sizes["mem"] == 2
        and tiles % 8 == 0
        and members % (tiles // 2) == 0
        and tiles * columns == levels
        and width <= levels
        and total_members % 8 == 0
        and total_members + 48 == levels
        and columns == 8
        and block_rows == 4
        and fine_rows == 128
        and levels == 128
    )


def body(
    ens_coarse,
    col_interp,
    row_weights,
    ctrl_vec,
    band_loc,
    row_loc,
    level_loc,
    hx_pert,
    innov,
    obs_prec,
    obs_region,
):
    sizes = {axis: lax.axis_size(axis) for axis in ("grp", "tile", "mem")}
    total_members = hx_pert.shape[1]
    if fits(sizes, total_members, ens_coarse.shape, band_loc.shape[0], row_loc.shape[0], level_loc.shape[0]):
        return member_plan(
            ens_coarse, col_interp, row_weights, ctrl_vec, band_loc, row_loc, level_loc,
            hx_pert, innov, obs_prec, obs_region,
        )
    observed = hx_pert[0]
    weighted = (observed * obs_prec[0][None, :]).astype(jnp.bfloat16)
    labels = lax.broadcasted_iota(jnp.int32, (NREG, observed.shape[1]), 0)
    member_of = obs_region[0][None, :] == labels
    masked = jnp.where(member_of[:, None, :], weighted[None], jnp.zeros((), jnp.bfloat16))
    gram_sums = jnp.einsum("rko,jo->rkj", masked, observed, preferred_element_type=jnp.float32)
    innov_rows = jnp.where(member_of, innov[0][None, :], 0.0)
    right_side = jnp.dot(
        innov_rows, weighted.astype(jnp.float32).T, precision=lax.Precision.HIGHEST
    )
    sums = jnp.concatenate([gram_sums, right_side[:, :, None]], axis=2)
    sums = swap_add(lax.psum(sums, "grp") if lax.axis_size("grp") > 1 else sums)
    increment = plain_increment(
        ens_coarse, col_interp, row_weights, ctrl_vec, band_loc, row_loc, level_loc, total_members
    )
    own_weights = solve_weights(sums)
    weights = collect(own_weights)
    return (increment[None], weights)


def solution(mesh):
    placed = (
        P("grp", "mem", None, "tile", None),
        P(),
        P(),
        P("grp", None, "tile", None),
        P("tile", None),
        P(),
        P(),
        P("grp", None, ("tile", "mem")),
        P("grp", ("tile", "mem")),
        P("grp", ("tile", "mem")),
        P("grp", ("tile", "mem")),
    )
    return jax.shard_map(
        body,
        mesh=mesh,
        in_specs=placed,
        out_specs=(P("grp", "mem", "tile", None), P("tile", None)),
        check_vma=False,
    )
```

```python
import functools

import jax
import jax.numpy as jnp
from jax import lax
from jax.experimental import pallas as pl
from jax.experimental.pallas import tpu as pltpu
from jax.sharding import PartitionSpec as P

NREG = 8
GROUP = 16
MESH = pl.DeviceIdType.MESH


def extended(value, sides, width):
    for axis, dim in sides:
        peers, length = (lax.axis_size(axis), value.shape[dim])
        up = [(i, (i + 1) % peers) for i in range(peers - 1)]
        down = [(j, i) for i, j in up]
        last = lax.slice_in_dim(value, length - width, length, axis=dim)
        first = lax.slice_in_dim(value, 0, width, axis=dim)
        before = lax.ppermute(last, axis, up)
        after = lax.ppermute(first, axis, down)
        value = jnp.concatenate([before, value, after], axis=dim)
    return value


def swap_add(value):
    peers = lax.axis_size("mem")
    me = lax.axis_index("mem")
    length = value.shape[0] // peers
    total = lax.dynamic_slice_in_dim(value, me * length, length, 0)
    for shift in range(1, peers):
        other = lax.rem(me + shift, peers)
        part = lax.dynamic_slice_in_dim(value, other * length, length, 0)
        pairs = [(i, (i + shift) % peers) for i in range(peers)]
        total = total + lax.ppermute(part, "mem", pairs)
    return total


def collect(value):
    peers = lax.axis_size("mem")
    me = lax.axis_index("mem")
    length = value.shape[0]
    result = jnp.zeros((peers * length,) + value.shape[1:], value.dtype)
    result = lax.dynamic_update_slice_in_dim(result, value, me * length, 0)
    for shift in range(1, peers):
        pairs = [(i, (i + shift) % peers) for i in range(peers)]
        moved = lax.ppermute(value, "mem", pairs)
        source = lax.rem(me + peers - shift, peers)
        result = lax.dynamic_update_slice_in_dim(result, moved, source * length, 0)
    return result


def row_matrix(row_weights, fine_rows, coarse_rows):
    fine_index = lax.broadcasted_iota(jnp.int32, (fine_rows, coarse_rows), 0)
    coarse_index = lax.broadcasted_iota(jnp.int32, (fine_rows, coarse_rows), 1)
    weights = row_weights.astype(jnp.float32)
    stencil = jnp.zeros((fine_rows, coarse_rows), jnp.float32)
    for offset in range(3):
        matched = coarse_index == fine_index // 2 + offset - 1
        stencil = stencil + jnp.where(matched, weights[offset][:, None], 0.0)
    return stencil.astype(jnp.bfloat16)


def eliminate(tables):
    members, lanes = tables[0].shape
    row_index = lax.broadcasted_iota(jnp.int32, (members, lanes), 0)
    col_index = lax.broadcasted_iota(jnp.int32, (members, lanes), 1)
    filler = jnp.zeros((lanes - members, lanes), jnp.float32)
    systems = []
    for table in tables:
        mirrored = jnp.concatenate([table, filler], axis=0).T[:members]
        table = jnp.where(col_index < members, 0.5 * (table + mirrored), table)
        systems.append(table + jnp.where(row_index == col_index, float(members - 1), 0.0))
    for k in range(members):
        for region, table in enumerate(systems):
            row = table[k : k + 1]
            row = row / row[:, k : k + 1]
            column = table[:, k : k + 1] - jnp.where(row_index[:, :1] == k, 1.0, 0.0)
            systems[region] = table - column * row
    return [jnp.concatenate([table, filler], axis=0).T[members : members + 8] for table in systems]


def solve_kernel(sums, result):
    for region, rows in enumerate(eliminate([sums[r] for r in range(sums.shape[0])])):
        result[region] = rows


def solve_weights(sums):
    regions, members, width = sums.shape
    lanes = 128 * (-(-(members + 8) // 128))
    padded = jnp.pad(sums, ((0, 0), (0, 0), (0, lanes - width)))
    result = pl.pallas_call(
        solve_kernel,
        out_shape=jax.ShapeDtypeStruct((regions, 8, lanes), jnp.float32),
        in_specs=[pl.BlockSpec(memory_space=pltpu.VMEM)],
        out_specs=pl.BlockSpec(memory_space=pltpu.VMEM),
        cost_estimate=pl.CostEstimate(flops=10**9, bytes_accessed=4 * padded.size, transcendentals=0),
    )(padded)
    return result[:, 0, :members]


def plain_increment(
    ens_coarse, col_interp, row_weights, ctrl_vec, band_loc, row_loc, level_loc, total_members
):
    fine_rows = row_weights.shape[1]
    columns = band_loc.shape[0]
    coarse_cols = jnp.einsum(
        "tklic,jc->tklij", ens_coarse, col_interp, preferred_element_type=jnp.float32
    ).astype(jnp.bfloat16)
    stencil = row_matrix(row_weights, fine_rows, fine_rows // 2)
    refined = jnp.einsum(
        "tklij,ri->tkljr",
        lax.all_to_all(coarse_cols, "tile", split_axis=4, concat_axis=3, tiled=True),
        stencil,
        preferred_element_type=jnp.float32,
    ).astype(jnp.bfloat16)
    member_fine = refined[0]
    slot_term = member_fine * ctrl_vec[0][None]
    projected = slot_term.astype(jnp.bfloat16)
    if lax.axis_size("grp") > 1:
        projected = lax.psum(projected, "grp")
    padded = extended(projected, (("tile", 2),), columns)
    banded = jnp.einsum(
        "jq,klqr->kljr", band_loc, padded, preferred_element_type=jnp.float32
    ).astype(jnp.bfloat16)
    row_mixed = jnp.einsum(
        "kljs,rs->kljr", banded, row_loc, preferred_element_type=jnp.float32
    ).astype(jnp.bfloat16)
    localized = jnp.einsum(
        "lm,kmjr->kljr", level_loc, row_mixed, preferred_element_type=jnp.float32
    ).astype(jnp.bfloat16)
    return swap_add(
        jnp.sum(member_fine.astype(jnp.float32) * localized.astype(jnp.float32), axis=0)
    ) / (total_members - 1)


def place():
    tile = lax.axis_index("tile")
    core = lax.rem(tile, 2)
    chip = lax.div(tile, 2)
    return lax.div(chip, 2), lax.rem(chip, 2), core, lax.axis_index("mem")


def target(z, x, core, y):
    return {"tile": (z * 2 + x) * 2 + core, "mem": y}


def greet(peers):
    barrier = pltpu.get_barrier_semaphore()
    for peer in peers:
        pl.semaphore_signal(barrier, inc=1, device_id=peer, device_id_type=MESH)
    pl.semaphore_wait(barrier, len(peers))


def fused_kernel(
    depth, scale, raw, *refs
):
    sources, refs = refs[:10], refs[10:]
    outputs, places, refs = refs[:2], refs[2:12], refs[12:]
    loads, refs = refs[0], refs[1:]
    copies = [
        pltpu.make_async_copy(source, place_in, loads.at[n])
        for n, (source, place_in) in enumerate(zip(sources, places))
    ]
    for copy in copies:
        copy.start()
    fused_steps(depth, scale, raw, copies, *places, *outputs, *refs)


def fused_steps(
    depth, scale, raw, copies, ctrl, band_in, columns_in, row_weights, row_loc, levels_in,
    observed, innov, precision, region, result, weights,
    own, interp, stencil, level_loc, shifted, gram, gram_in, solved, solved_in,
    blocks, slots, halo, coarse, fine, proj, banded, kron, acc, part,
    first, mid, second, sums, far,
    send_raw, recv_raw, send_pair, recv_pair,
    send_a, recv_a, send_x, recv_x, send_y, recv_y, send_h, recv_h,
    send_first, recv_first, send_second, recv_second, send_far, recv_far,
    send_g, recv_g, send_w, recv_w, send_z
):
    z, x, core, y = place()
    f32, bf16 = jnp.float32, jnp.bfloat16
    members, chips = blocks.shape[0], blocks.shape[1]
    columns, rows, levels = fine.shape
    coarse_rows = stencil.shape[1]
    stride = coarse_rows + 8
    kept = acc.shape[0]
    per_side = depth // 2
    count = per_side * 2
    side = lax.div(z, per_side)
    chip = z * 2 + x
    across, beside = target(z, x, core, 1 - y), target(z, 1 - x, core, y)
    partner = target(z, x, 1 - core, y)
    copies[0].wait()
    for j in range(8):
        own[j // 4, (j % 4) * rows : (j % 4 + 1) * rows, :] = ctrl[:, j, :].T.astype(bf16)
    copies[1].wait()
    window = band_in.shape[1]
    widen = (
        lax.broadcasted_iota(jnp.int32, (window, levels), 0)
        == lax.broadcasted_iota(jnp.int32, (window, levels), 1)
    ).astype(bf16)
    band_rows = jnp.dot(band_in[...], widen, preferred_element_type=f32)
    band_rows = jnp.concatenate([band_rows, jnp.zeros_like(band_rows)], axis=0).astype(bf16)
    for h in range(2):
        own[h, 4 * rows : 4 * rows + 16, :] = band_rows
    line = [(lax.rem(z + dz, depth), lax.rem(core + dc, 2)) for dz in range(depth) for dc in range(2)]
    greet(
        [target(zz, x, cc, y) for zz, cc in line[1:]]
        + [target(lax.rem(z + dz, depth), 1 - x, core, y) for dz in range(depth)]
        + [across, target(z, 1 - x, core, 1 - y)]
    )

    mine = lax.rem(z, per_side) * 4 + x * 2 + core
    kind = lax.rem(z, per_side) * 2 + core

    def is_self(zz):
        return jnp.logical_and(z == zz, core == side)

    def is_gate(zz):
        return zz == per_side - 1 + zz // per_side

    def direct(zz):
        near_side = True if is_gate(zz) else side == zz // per_side
        return jnp.logical_and(jnp.logical_not(is_self(zz)), near_side)

    def relays(zz):
        here = jnp.logical_and(side == zz // per_side, side != core)
        return jnp.logical_and(here, z == per_side - 1 + side)

    for zz in range(depth):
        @pl.when(direct(zz))
        def _():
            pltpu.make_async_remote_copy(
                own.at[y], slots.at[mine, y], send_a.at[zz], recv_a.at[kind],
                target(zz, x, side, y), MESH,
            ).start()

        @pl.when(is_self(zz))
        def _():
            pltpu.make_async_copy(own.at[y], slots.at[mine, y], recv_a.at[kind]).start()

    def raw_copy(m, step):
        to = lax.rem(chip + step, chips)
        return pltpu.make_async_remote_copy(
            raw.at[to * members + m], blocks.at[m, chip, core], send_raw.at[m, step],
            recv_raw.at[m, chip], target(lax.div(to, 2), lax.rem(to, 2), core, y), MESH,
        )

    def send_member(m):
        for step in range(1, chips):
            raw_copy(m, step).start()
        pltpu.make_async_copy(
            raw.at[chip * members + m], blocks.at[m, chip, core], recv_raw.at[m, chip]
        ).start()

    def pair_copy(m):
        held = blocks.at[m, :, core]
        return pltpu.make_async_remote_copy(held, held, send_pair.at[m], recv_pair.at[m], partner, MESH)

    early = min(2, members)
    for m in range(early):
        send_member(m)

    def done(ref, sem):
        pltpu.make_async_copy(ref, ref, sem).wait()

    for copy in copies[2:]:
        copy.wait()
    people, spots = observed.shape
    hx = observed[...]
    weighted = (hx.astype(f32) * precision[...]).astype(bf16).astype(f32)
    rest = innov[...]
    thirds = jnp.zeros((48, spots), f32)
    third_at = lax.broadcasted_iota(jnp.int32, (48, spots), 0)
    for n in range(3):
        third = rest.astype(bf16).astype(f32)
        thirds = jnp.where(third_at == n, third, thirds)
        rest = rest - third
    right = jnp.concatenate([hx, thirds.astype(bf16)], axis=0)
    for g in range(NREG):
        masked = jnp.where(region[...] == g, weighted, 0.0).astype(bf16)
        gram[g] = lax.dot_general(
            masked, right, (((1,), (1,)), ((), ())), preferred_element_type=f32
        )
    per_half = NREG // 2
    grams = pltpu.make_async_remote_copy(
        gram.at[pl.ds((1 - y) * per_half, per_half)], gram_in, send_g, recv_g, across, MESH
    )
    grams.start()

    coarse_width = columns_in.shape[0]
    fill = jnp.zeros((levels - coarse_width, levels), f32)
    shifted[...] = jnp.zeros_like(shifted)
    shifted[8 : 8 + levels, :] = jnp.concatenate([columns_in[...].astype(f32), fill], axis=0).T
    interp[...] = shifted[pl.ds(pl.multiple_of(core * kept, 8), columns), :][:, :coarse_width].astype(bf16)
    coarse_at = lax.broadcasted_iota(jnp.int32, (coarse_rows, rows), 0)
    parent_at = lax.broadcasted_iota(jnp.int32, (coarse_rows, rows), 1) // 2
    spreading = jnp.zeros((coarse_rows, rows), f32)
    for n in range(3):
        spreading = spreading + jnp.where(
            coarse_at == parent_at + n - 1, row_weights[n : n + 1, :].astype(f32), 0.0
        )
    stencil[...] = jnp.concatenate([spreading, fill], axis=0).T[:, :coarse_rows].astype(bf16)
    flipped = levels_in[...].astype(f32).T.astype(bf16)
    level_loc[...] = jnp.zeros_like(level_loc)
    level_loc[:levels, :levels] = flipped
    level_loc[levels:, levels:] = flipped

    def forward(slot, send, recv, peer):
        held = slots.at[slot, y]
        pltpu.make_async_remote_copy(held, held, send, recv, peer, MESH).start()

    for k in range(count):
        slot = (k // 2) * 4 + x * 2 + k % 2
        done(slots.at[slot, y], recv_a.at[k])
        for zz in range(depth):
            if not is_gate(zz):
                @pl.when(relays(zz))
                def _():
                    forward(slot, send_z.at[k, zz], recv_a.at[k], target(zz, x, core, y))

        forward(slot, send_x.at[k], recv_x.at[k], beside)
        forward(slot, send_y.at[k], recv_y.at[k], across)
    for k in range(count):
        slot = (k // 2) * 4 + (1 - x) * 2 + k % 2
        done(slots.at[slot, y], recv_x.at[k])
        forward(slot, send_y.at[count + k], recv_y.at[count + k], across)
    for m in range(early, members):
        send_member(m)
    grams.wait_recv()
    answers = eliminate([gram[y * per_half + g] + gram_in[g] for g in range(per_half)])
    for g, rows_solved in enumerate(answers):
        solved[g : g + 1, :] = rows_solved[0:1] + rows_solved[1:2] + rows_solved[2:3]
    solved[per_half:, :] = jnp.zeros_like(solved[per_half:, :])
    for k in range(count):
        done(slots.at[(k // 2) * 4 + x * 2 + k % 2, 1 - y], recv_y.at[k])
    for k in range(count):
        done(slots.at[(k // 2) * 4 + (1 - x) * 2 + k % 2, 1 - y], recv_y.at[count + k])
    edges = pltpu.make_async_remote_copy(
        slots.at[(1 - core) * (2 * count - 1)], halo, send_h, recv_h, partner, MESH
    )
    edges.start()

    acc[...] = jnp.zeros_like(acc)
    tall_at = lax.broadcasted_iota(jnp.int32, (128, 8), 0)
    wide_at = lax.broadcasted_iota(jnp.int32, (128, 24 * GROUP), 1)
    deep_at = lax.broadcasted_iota(jnp.int32, (128, 24 * GROUP), 0)
    spread_rows = (tall_at // GROUP == lax.broadcasted_iota(jnp.int32, (128, 8), 1)).astype(bf16)
    spread_cols = (deep_at == wide_at // GROUP).astype(bf16)
    same = lax.rem(deep_at, GROUP) == lax.rem(wide_at, GROUP)
    for b in range(kept // 8):
        band = slots[b, 0, 4 * rows : 4 * rows + 8, :]
        tall = jnp.dot(spread_rows, band, preferred_element_type=f32).astype(bf16)
        wide = jnp.dot(tall, spread_cols, preferred_element_type=f32)
        kron[b] = jnp.where(same, wide, 0.0).astype(bf16)
    edges.wait()
    answer = pltpu.make_async_remote_copy(solved, solved_in, send_w, recv_w, across, MESH)
    answer.start()

    def slot_of(k, xx):
        return (k // 2) * 4 + xx * 2 + k % 2

    def first_copies(k, only=None):
        if k % 2 == 0:
            pieces = [(part.at[slot_of(k, 1 - x)], first.at[k], beside)]
        else:
            pieces = [(part.at[slot_of(k, xx), 1 - y], first.at[k, xx], across) for xx in range(2)]
        if only is not None:
            pieces = pieces[only : only + 1]
        return [
            pltpu.make_async_remote_copy(
                source, landing, send_first.at[k, n], recv_first.at[k, n], peer, MESH
            )
            for n, (source, landing, peer) in enumerate(pieces, only or 0)
        ]

    def second_copy(k):
        peer = across if k % 2 == 0 else beside
        return pltpu.make_async_remote_copy(
            mid.at[k], second.at[k], send_second.at[k], recv_second.at[k], peer, MESH
        )

    def send_slot(b):
        k, xx = (b // 4) * 2 + b % 2, (b // 2) % 2
        if k % 2 == 1:
            first_copies(k, xx)[0].start()
        else:
            @pl.when(x != xx)
            def _():
                first_copies(k)[0].start()

    def refine(pair, table):
        base = 2 * pair * stride
        joined = jnp.concatenate(
            [coarse[pl.ds(base + k * stride, coarse_rows), :].astype(bf16) for k in range(2)], axis=1
        )
        fresh = jnp.dot(stencil[...], joined, preferred_element_type=f32).astype(bf16)
        for k in range(2):
            piece = fresh[:, k * levels : (k + 1) * levels]
            j = 2 * pair + k
            fine[j] = piece
            proj[j] = (piece.astype(f32) * table(k).astype(f32)).astype(bf16)

    @pl.loop(0, members)
    def _(m):
        for c in range(chips):
            done(blocks.at[m, c, core], recv_raw.at[m, c])
        copy = pair_copy(m)
        copy.start()
        def interpolate(half):
            for c in range(chips):
                for two in range(2):
                    pair = jnp.concatenate(
                        [blocks[m, c, half, 2 * two], blocks[m, c, half, 2 * two + 1]], axis=1
                    )
                    mixed = jnp.dot(interp[...], pair, preferred_element_type=f32)
                    row = 8 * c + 4 * half + 2 * two
                    for k in range(2):
                        coarse[pl.ds(row + k, columns, stride=stride), :] = mixed[
                            :, k * levels : (k + 1) * levels
                        ]

        interpolate(core)
        copy.wait_recv()
        interpolate(1 - core)

        for pair in range(4):
            def table(k):
                j = 2 * pair + k
                return halo[j // 4, (j % 4) * rows : (j % 4 + 1) * rows, :]

            refine(pair, table)
            refine(columns // 2 - 4 + pair, table)

        for b in range(kept // 8):
            for pair in range(4):
                def table(k):
                    j = 2 * pair + k
                    return slots[b, j // 4, (j % 4) * rows : (j % 4 + 1) * rows, :]

                refine(4 + 4 * b + pair, table)

        def band_mix(b):
            for pair in range(rows // (2 * GROUP)):
                parts = []
                for k in range(2):
                    at = (2 * pair + k) * GROUP
                    parts.append(proj[8 * b : 8 * b + 24, at : at + GROUP, :].reshape(24 * GROUP, levels))
                mixed = jnp.dot(
                    kron[b], jnp.concatenate(parts, axis=1), preferred_element_type=f32
                ).astype(bf16)
                for k in range(2):
                    at = (2 * pair + k) * GROUP
                    banded[b % 2, :, at : at + GROUP, :] = mixed[
                        :, k * levels : (k + 1) * levels
                    ].reshape(8, GROUP, levels)

        def level_mix(b):
            for pair in range(4):
                joined = jnp.concatenate(
                    [banded[b % 2, 2 * pair], banded[b % 2, 2 * pair + 1]], axis=1
                )
                mixed = jnp.dot(row_loc[...], joined, preferred_element_type=f32).astype(bf16)
                localized = jnp.dot(mixed, level_loc[...], preferred_element_type=f32)
                for k in range(2):
                    j = 8 * b + 2 * pair + k
                    acc[j] += fine[8 + j].astype(f32) * localized[:, k * levels : (k + 1) * levels]

        for b in range(0, kept // 8, 2):
            band_mix(b)
            band_mix(b + 1)
            level_mix(b)
            level_mix(b + 1)

            @pl.when(m == members - 1)
            def _():
                for slot in (b, b + 1):
                    for pair in range(4):
                        two = [acc[8 * slot + 2 * pair + k] for k in range(2)]
                        for h in range(2):
                            at = slice(h * levels // 2, (h + 1) * levels // 2)
                            part[slot, h, pair] = jnp.concatenate(
                                [value[:, at] for value in two], axis=1
                            ).astype(bf16)
                if b > 0:
                    send_slot(b - 2)
                    send_slot(b - 1)

    send_slot(kept // 8 - 2)
    send_slot(kept // 8 - 1)

    def step_first(k):
        for copy in first_copies(k):
            copy.wait_recv()
        if k % 2 == 0:
            total = part[slot_of(k, x), 1 - y].astype(f32) + first[k, 1 - y].astype(f32)
        else:
            total = part[slot_of(k, 1 - x), y].astype(f32) + first[k, 1 - x].astype(f32)
        mid[k] = total.astype(bf16)
        second_copy(k).start()

    def step_second(k):
        second_copy(k).wait_recv()
        kept_at = y if k % 2 == 0 else x
        total = part[slot_of(k, x), y].astype(f32) + first[k, kept_at].astype(f32)
        sums[k] = (total + second[k].astype(f32)).astype(bf16)
        owner = per_side * core + k // 2
        to_self = jnp.logical_and(z == owner, core == k % 2)

        @pl.when(jnp.logical_not(to_self))
        def _():
            pltpu.make_async_remote_copy(
                sums.at[k], far.at[z], send_far.at[k], recv_far.at[z],
                target(owner, x, k % 2, y), MESH,
            ).start()

        @pl.when(to_self)
        def _():
            pltpu.make_async_copy(sums.at[k], far.at[z], recv_far.at[z]).start()

    for k in range(0, count, 2):
        step_first(k)
        step_first(k + 1)
        step_second(k)
        step_second(k + 1)

    answer.wait()
    held, came = solved[:per_half, :people], solved_in[:per_half, :people]
    weights[:per_half, :] = jnp.where(y == 0, held, came)
    weights[per_half:, :] = jnp.where(y == 0, came, held)
    grams.wait_send()
    for m in range(members):
        for step in range(1, chips):
            raw_copy(m, step).wait_send()
        pair_copy(m).wait_send()
    for k in range(count):
        done(slots.at[(k // 2) * 4 + x * 2 + k % 2, y], send_x.at[k])
    for k in range(2 * count):
        done(slots.at[k, y], send_y.at[k])
    for zz in range(depth):
        @pl.when(direct(zz))
        def _():
            done(own.at[y], send_a.at[zz])

        if not is_gate(zz):
            @pl.when(relays(zz))
            def _():
                for k in range(count):
                    done(own.at[y], send_z.at[k, zz])

    for zz in range(depth):
        done(far.at[zz], recv_far.at[zz])

    half = levels // 2
    for pair in range(4):
        value = far[0, pair].astype(f32)
        for zz in range(1, depth):
            value = value + far[zz, pair].astype(f32)
        value = value.T * scale
        for k in range(2):
            result[:, 2 * pair + k, :] = value[k * half : (k + 1) * half]
    for k in range(count):
        for copy in first_copies(k):
            copy.wait_send()
        second_copy(k).wait_send()
        owner = per_side * core + k // 2

        @pl.when(jnp.logical_not(jnp.logical_and(z == owner, core == k % 2)))
        def _():
            done(sums.at[k], send_far.at[k])


def fused(
    raw, ctrl, band, columns_in, row_weights, row_loc, level_loc, observed, innov, precision, region,
    depth, scale
):
    bf16, f32 = jnp.bfloat16, jnp.float32
    chips = depth * 2
    members = raw.shape[0] // chips
    columns = 8 * chips + 16
    coarse_rows, rows = row_weights.shape[1] // 2, row_weights.shape[1]
    levels = row_loc.shape[0]
    people = observed.shape[0]
    kept = columns - 16
    count = depth
    loaded = (
        ctrl, band, columns_in, row_weights, row_loc, level_loc, observed, innov, precision, region
    )
    dma = pltpu.SemaphoreType.DMA
    vmem = pl.BlockSpec(memory_space=pltpu.VMEM)
    own = jax.ShapeDtypeStruct((2, 4 * rows + 16, levels), bf16)
    piece = (4, rows, levels)
    flops = 2 * members * levels * rows * columns * (coarse_rows + 24 * GROUP + rows + levels)
    return pl.pallas_call(
        functools.partial(fused_kernel, depth, scale),
        out_shape=(
            jax.ShapeDtypeStruct((levels // 2, 8, rows), f32),
            jax.ShapeDtypeStruct((NREG, people), f32),
        ),
        in_specs=[pl.BlockSpec(memory_space=pltpu.HBM)] * 11,
        out_specs=(vmem, vmem),
        scratch_shapes=[
            *[pltpu.VMEM(value.shape, value.dtype) for value in loaded],
            dma((len(loaded),)),
            pltpu.VMEM(own.shape, bf16),
            pltpu.VMEM((columns, raw.shape[2]), bf16),
            pltpu.VMEM((rows, coarse_rows), bf16),
            pltpu.VMEM((2 * levels, 2 * levels), bf16),
            pltpu.VMEM((2 * kept + 16, levels), f32),
            pltpu.VMEM((NREG, people, 128), f32),
            pltpu.VMEM((NREG // 2, people, 128), f32),
            pltpu.VMEM((8, 128), f32),
            pltpu.VMEM((8, 128), f32),
            pltpu.VMEM((members, chips, 2) + raw.shape[1:], bf16),
            pltpu.VMEM((kept // 8,) + own.shape, bf16),
            pltpu.VMEM(own.shape, bf16),
            pltpu.VMEM((columns * (coarse_rows + 8), levels), f32),
            pltpu.VMEM((columns, rows, levels), bf16),
            pltpu.VMEM((columns, rows, levels), bf16),
            pltpu.VMEM((2, 8, rows, levels), bf16),
            pltpu.VMEM((kept // 8, 8 * GROUP, 24 * GROUP), bf16),
            pltpu.VMEM((kept, rows, levels), f32),
            pltpu.VMEM((kept // 8, 2) + piece, bf16),
            pltpu.VMEM((count, 2) + piece, bf16),
            pltpu.VMEM((count,) + piece, bf16),
            pltpu.VMEM((count,) + piece, bf16),
            pltpu.VMEM((count,) + piece, bf16),
            pltpu.VMEM((depth,) + piece, bf16),
            dma((members, chips)), dma((members, chips)), dma((members,)), dma((members,)),
            dma((depth,)), dma((count,)), dma((count,)), dma((count,)),
            dma((2 * count,)), dma((2 * count,)), dma, dma,
            dma((count, 2)), dma((count, 2)), dma((count,)), dma((count,)), dma((count,)), dma((depth,)),
            dma, dma, dma, dma, dma((count, depth)),
        ],
        compiler_params=pltpu.CompilerParams(
            collective_id=0, has_side_effects=True, vmem_limit_bytes=67043328
        ),
        cost_estimate=pl.CostEstimate(flops=flops, bytes_accessed=4 * raw.size, transcendentals=0),
    )(raw, *loaded)


def member_plan(
    ens_coarse,
    col_interp,
    row_weights,
    ctrl_vec,
    band_loc,
    row_loc,
    level_loc,
    hx_pert,
    innov,
    obs_prec,
    obs_region,
):
    raw = jnp.transpose(ens_coarse[0], (0, 2, 3, 1))
    increment, weights = fused(
        raw, ctrl_vec[0], band_loc, col_interp.T, row_weights, row_loc, level_loc,
        hx_pert[0], innov, obs_prec, obs_region,
        lax.axis_size("tile") // 4, 1.0 / (hx_pert.shape[1] - 1),
    )
    return (increment[None], weights)


def fits(mesh_sizes, total_members, block, columns, fine_rows, levels):
    tiles = mesh_sizes["tile"]
    members, block_rows, width = block[1], block[3], block[4]
    return (
        mesh_sizes["grp"] == 1
        and mesh_sizes["mem"] == 2
        and tiles % 8 == 0
        and members % (tiles // 2) == 0
        and tiles * columns == levels
        and width <= levels
        and total_members % 8 == 0
        and total_members + 48 == levels
        and columns == 8
        and block_rows == 4
        and fine_rows == 128
        and levels == 128
    )


def body(
    ens_coarse,
    col_interp,
    row_weights,
    ctrl_vec,
    band_loc,
    row_loc,
    level_loc,
    hx_pert,
    innov,
    obs_prec,
    obs_region,
):
    sizes = {axis: lax.axis_size(axis) for axis in ("grp", "tile", "mem")}
    total_members = hx_pert.shape[1]
    if fits(sizes, total_members, ens_coarse.shape, band_loc.shape[0], row_loc.shape[0], level_loc.shape[0]):
        return member_plan(
            ens_coarse, col_interp, row_weights, ctrl_vec, band_loc, row_loc, level_loc,
            hx_pert, innov, obs_prec, obs_region,
        )
    observed = hx_pert[0]
    weighted = (observed * obs_prec[0][None, :]).astype(jnp.bfloat16)
    labels = lax.broadcasted_iota(jnp.int32, (NREG, observed.shape[1]), 0)
    member_of = obs_region[0][None, :] == labels
    masked = jnp.where(member_of[:, None, :], weighted[None], jnp.zeros((), jnp.bfloat16))
    gram_sums = jnp.einsum("rko,jo->rkj", masked, observed, preferred_element_type=jnp.float32)
    innov_rows = jnp.where(member_of, innov[0][None, :], 0.0)
    right_side = jnp.dot(
        innov_rows, weighted.astype(jnp.float32).T, precision=lax.Precision.HIGHEST
    )
    sums = jnp.concatenate([gram_sums, right_side[:, :, None]], axis=2)
    sums = swap_add(lax.psum(sums, "grp") if lax.axis_size("grp") > 1 else sums)
    increment = plain_increment(
        ens_coarse, col_interp, row_weights, ctrl_vec, band_loc, row_loc, level_loc, total_members
    )
    own_weights = solve_weights(sums)
    weights = collect(own_weights)
    return (increment[None], weights)


def solution(mesh):
    placed = (
        P("grp", "mem", None, "tile", None),
        P(),
        P(),
        P("grp", None, "tile", None),
        P("tile", None),
        P(),
        P(),
        P("grp", None, ("tile", "mem")),
        P("grp", ("tile", "mem")),
        P("grp", ("tile", "mem")),
        P("grp", ("tile", "mem")),
    )
    return jax.shard_map(
        body,
        mesh=mesh,
        in_specs=placed,
        out_specs=(P("grp", "mem", "tile", None), P("tile", None)),
        check_vma=False,
    )
```

```python
import functools

import jax
import jax.numpy as jnp
from jax import lax
from jax.experimental import pallas as pl
from jax.experimental.pallas import tpu as pltpu
from jax.sharding import PartitionSpec as P

NREG = 8
GROUP = 16
MESH = pl.DeviceIdType.MESH


def extended(value, sides, width):
    for axis, dim in sides:
        peers, length = (lax.axis_size(axis), value.shape[dim])
        up = [(i, (i + 1) % peers) for i in range(peers - 1)]
        down = [(j, i) for i, j in up]
        last = lax.slice_in_dim(value, length - width, length, axis=dim)
        first = lax.slice_in_dim(value, 0, width, axis=dim)
        before = lax.ppermute(last, axis, up)
        after = lax.ppermute(first, axis, down)
        value = jnp.concatenate([before, value, after], axis=dim)
    return value


def swap_add(value):
    peers = lax.axis_size("mem")
    me = lax.axis_index("mem")
    length = value.shape[0] // peers
    total = lax.dynamic_slice_in_dim(value, me * length, length, 0)
    for shift in range(1, peers):
        other = lax.rem(me + shift, peers)
        part = lax.dynamic_slice_in_dim(value, other * length, length, 0)
        pairs = [(i, (i + shift) % peers) for i in range(peers)]
        total = total + lax.ppermute(part, "mem", pairs)
    return total


def collect(value):
    peers = lax.axis_size("mem")
    me = lax.axis_index("mem")
    length = value.shape[0]
    result = jnp.zeros((peers * length,) + value.shape[1:], value.dtype)
    result = lax.dynamic_update_slice_in_dim(result, value, me * length, 0)
    for shift in range(1, peers):
        pairs = [(i, (i + shift) % peers) for i in range(peers)]
        moved = lax.ppermute(value, "mem", pairs)
        source = lax.rem(me + peers - shift, peers)
        result = lax.dynamic_update_slice_in_dim(result, moved, source * length, 0)
    return result


def row_matrix(row_weights, fine_rows, coarse_rows):
    fine_index = lax.broadcasted_iota(jnp.int32, (fine_rows, coarse_rows), 0)
    coarse_index = lax.broadcasted_iota(jnp.int32, (fine_rows, coarse_rows), 1)
    weights = row_weights.astype(jnp.float32)
    stencil = jnp.zeros((fine_rows, coarse_rows), jnp.float32)
    for offset in range(3):
        matched = coarse_index == fine_index // 2 + offset - 1
        stencil = stencil + jnp.where(matched, weights[offset][:, None], 0.0)
    return stencil.astype(jnp.bfloat16)


def eliminate(tables):
    members, lanes = tables[0].shape
    row_index = lax.broadcasted_iota(jnp.int32, (members, lanes), 0)
    col_index = lax.broadcasted_iota(jnp.int32, (members, lanes), 1)
    filler = jnp.zeros((lanes - members, lanes), jnp.float32)
    systems = []
    for table in tables:
        mirrored = jnp.concatenate([table, filler], axis=0).T[:members]
        table = jnp.where(col_index < members, 0.5 * (table + mirrored), table)
        systems.append(table + jnp.where(row_index == col_index, float(members - 1), 0.0))
    for k in range(members):
        for region, table in enumerate(systems):
            column = jnp.broadcast_to(table[:, k : k + 1], table.shape)
            row = table[k : k + 1] * (1.0 / column[k : k + 1])
            column = jnp.where(row_index == k, column - 1.0, column)
            systems[region] = table - column * row
    return [jnp.concatenate([table, filler], axis=0).T[members : members + 8] for table in systems]


def solve_kernel(sums, result):
    for region, rows in enumerate(eliminate([sums[r] for r in range(sums.shape[0])])):
        result[region] = rows


def solve_weights(sums):
    regions, members, width = sums.shape
    lanes = 128 * (-(-(members + 8) // 128))
    padded = jnp.pad(sums, ((0, 0), (0, 0), (0, lanes - width)))
    result = pl.pallas_call(
        solve_kernel,
        out_shape=jax.ShapeDtypeStruct((regions, 8, lanes), jnp.float32),
        in_specs=[pl.BlockSpec(memory_space=pltpu.VMEM)],
        out_specs=pl.BlockSpec(memory_space=pltpu.VMEM),
        cost_estimate=pl.CostEstimate(flops=10**9, bytes_accessed=4 * padded.size, transcendentals=0),
    )(padded)
    return result[:, 0, :members]


def plain_increment(
    ens_coarse, col_interp, row_weights, ctrl_vec, band_loc, row_loc, level_loc, total_members
):
    fine_rows = row_weights.shape[1]
    columns = band_loc.shape[0]
    coarse_cols = jnp.einsum(
        "tklic,jc->tklij", ens_coarse, col_interp, preferred_element_type=jnp.float32
    ).astype(jnp.bfloat16)
    stencil = row_matrix(row_weights, fine_rows, fine_rows // 2)
    refined = jnp.einsum(
        "tklij,ri->tkljr",
        lax.all_to_all(coarse_cols, "tile", split_axis=4, concat_axis=3, tiled=True),
        stencil,
        preferred_element_type=jnp.float32,
    ).astype(jnp.bfloat16)
    member_fine = refined[0]
    slot_term = member_fine * ctrl_vec[0][None]
    projected = slot_term.astype(jnp.bfloat16)
    if lax.axis_size("grp") > 1:
        projected = lax.psum(projected, "grp")
    padded = extended(projected, (("tile", 2),), columns)
    banded = jnp.einsum(
        "jq,klqr->kljr", band_loc, padded, preferred_element_type=jnp.float32
    ).astype(jnp.bfloat16)
    row_mixed = jnp.einsum(
        "kljs,rs->kljr", banded, row_loc, preferred_element_type=jnp.float32
    ).astype(jnp.bfloat16)
    localized = jnp.einsum(
        "lm,kmjr->kljr", level_loc, row_mixed, preferred_element_type=jnp.float32
    ).astype(jnp.bfloat16)
    return swap_add(
        jnp.sum(member_fine.astype(jnp.float32) * localized.astype(jnp.float32), axis=0)
    ) / (total_members - 1)


def place():
    tile = lax.axis_index("tile")
    core = lax.rem(tile, 2)
    chip = lax.div(tile, 2)
    return lax.div(chip, 2), lax.rem(chip, 2), core, lax.axis_index("mem")


def target(z, x, core, y):
    return {"tile": (z * 2 + x) * 2 + core, "mem": y}


def greet(peers):
    barrier = pltpu.get_barrier_semaphore()
    for peer in peers:
        pl.semaphore_signal(barrier, inc=1, device_id=peer, device_id_type=MESH)
    pl.semaphore_wait(barrier, len(peers))


def fused_kernel(
    depth, scale, raw, *refs
):
    sources, refs = refs[:10], refs[10:]
    outputs, places, refs = refs[:2], refs[2:12], refs[12:]
    loads, refs = refs[0], refs[1:]
    copies = [
        pltpu.make_async_copy(source, place_in, loads.at[n])
        for n, (source, place_in) in enumerate(zip(sources, places))
    ]
    for copy in copies:
        copy.start()
    fused_steps(depth, scale, raw, copies, *places, *outputs, *refs)


def fused_steps(
    depth, scale, raw, copies, ctrl, band_in, columns_in, row_weights, row_loc, levels_in,
    observed, innov, precision, region, result, weights,
    own, interp, stencil, level_loc, shifted, gram, gram_in, solved, solved_in,
    blocks, slots, halo, coarse, fine, proj, banded, kron, acc, part,
    first, mid, second, sums, far,
    send_raw, recv_raw, send_pair, recv_pair,
    send_a, recv_a, send_x, recv_x, send_y, recv_y, send_h, recv_h,
    send_first, recv_first, send_second, recv_second, send_far, recv_far,
    send_g, recv_g, send_w, recv_w, send_z
):
    z, x, core, y = place()
    f32, bf16 = jnp.float32, jnp.bfloat16
    members, chips = blocks.shape[0], blocks.shape[1]
    columns, rows, levels = fine.shape
    coarse_rows = stencil.shape[1]
    stride = coarse_rows + 8
    kept = acc.shape[0]
    per_side = depth // 2
    count = per_side * 2
    side = lax.div(z, per_side)
    chip = z * 2 + x
    across, beside = target(z, x, core, 1 - y), target(z, 1 - x, core, y)
    partner = target(z, x, 1 - core, y)
    copies[0].wait()
    for j in range(8):
        own[j // 4, (j % 4) * rows : (j % 4 + 1) * rows, :] = ctrl[:, j, :].T.astype(bf16)
    copies[1].wait()
    window = band_in.shape[1]
    widen = (
        lax.broadcasted_iota(jnp.int32, (window, levels), 0)
        == lax.broadcasted_iota(jnp.int32, (window, levels), 1)
    ).astype(bf16)
    band_rows = jnp.dot(band_in[...], widen, preferred_element_type=f32)
    band_rows = jnp.concatenate([band_rows, jnp.zeros_like(band_rows)], axis=0).astype(bf16)
    for h in range(2):
        own[h, 4 * rows : 4 * rows + 16, :] = band_rows
    line = [(lax.rem(z + dz, depth), lax.rem(core + dc, 2)) for dz in range(depth) for dc in range(2)]
    greet(
        [target(zz, x, cc, y) for zz, cc in line[1:]]
        + [target(lax.rem(z + dz, depth), 1 - x, core, y) for dz in range(depth)]
        + [across, target(z, 1 - x, core, 1 - y)]
    )

    mine = lax.rem(z, per_side) * 4 + x * 2 + core
    kind = lax.rem(z, per_side) * 2 + core

    def is_self(zz):
        return jnp.logical_and(z == zz, core == side)

    def is_gate(zz):
        return zz == per_side - 1 + zz // per_side

    def direct(zz):
        near_side = True if is_gate(zz) else side == zz // per_side
        return jnp.logical_and(jnp.logical_not(is_self(zz)), near_side)

    def relays(zz):
        here = jnp.logical_and(side == zz // per_side, side != core)
        return jnp.logical_and(here, z == per_side - 1 + side)

    for zz in range(depth):
        @pl.when(direct(zz))
        def _():
            pltpu.make_async_remote_copy(
                own.at[y], slots.at[mine, y], send_a.at[zz], recv_a.at[kind],
                target(zz, x, side, y), MESH,
            ).start()

        @pl.when(is_self(zz))
        def _():
            pltpu.make_async_copy(own.at[y], slots.at[mine, y], recv_a.at[kind]).start()

    def raw_copy(m, step):
        to = lax.rem(chip + step, chips)
        return pltpu.make_async_remote_copy(
            raw.at[to * members + m], blocks.at[m, chip, core], send_raw.at[m, step],
            recv_raw.at[m, chip], target(lax.div(to, 2), lax.rem(to, 2), core, y), MESH,
        )

    def send_member(m):
        for step in range(1, chips):
            raw_copy(m, step).start()
        pltpu.make_async_copy(
            raw.at[chip * members + m], blocks.at[m, chip, core], recv_raw.at[m, chip]
        ).start()

    def pair_copy(m):
        held = blocks.at[m, :, core]
        return pltpu.make_async_remote_copy(held, held, send_pair.at[m], recv_pair.at[m], partner, MESH)

    early = min(2, members)
    for m in range(early):
        send_member(m)

    def done(ref, sem):
        pltpu.make_async_copy(ref, ref, sem).wait()

    for copy in copies[2:]:
        copy.wait()
    people, spots = observed.shape
    hx = observed[...]
    weighted = (hx.astype(f32) * precision[...]).astype(bf16).astype(f32)
    rest = innov[...]
    thirds = jnp.zeros((48, spots), f32)
    third_at = lax.broadcasted_iota(jnp.int32, (48, spots), 0)
    for n in range(3):
        third = rest.astype(bf16).astype(f32)
        thirds = jnp.where(third_at == n, third, thirds)
        rest = rest - third
    right = jnp.concatenate([hx, thirds.astype(bf16)], axis=0)
    for g in range(NREG):
        masked = jnp.where(region[...] == g, weighted, 0.0).astype(bf16)
        gram[g] = lax.dot_general(
            masked, right, (((1,), (1,)), ((), ())), preferred_element_type=f32
        )
    per_half = NREG // 2
    grams = pltpu.make_async_remote_copy(
        gram.at[pl.ds((1 - y) * per_half, per_half)], gram_in, send_g, recv_g, across, MESH
    )
    grams.start()

    coarse_width = columns_in.shape[0]
    fill = jnp.zeros((levels - coarse_width, levels), f32)
    shifted[...] = jnp.zeros_like(shifted)
    shifted[8 : 8 + levels, :] = jnp.concatenate([columns_in[...].astype(f32), fill], axis=0).T
    interp[...] = shifted[pl.ds(pl.multiple_of(core * kept, 8), columns), :][:, :coarse_width].astype(bf16)
    coarse_at = lax.broadcasted_iota(jnp.int32, (coarse_rows, rows), 0)
    parent_at = lax.broadcasted_iota(jnp.int32, (coarse_rows, rows), 1) // 2
    spreading = jnp.zeros((coarse_rows, rows), f32)
    for n in range(3):
        spreading = spreading + jnp.where(
            coarse_at == parent_at + n - 1, row_weights[n : n + 1, :].astype(f32), 0.0
        )
    stencil[...] = jnp.concatenate([spreading, fill], axis=0).T[:, :coarse_rows].astype(bf16)
    flipped = levels_in[...].astype(f32).T.astype(bf16)
    level_loc[...] = jnp.zeros_like(level_loc)
    level_loc[:levels, :levels] = flipped
    level_loc[levels:, levels:] = flipped

    def forward(slot, send, recv, peer):
        held = slots.at[slot, y]
        pltpu.make_async_remote_copy(held, held, send, recv, peer, MESH).start()

    for k in range(count):
        slot = (k // 2) * 4 + x * 2 + k % 2
        done(slots.at[slot, y], recv_a.at[k])
        for zz in range(depth):
            if not is_gate(zz):
                @pl.when(relays(zz))
                def _():
                    forward(slot, send_z.at[k, zz], recv_a.at[k], target(zz, x, core, y))

        forward(slot, send_x.at[k], recv_x.at[k], beside)
        forward(slot, send_y.at[k], recv_y.at[k], across)
    for k in range(count):
        slot = (k // 2) * 4 + (1 - x) * 2 + k % 2
        done(slots.at[slot, y], recv_x.at[k])
        forward(slot, send_y.at[count + k], recv_y.at[count + k], across)
    for m in range(early, members):
        send_member(m)
    grams.wait_recv()
    answers = eliminate([gram[y * per_half + g] + gram_in[g] for g in range(per_half)])
    for g, rows_solved in enumerate(answers):
        solved[g : g + 1, :] = rows_solved[0:1] + rows_solved[1:2] + rows_solved[2:3]
    solved[per_half:, :] = jnp.zeros_like(solved[per_half:, :])
    for k in range(count):
        done(slots.at[(k // 2) * 4 + x * 2 + k % 2, 1 - y], recv_y.at[k])
    for k in range(count):
        done(slots.at[(k // 2) * 4 + (1 - x) * 2 + k % 2, 1 - y], recv_y.at[count + k])
    edges = pltpu.make_async_remote_copy(
        slots.at[(1 - core) * (2 * count - 1)], halo, send_h, recv_h, partner, MESH
    )
    edges.start()

    acc[...] = jnp.zeros_like(acc)
    tall_at = lax.broadcasted_iota(jnp.int32, (128, 8), 0)
    wide_at = lax.broadcasted_iota(jnp.int32, (128, 24 * GROUP), 1)
    deep_at = lax.broadcasted_iota(jnp.int32, (128, 24 * GROUP), 0)
    spread_rows = (tall_at // GROUP == lax.broadcasted_iota(jnp.int32, (128, 8), 1)).astype(bf16)
    spread_cols = (deep_at == wide_at // GROUP).astype(bf16)
    same = lax.rem(deep_at, GROUP) == lax.rem(wide_at, GROUP)
    for b in range(kept // 8):
        band = slots[b, 0, 4 * rows : 4 * rows + 8, :]
        tall = jnp.dot(spread_rows, band, preferred_element_type=f32).astype(bf16)
        wide = jnp.dot(tall, spread_cols, preferred_element_type=f32)
        kron[b] = jnp.where(same, wide, 0.0).astype(bf16)
    edges.wait()
    answer = pltpu.make_async_remote_copy(solved, solved_in, send_w, recv_w, across, MESH)
    answer.start()

    def slot_of(k, xx):
        return (k // 2) * 4 + xx * 2 + k % 2

    def first_copies(k, only=None):
        if k % 2 == 0:
            pieces = [(part.at[slot_of(k, 1 - x)], first.at[k], beside)]
        else:
            pieces = [(part.at[slot_of(k, xx), 1 - y], first.at[k, xx], across) for xx in range(2)]
        if only is not None:
            pieces = pieces[only : only + 1]
        return [
            pltpu.make_async_remote_copy(
                source, landing, send_first.at[k, n], recv_first.at[k, n], peer, MESH
            )
            for n, (source, landing, peer) in enumerate(pieces, only or 0)
        ]

    def second_copy(k):
        peer = across if k % 2 == 0 else beside
        return pltpu.make_async_remote_copy(
            mid.at[k], second.at[k], send_second.at[k], recv_second.at[k], peer, MESH
        )

    def send_slot(b):
        k, xx = (b // 4) * 2 + b % 2, (b // 2) % 2
        if k % 2 == 1:
            first_copies(k, xx)[0].start()
        else:
            @pl.when(x != xx)
            def _():
                first_copies(k)[0].start()

    def refine(pair, table):
        base = 2 * pair * stride
        joined = jnp.concatenate(
            [coarse[pl.ds(base + k * stride, coarse_rows), :].astype(bf16) for k in range(2)], axis=1
        )
        fresh = jnp.dot(stencil[...], joined, preferred_element_type=f32).astype(bf16)
        for k in range(2):
            piece = fresh[:, k * levels : (k + 1) * levels]
            j = 2 * pair + k
            fine[j] = piece
            proj[j] = (piece.astype(f32) * table(k).astype(f32)).astype(bf16)

    @pl.loop(0, members)
    def _(m):
        for c in range(chips):
            done(blocks.at[m, c, core], recv_raw.at[m, c])
        copy = pair_copy(m)
        copy.start()
        def interpolate(half):
            for c in range(chips):
                for two in range(2):
                    pair = jnp.concatenate(
                        [blocks[m, c, half, 2 * two], blocks[m, c, half, 2 * two + 1]], axis=1
                    )
                    mixed = jnp.dot(interp[...], pair, preferred_element_type=f32)
                    row = 8 * c + 4 * half + 2 * two
                    for k in range(2):
                        coarse[pl.ds(row + k, columns, stride=stride), :] = mixed[
                            :, k * levels : (k + 1) * levels
                        ]

        interpolate(core)
        copy.wait_recv()
        interpolate(1 - core)

        for pair in range(4):
            def table(k):
                j = 2 * pair + k
                return halo[j // 4, (j % 4) * rows : (j % 4 + 1) * rows, :]

            refine(pair, table)
            refine(columns // 2 - 4 + pair, table)

        for b in range(kept // 8):
            for pair in range(4):
                def table(k):
                    j = 2 * pair + k
                    return slots[b, j // 4, (j % 4) * rows : (j % 4 + 1) * rows, :]

                refine(4 + 4 * b + pair, table)

        def band_mix(b):
            for pair in range(rows // (2 * GROUP)):
                parts = []
                for k in range(2):
                    at = (2 * pair + k) * GROUP
                    parts.append(proj[8 * b : 8 * b + 24, at : at + GROUP, :].reshape(24 * GROUP, levels))
                mixed = jnp.dot(
                    kron[b], jnp.concatenate(parts, axis=1), preferred_element_type=f32
                ).astype(bf16)
                for k in range(2):
                    at = (2 * pair + k) * GROUP
                    banded[b % 2, :, at : at + GROUP, :] = mixed[
                        :, k * levels : (k + 1) * levels
                    ].reshape(8, GROUP, levels)

        def level_mix(b):
            for pair in range(4):
                joined = jnp.concatenate(
                    [banded[b % 2, 2 * pair], banded[b % 2, 2 * pair + 1]], axis=1
                )
                mixed = jnp.dot(row_loc[...], joined, preferred_element_type=f32).astype(bf16)
                localized = jnp.dot(mixed, level_loc[...], preferred_element_type=f32)
                for k in range(2):
                    j = 8 * b + 2 * pair + k
                    acc[j] += fine[8 + j].astype(f32) * localized[:, k * levels : (k + 1) * levels]

        for b in range(0, kept // 8, 2):
            band_mix(b)
            band_mix(b + 1)
            level_mix(b)
            level_mix(b + 1)

            @pl.when(m == members - 1)
            def _():
                for slot in (b, b + 1):
                    for pair in range(4):
                        two = [acc[8 * slot + 2 * pair + k] for k in range(2)]
                        for h in range(2):
                            at = slice(h * levels // 2, (h + 1) * levels // 2)
                            part[slot, h, pair] = jnp.concatenate(
                                [value[:, at] for value in two], axis=1
                            ).astype(bf16)
                if b > 0:
                    send_slot(b - 2)
                    send_slot(b - 1)

    send_slot(kept // 8 - 2)
    send_slot(kept // 8 - 1)

    def step_first(k):
        for copy in first_copies(k):
            copy.wait_recv()
        if k % 2 == 0:
            total = part[slot_of(k, x), 1 - y].astype(f32) + first[k, 1 - y].astype(f32)
        else:
            total = part[slot_of(k, 1 - x), y].astype(f32) + first[k, 1 - x].astype(f32)
        mid[k] = total.astype(bf16)
        second_copy(k).start()

    def step_second(k):
        second_copy(k).wait_recv()
        kept_at = y if k % 2 == 0 else x
        total = part[slot_of(k, x), y].astype(f32) + first[k, kept_at].astype(f32)
        sums[k] = (total + second[k].astype(f32)).astype(bf16)
        owner = per_side * core + k // 2
        to_self = jnp.logical_and(z == owner, core == k % 2)

        @pl.when(jnp.logical_not(to_self))
        def _():
            pltpu.make_async_remote_copy(
                sums.at[k], far.at[z], send_far.at[k], recv_far.at[z],
                target(owner, x, k % 2, y), MESH,
            ).start()

        @pl.when(to_self)
        def _():
            pltpu.make_async_copy(sums.at[k], far.at[z], recv_far.at[z]).start()

    for k in range(0, count, 2):
        step_first(k)
        step_first(k + 1)
        step_second(k)
        step_second(k + 1)

    answer.wait()
    held, came = solved[:per_half, :people], solved_in[:per_half, :people]
    weights[:per_half, :] = jnp.where(y == 0, held, came)
    weights[per_half:, :] = jnp.where(y == 0, came, held)
    grams.wait_send()
    for m in range(members):
        for step in range(1, chips):
            raw_copy(m, step).wait_send()
        pair_copy(m).wait_send()
    for k in range(count):
        done(slots.at[(k // 2) * 4 + x * 2 + k % 2, y], send_x.at[k])
    for k in range(2 * count):
        done(slots.at[k, y], send_y.at[k])
    for zz in range(depth):
        @pl.when(direct(zz))
        def _():
            done(own.at[y], send_a.at[zz])

        if not is_gate(zz):
            @pl.when(relays(zz))
            def _():
                for k in range(count):
                    done(own.at[y], send_z.at[k, zz])

    for zz in range(depth):
        done(far.at[zz], recv_far.at[zz])

    half = levels // 2
    for pair in range(4):
        value = far[0, pair].astype(f32)
        for zz in range(1, depth):
            value = value + far[zz, pair].astype(f32)
        value = value.T * scale
        for k in range(2):
            result[:, 2 * pair + k, :] = value[k * half : (k + 1) * half]
    for k in range(count):
        for copy in first_copies(k):
            copy.wait_send()
        second_copy(k).wait_send()
        owner = per_side * core + k // 2

        @pl.when(jnp.logical_not(jnp.logical_and(z == owner, core == k % 2)))
        def _():
            done(sums.at[k], send_far.at[k])


def fused(
    raw, ctrl, band, columns_in, row_weights, row_loc, level_loc, observed, innov, precision, region,
    depth, scale
):
    bf16, f32 = jnp.bfloat16, jnp.float32
    chips = depth * 2
    members = raw.shape[0] // chips
    columns = 8 * chips + 16
    coarse_rows, rows = row_weights.shape[1] // 2, row_weights.shape[1]
    levels = row_loc.shape[0]
    people = observed.shape[0]
    kept = columns - 16
    count = depth
    loaded = (
        ctrl, band, columns_in, row_weights, row_loc, level_loc, observed, innov, precision, region
    )
    dma = pltpu.SemaphoreType.DMA
    vmem = pl.BlockSpec(memory_space=pltpu.VMEM)
    own = jax.ShapeDtypeStruct((2, 4 * rows + 16, levels), bf16)
    piece = (4, rows, levels)
    flops = 2 * members * levels * rows * columns * (coarse_rows + 24 * GROUP + rows + levels)
    return pl.pallas_call(
        functools.partial(fused_kernel, depth, scale),
        out_shape=(
            jax.ShapeDtypeStruct((levels // 2, 8, rows), f32),
            jax.ShapeDtypeStruct((NREG, people), f32),
        ),
        in_specs=[pl.BlockSpec(memory_space=pltpu.HBM)] * 11,
        out_specs=(vmem, vmem),
        scratch_shapes=[
            *[pltpu.VMEM(value.shape, value.dtype) for value in loaded],
            dma((len(loaded),)),
            pltpu.VMEM(own.shape, bf16),
            pltpu.VMEM((columns, raw.shape[2]), bf16),
            pltpu.VMEM((rows, coarse_rows), bf16),
            pltpu.VMEM((2 * levels, 2 * levels), bf16),
            pltpu.VMEM((2 * kept + 16, levels), f32),
            pltpu.VMEM((NREG, people, 128), f32),
            pltpu.VMEM((NREG // 2, people, 128), f32),
            pltpu.VMEM((8, 128), f32),
            pltpu.VMEM((8, 128), f32),
            pltpu.VMEM((members, chips, 2) + raw.shape[1:], bf16),
            pltpu.VMEM((kept // 8,) + own.shape, bf16),
            pltpu.VMEM(own.shape, bf16),
            pltpu.VMEM((columns * (coarse_rows + 8), levels), f32),
            pltpu.VMEM((columns, rows, levels), bf16),
            pltpu.VMEM((columns, rows, levels), bf16),
            pltpu.VMEM((2, 8, rows, levels), bf16),
            pltpu.VMEM((kept // 8, 8 * GROUP, 24 * GROUP), bf16),
            pltpu.VMEM((kept, rows, levels), f32),
            pltpu.VMEM((kept // 8, 2) + piece, bf16),
            pltpu.VMEM((count, 2) + piece, bf16),
            pltpu.VMEM((count,) + piece, bf16),
            pltpu.VMEM((count,) + piece, bf16),
            pltpu.VMEM((count,) + piece, bf16),
            pltpu.VMEM((depth,) + piece, bf16),
            dma((members, chips)), dma((members, chips)), dma((members,)), dma((members,)),
            dma((depth,)), dma((count,)), dma((count,)), dma((count,)),
            dma((2 * count,)), dma((2 * count,)), dma, dma,
            dma((count, 2)), dma((count, 2)), dma((count,)), dma((count,)), dma((count,)), dma((depth,)),
            dma, dma, dma, dma, dma((count, depth)),
        ],
        compiler_params=pltpu.CompilerParams(
            collective_id=0, has_side_effects=True, vmem_limit_bytes=67043328
        ),
        cost_estimate=pl.CostEstimate(flops=flops, bytes_accessed=4 * raw.size, transcendentals=0),
    )(raw, *loaded)


def member_plan(
    ens_coarse,
    col_interp,
    row_weights,
    ctrl_vec,
    band_loc,
    row_loc,
    level_loc,
    hx_pert,
    innov,
    obs_prec,
    obs_region,
):
    raw = jnp.transpose(ens_coarse[0], (0, 2, 3, 1))
    increment, weights = fused(
        raw, ctrl_vec[0], band_loc, col_interp.T, row_weights, row_loc, level_loc,
        hx_pert[0], innov, obs_prec, obs_region,
        lax.axis_size("tile") // 4, 1.0 / (hx_pert.shape[1] - 1),
    )
    return (increment[None], weights)


def fits(mesh_sizes, total_members, block, columns, fine_rows, levels):
    tiles = mesh_sizes["tile"]
    members, block_rows, width = block[1], block[3], block[4]
    return (
        mesh_sizes["grp"] == 1
        and mesh_sizes["mem"] == 2
        and tiles % 8 == 0
        and members % (tiles // 2) == 0
        and tiles * columns == levels
        and width <= levels
        and total_members % 8 == 0
        and total_members + 48 == levels
        and columns == 8
        and block_rows == 4
        and fine_rows == 128
        and levels == 128
    )


def body(
    ens_coarse,
    col_interp,
    row_weights,
    ctrl_vec,
    band_loc,
    row_loc,
    level_loc,
    hx_pert,
    innov,
    obs_prec,
    obs_region,
):
    sizes = {axis: lax.axis_size(axis) for axis in ("grp", "tile", "mem")}
    total_members = hx_pert.shape[1]
    if fits(sizes, total_members, ens_coarse.shape, band_loc.shape[0], row_loc.shape[0], level_loc.shape[0]):
        return member_plan(
            ens_coarse, col_interp, row_weights, ctrl_vec, band_loc, row_loc, level_loc,
            hx_pert, innov, obs_prec, obs_region,
        )
    observed = hx_pert[0]
    weighted = (observed * obs_prec[0][None, :]).astype(jnp.bfloat16)
    labels = lax.broadcasted_iota(jnp.int32, (NREG, observed.shape[1]), 0)
    member_of = obs_region[0][None, :] == labels
    masked = jnp.where(member_of[:, None, :], weighted[None], jnp.zeros((), jnp.bfloat16))
    gram_sums = jnp.einsum("rko,jo->rkj", masked, observed, preferred_element_type=jnp.float32)
    innov_rows = jnp.where(member_of, innov[0][None, :], 0.0)
    right_side = jnp.dot(
        innov_rows, weighted.astype(jnp.float32).T, precision=lax.Precision.HIGHEST
    )
    sums = jnp.concatenate([gram_sums, right_side[:, :, None]], axis=2)
    sums = swap_add(lax.psum(sums, "grp") if lax.axis_size("grp") > 1 else sums)
    increment = plain_increment(
        ens_coarse, col_interp, row_weights, ctrl_vec, band_loc, row_loc, level_loc, total_members
    )
    own_weights = solve_weights(sums)
    weights = collect(own_weights)
    return (increment[None], weights)


def solution(mesh):
    placed = (
        P("grp", "mem", None, "tile", None),
        P(),
        P(),
        P("grp", None, "tile", None),
        P("tile", None),
        P(),
        P(),
        P("grp", None, ("tile", "mem")),
        P("grp", ("tile", "mem")),
        P("grp", ("tile", "mem")),
        P("grp", ("tile", "mem")),
    )
    return jax.shard_map(
        body,
        mesh=mesh,
        in_specs=placed,
        out_specs=(P("grp", "mem", "tile", None), P("tile", None)),
        check_vma=False,
    )
```
